32 devices in a mesh: gx: 4 (over x, core), gy: 2 (over y), gz: 4 (over z).
Axes of the slice: x: 2, y: 2, z: 4, core: 2. Of those that a mesh axis runs over, the one named last changes fastest.
Arguments:
- right_side: float32 [32, 32, 512], P('gx', 'gy', 'gz'), may hold values from -6 to 6
- conductance: float32 [32, 32, 512], P('gx', 'gy', 'gz'), may hold values from 0.25 to 4
- extents: int32 [4, 2, 4], P('gx', 'gy', 'gz'), may hold values from 64 to 128, as said below
- coarse_factor: bfloat16 [32, 32], replicated, may hold values from -1 to 3, as said below
Outputs:
- solution_field: float32 [32, 32, 512], P('gx', 'gy', 'gz')
- residual: float32 [32, 32, 512], P('gx', 'gy', 'gz')
The draws below stay inside these ranges and needn't reach their ends.
Inputs may be any that keep to these rules, and one draw needn't show every extreme that they name: `extents`: cells of a block whose third local index is below its count are fluid, the others padding; in every draw some block has all 128 layers fluid. `coarse_factor`: lower triangular with a positive diagonal.
All inputs are finite; a program needn't handle non-finite values.
Results may differ from the reference program's by a relative error of at most 0.0003.
Values sent between devices are 32-bit elements; how exact they have to be, the bound alone decides.
A program may use at most 64 MiB of HBM per device.

```python
import math
import jax
import jax.numpy as jnp
from jax import lax

CX = 8
CY = 16
CZ = 128
ITERS = 2
NX = 32
NY = 32
NZ = 512
NB = 32
N_GX = 4
N_GY = 2
N_GZ = 4


def draw_right_side(key, part):
    key_cells, key_blocks = jax.random.split(jax.random.fold_in(key, 11), 2)
    blocks = (NX // CX, NY // CY, NZ // CZ)
    values = jnp.clip(jax.random.normal(key_cells, (NX, NY, NZ), jnp.float32), -4.0, 4.0)
    offsets = jax.random.uniform(key_blocks, blocks, jnp.float32, -1.5, 1.5)
    spread = jnp.repeat(jnp.repeat(jnp.repeat(offsets, CX, axis=0), CY, axis=1), CZ, axis=2)
    return values + spread


def draw_extents(key, part):
    key_counts, key_full = jax.random.split(jax.random.fold_in(key, 23))
    blocks = (NX // CX, NY // CY, NZ // CZ)
    counts = jax.random.randint(key_counts, blocks, CZ // 2, CZ + 1).reshape(-1)
    chosen = jax.random.randint(key_full, (), 0, counts.shape[0])
    counts = jnp.where(jnp.arange(counts.shape[0]) == chosen, CZ, counts)
    return counts.reshape(blocks).astype(jnp.int32)


def draw_coarse_factor(key, part):
    key_diag, key_low = jax.random.split(jax.random.fold_in(key, 37))
    diagonal = jax.random.uniform(key_diag, (NB,), jnp.float32, 1.0, 2.0)
    lower = jnp.clip(jax.random.normal(key_low, (NB, NB), jnp.float32), -6.0, 6.0)
    lower = jnp.tril(lower, -1) * (0.5 / math.sqrt(NB))
    return (lower + jnp.diag(diagonal)).astype(jnp.bfloat16)


def shard_levels(rng, shape, cuts, low, top_value):
    def one(axis_at, shards_of):
        steps = jax.random.uniform(jax.random.fold_in(jax.random.fold_in(rng, 6), axis_at), (shards_of,), jnp.float32, low / len(cuts), top_value / len(cuts))
        return jnp.repeat(jnp.exp(steps), shape[axis_at] // shards_of).reshape((-1,) + (1,) * (len(shape) - axis_at - 1))

    loudness = one(*cuts[0])
    for cut in cuts[1:]:
        loudness = loudness * one(*cut)
    return loudness


def setup_inputs(seed: int = 0) -> dict:
    streams_of = jax.random.split(jax.random.key(seed), 5)
    right_side = draw_right_side(jax.random.fold_in(streams_of[4], 71), 0)
    conductance = jnp.clip(jnp.exp(math.log(4.0) - 2.7725887 * jax.random.uniform(streams_of[1], (NX, NY, NZ), jnp.float32) ** shard_levels(streams_of[1], (NX, NY, NZ), ((0, 4), (1, 2), (2, 4)), -0.2, 0.2)), 0.25, 4.0)
    extents = draw_extents(jax.random.fold_in(streams_of[4], 71), 0)
    coarse_factor = draw_coarse_factor(jax.random.fold_in(streams_of[4], 71), 0)
    return dict(right_side=right_side, conductance=conductance, extents=extents, coarse_factor=coarse_factor)


OMEGA = 0.8

def neighbour_slices():
    inner = slice(1, -1)
    return [(slice(2, None), inner, inner), (slice(None, -2), inner, inner), (inner, slice(2, None), inner), (inner, slice(None, -2), inner), (inner, inner, slice(2, None)), (inner, inner, slice(None, -2))]

def face_terms(padded, cond_padded):
    centre = (slice(1, -1), slice(1, -1), slice(1, -1))
    value_mid = padded[centre]
    cond_mid = cond_padded[centre]
    summed = jnp.zeros_like(value_mid)
    for place in neighbour_slices():
        summed = summed + 0.5 * (cond_mid + cond_padded[place]) * (value_mid - padded[place])
    return summed

def coef_total(cond_padded):
    centre = (slice(1, -1), slice(1, -1), slice(1, -1))
    cond_mid = cond_padded[centre]
    summed = jnp.zeros_like(cond_mid)
    for place in neighbour_slices():
        summed = summed + 0.5 * (cond_mid + cond_padded[place])
    return summed

def pool_sum(field):
    first, second, third = field.shape
    return field.reshape(first // 2, 2, second // 2, 2, third // 2, 2).sum(axis=(1, 3, 5))

def pool_max(field):
    first, second, third = field.shape
    return field.reshape(first // 2, 2, second // 2, 2, third // 2, 2).max(axis=(1, 3, 5))

def expand(field):
    first, second, third = field.shape
    wide = jnp.broadcast_to(field[:, None, :, None, :, None], (first, 2, second, 2, third, 2))
    return wide.reshape(2 * first, 2 * second, 2 * third)

def make_level(cond_padded, fluid, scale):
    inverse = fluid / (scale * coef_total(cond_padded) + 1.0 - fluid)
    return (cond_padded, fluid, scale, inverse)

def apply_level(field, level):
    padded = jnp.pad(field, 1)
    return level[2] * level[1] * face_terms(padded, level[0])

def cycle(resid, levels, depth):
    level = levels[depth]
    first = OMEGA * level[3] * resid
    if depth == len(levels) - 1:
        return first
    image = apply_level(first, level)
    below = cycle(pool_sum(resid - image), levels, depth + 1)
    second = first + level[1] * expand(below)
    return second + OMEGA * level[3] * (resid - apply_level(second, level))

def reference(right_side, conductance, extents, coarse_factor):
    factor = coarse_factor.astype(jnp.float32)
    layer = lax.broadcasted_iota(jnp.int32, right_side.shape, 2) % CZ
    limit = jnp.repeat(jnp.repeat(jnp.repeat(extents, CX, axis=0), CY, axis=1), CZ, axis=2)
    fluid = (layer < limit).astype(jnp.float32)
    fluid_mid = pool_max(fluid)
    cond_mid = pool_sum(conductance) / 8.0
    levels = [make_level(jnp.pad(conductance, 1), fluid, 1.0), make_level(jnp.pad(cond_mid, 1), fluid_mid, 4.0)]
    block_cells = CX * CY * CZ

    def precondition(resid):
        smoothed = cycle(resid, levels, 0)
        means = resid.reshape(N_GX, CX, N_GY, CY, N_GZ, CZ).sum(axis=(1, 3, 5)).reshape(-1) / block_cells
        coarse = jax.scipy.linalg.cho_solve((factor, True), means)
        blockwise = coarse.reshape(N_GX, N_GY, N_GZ)
        spread = jnp.repeat(jnp.repeat(jnp.repeat(blockwise, CX, axis=0), CY, axis=1), CZ, axis=2)
        return smoothed + fluid * spread
    resid = fluid * right_side
    solution = jnp.zeros_like(resid)
    precond = precondition(resid)
    inner_now = jnp.sum(resid * precond)
    direction = precond
    for step in range(ITERS):
        image = apply_level(direction, levels[0])
        alpha = inner_now / jnp.sum(direction * image)
        solution = solution + alpha * direction
        resid = resid - alpha * image
        if step + 1 < ITERS:
            precond = precondition(resid)
            inner_next = jnp.sum(resid * precond)
            direction = precond + inner_next / inner_now * direction
            inner_now = inner_next
    return (solution, resid)
```

```python
import functools

import jax
import jax.numpy as jnp
from jax import lax
from jax.experimental import pallas as pl
from jax.experimental.pallas import tpu as pltpu
from jax.sharding import PartitionSpec as P

OMEGA = 0.8
HALO = 8
GROUP = 3 * HALO
MESH = pl.DeviceIdType.MESH
HIGH = lax.Precision.HIGHEST
DIRS = [
    (dx, dy, dz)
    for dx in (-1, 0, 1)
    for dy in (-1, 0, 1)
    for dz in (-1, 0, 1)
    if (dx, dy, dz) != (0, 0, 0)
]
DIRS.sort(key=lambda d: -sum(abs(a) for a in d))


def code(dx, dy, dz):
    return (dx + 1) * 9 + (dy + 1) * 3 + dz + 1


class Edge:
    def __init__(self, bx, bz):
        self.bx, self.ex = bx, bx + 2 * HALO
        self.places = bz // GROUP
        tiles = -(-2 * self.ex // self.places)
        self.tiles = tiles + tiles % 2
        self.patterns, self.pattern_of = [], []
        for t in range(self.tiles):
            key = tuple(
                None if s is None else (self.block(s[0])[0], s[1])
                for s in (self.slab(t, j) for j in range(self.places))
            )
            if key not in self.patterns:
                self.patterns.append(key)
            self.pattern_of.append(self.patterns.index(key))

    def slab(self, t, j):
        slot = t + self.tiles * j
        return None if slot >= 2 * self.ex else (slot % self.ex, slot // self.ex)

    def place(self, s, side):
        slot = s + self.ex * side
        return slot % self.tiles, slot // self.tiles

    def block(self, s):
        if s < HALO:
            return 0, self.bx - HALO + s
        if s < HALO + self.bx:
            return 1, s - HALO
        return 2, s - HALO - self.bx


def kernel(
    counts,
    rhs_hbm,
    cond_hbm,
    ext_hbm,
    factor_hbm,
    sol_ref,
    res_ref,
    R,
    C,
    ext_ref,
    factor_ref,
    e_out,
    e_in,
    z_out,
    z_in,
    early_out,
    early,
    late_out,
    late,
    FL,
    F1,
    FX,
    FY,
    FZ,
    INV,
    C1,
    IC,
    SEC,
    D0,
    W,
    U,
    Q,
    YB,
    EY,
    send_c,
    recv_c,
    send_r,
    recv_r,
    send_e,
    recv_e,
    send_g,
    recv_g,
    load_sem,
):
    ngx, ngy, ngz = counts
    n = ngx * ngy * ngz
    ix, iy, iz = lax.axis_index("gx"), lax.axis_index("gy"), lax.axis_index("gz")
    me = (ix * ngy + iy) * ngz + iz
    bx, by, bz = sol_ref.shape
    ex, ey = bx + 2 * HALO, by + 2 * HALO
    edge = Edge(bx, bz)
    tiles = edge.tiles
    f32 = jnp.float32
    lo_x, hi_x = HALO, HALO + bx

    def turned(at, step, count):
        moved = at + step
        return jnp.where(moved >= count, moved - count, moved)

    def everyone(act):
        if n <= 64:
            xs = [turned(ix, t, ngx) for t in range(ngx)]
            ys = [turned(iy, t, ngy) for t in range(ngy)]
            zs = [turned(iz, t, ngz) for t in range(ngz)]
            steps = [(a, b, c) for a in range(ngx) for b in range(ngy) for c in range(ngz)]
            steps.sort(
                key=lambda t: -sum(min(a, m - a) for a, m in zip(t, (ngx, ngy, ngz)))
            )
            for a, b, c in steps[:-1]:
                act((xs[a], ys[b], zs[c]))
        else:

            def one(t, carry):
                flat = (me + t) % n
                act((flat // (ngy * ngz), (flat // ngz) % ngy, flat % ngz))
                return carry

            lax.fori_loop(1, n, one, 0)

    core_x, core_y = pl.ds(lo_x, bx), pl.ds(0, by)
    loads = [
        pltpu.make_async_copy(src, dst, load_sem.at[k])
        for k, (src, dst) in enumerate(
            (
                (rhs_hbm, R.at[core_x, core_y]),
                (cond_hbm, C.at[core_x, core_y]),
                (ext_hbm, ext_ref),
                (factor_hbm, factor_ref),
            )
        )
    ]
    for load in loads:
        load.start()

    barrier = pltpu.get_barrier_semaphore()
    everyone(
        lambda device: pl.semaphore_signal(
            barrier, inc=1, device_id=device, device_id_type=MESH
        )
    )

    def inside(d):
        ok = None
        for at, step, count in zip((ix, iy, iz), d, counts):
            if step == 0:
                continue
            here = (at + step >= 0) & (at + step < count)
            ok = here if ok is None else ok & here
        return ok

    def x_from(dx):
        return pl.ds(bx, HALO) if dx == 1 else pl.ds(HALO, bx if dx == 0 else HALO)

    def x_into(dx):
        if dx == 0:
            return pl.ds(HALO, bx)
        return pl.ds(0, HALO) if dx == 1 else pl.ds(hi_x, HALO)

    def y_from(dy):
        return pl.ds(by - HALO, HALO) if dy == 1 else pl.ds(0, by if dy == 0 else HALO)

    def y_into(dy):
        if dy == 0:
            return pl.ds(0, by)
        return pl.ds(by + HALO, HALO) if dy == 1 else pl.ds(by, HALO)

    def landing(f, d):
        dx, dy, dz = d
        if dz != 0:
            return z_in.at[f, 1 if dz == 1 else 0, 1 - dx, y_into(dy)]
        return (R, C)[f].at[x_into(dx), y_into(dy)]

    def remote(src, dst, send, recv, d):
        return pltpu.make_async_remote_copy(
            src_ref=src,
            dst_ref=dst,
            send_sem=send,
            recv_sem=recv,
            device_id=(ix + d[0], iy + d[1], iz + d[2]),
            device_id_type=MESH,
        )

    def copies(f, d):
        dx, dy, dz = d
        k = code(*d)
        if dz != 0:
            src = z_out.at[f, y_from(dy)]
        else:
            src = (R, C)[f].at[x_from(dx), y_from(dy)]
        send, recv = ((send_r, recv_r), (send_c, recv_c))[f]
        out = [remote(src, landing(f, d), send.at[k], recv.at[k], d)]
        if f == 1:
            out.append(remote(e_out, e_in.at[code(-dx, -dy, -dz)], send_e.at[k], recv_e.at[k], d))
        return out

    def start_all(f):
        for d in DIRS:

            @pl.when(inside(d))
            def _():
                for c in copies(f, d):
                    c.start()

    def wait_all(f):
        for d in DIRS:

            @pl.when(inside(tuple(-a for a in d)))
            def _():
                for c in copies(f, d):
                    c.wait_recv()

    def wait_sent(f):
        for d in DIRS:

            @pl.when(inside(d))
            def _():
                for c in copies(f, d):
                    c.wait_send()

    for d in DIRS:

        @pl.when(jnp.logical_not(inside(tuple(-a for a in d))))
        def _():
            for f in (0, 1):
                ref = landing(f, d)
                ref[...] = jnp.zeros(ref.shape, f32)
            e_in[code(*(-a for a in d))] = jnp.zeros((1, bz), f32)

    lane = lax.broadcasted_iota(jnp.int32, (ey, bz), 1)
    row = lax.broadcasted_iota(jnp.int32, (ey, bz), 0)
    odd_lane, odd_row = lane % 2 == 1, row % 2 == 1
    lane_y = lane[:by]

    def up_y(v, k=1):
        return pltpu.roll(v, k, 0)

    def dn_y(v, k=1):
        return pltpu.roll(v, ey - k, 0)

    def spin(v, k):
        k = k % bz
        return v if k == 0 else pltpu.roll(v, k, 1)

    def up_z(v, k=1):
        return pltpu.roll(v, k, 1)

    def dn_z(v, k=1):
        return pltpu.roll(v, bz - k, 1)

    for load in loads[:3]:
        load.wait()
    own_limit = ext_ref[0].astype(f32)
    e_out[...] = jnp.broadcast_to(own_limit, (1, bz))
    for f, field in ((1, C), (0, R)):
        packed = jnp.zeros((by, bz), f32)
        for k in range(bx):
            moved = spin(field[lo_x + k, :by], 2 * HALO * k + HALO)
            packed = jnp.where(lane_y // (2 * HALO) == k, moved, packed)
        z_out[f] = packed

    def total(v):
        return jnp.sum(v, axis=(0, 1), keepdims=True)

    acc = R[lo_x, :by]
    for k in range(1, bx):
        acc = acc + R[lo_x + k, :by]
    m0 = total(jnp.where(lane_y.astype(f32) < own_limit, acc, 0.0))
    early_row = jnp.broadcast_to(m0, (1, bz))
    early_out[...] = early_row
    early[pl.ds(me, 1)] = early_row[None]

    def remote_row(out, into, base, device):
        return pltpu.make_async_remote_copy(
            src_ref=out,
            dst_ref=into.at[me],
            send_sem=send_g.at[base],
            recv_sem=recv_g.at[base],
            device_id=device,
            device_id_type=MESH,
        )

    def spread(out, into, base):
        everyone(lambda device: remote_row(out, into, base, device).start())

    def collect(into, base):
        part = into.at[pl.ds(0, n - 1)]
        pltpu.make_async_copy(part, part, recv_g.at[base]).wait()
        pltpu.make_async_copy(part, part, send_g.at[base]).wait()

    pl.semaphore_wait(barrier, n - 1)
    start_all(1)
    spread(early_out, early, 0)
    start_all(0)

    loads[3].wait()
    L = factor_ref[...].astype(f32)
    ri = lax.broadcasted_iota(jnp.int32, (n, n), 0)
    ci = lax.broadcasted_iota(jnp.int32, (n, n), 1)
    eye = ri == ci
    X = jnp.where(eye, 1.0 / jnp.where(eye, L, 1.0), 0.0)
    s = 1
    while s < n:
        pick = (ri // (2 * s) == ci // (2 * s)) & (ri % (2 * s) >= s) & (ci % (2 * s) < s)
        low = jnp.where(pick, L, 0.0)
        X = X - jnp.dot(
            X,
            jnp.dot(low, X, precision=HIGH, preferred_element_type=f32),
            precision=HIGH,
            preferred_element_type=f32,
        )
        s *= 2
    inverse = lax.dot_general(
        X, X, (((0,), (0,)), ((), ())), precision=HIGH, preferred_element_type=f32
    )

    one_lane = lax.broadcasted_iota(jnp.int32, (1, bz), 1)
    bands = ((0, by), (1, HALO), (-1, HALO))

    def tables(value):
        rows = {
            (dx, dy, dz): value(dx, dy, dz)
            for dx in (-1, 0, 1)
            for dy in (-1, 0, 1)
            for dz in (-1, 0, 1)
        }
        out = [
            jnp.concatenate(
                [jnp.broadcast_to(rows[dx, dy, 0], (count, bz)) for dy, count in bands], axis=0
            )
            for dx in (-1, 0, 1)
        ]
        for pattern in edge.patterns:
            parts = []
            for dy, count in bands:
                line = None
                for j, key in enumerate(pattern):
                    if key is None:
                        continue
                    dx, start = key[0] - 1, GROUP * j
                    if key[1] == 0:
                        here = jnp.where(
                            one_lane < start + HALO, rows[dx, dy, -1], rows[dx, dy, 0]
                        )
                    else:
                        here = jnp.where(
                            one_lane < start + 2 * HALO, rows[dx, dy, 0], rows[dx, dy, 1]
                        )
                    line = here if line is None else jnp.where(one_lane >= start, here, line)
                parts.append(jnp.broadcast_to(line, (count, bz)))
            out.append(jnp.concatenate(parts, axis=0))
        return out

    def depths():
        plain = one_lane
        out = [plain] * 3
        for pattern in edge.patterns:
            line = None
            for j, key in enumerate(pattern):
                off = one_lane - GROUP * j
                if key is None:
                    here = jnp.full((1, bz), bz, jnp.int32)
                elif key[1] == 0:
                    here = jnp.where(off < HALO, off + bz - HALO, off - HALO)
                else:
                    here = jnp.where(off < 2 * HALO, off + bz - 2 * HALO, off - 2 * HALO)
                line = here if line is None else jnp.where(off >= 0, here, line)
            line = jnp.where(one_lane >= GROUP * edge.places, bz, line)
            out.append(line)
        return out

    def flag_of(i):
        return edge.block(i)[0] if i < ex else 3 + edge.pattern_of[i - ex]

    def build_edges(f, field):
        for t in range(tiles):
            acc = None
            for j in range(edge.places):
                slab = edge.slab(t, j)
                start = GROUP * j
                if slab is None:
                    acc = jnp.where(lane >= start, 0.0, acc)
                    break
                s, side = slab
                which, k = edge.block(s)
                at = 2 * HALO * k
                if side == 0:
                    own = spin(field[s], start + HALO)
                    far = spin(z_in[f, 1, which], start - at)
                    here = jnp.where(lane < start + HALO, far, own)
                else:
                    own = spin(field[s], start + 2 * HALO - bz)
                    far = spin(z_in[f, 0, which], start + HALO - at)
                    here = jnp.where(lane < start + 2 * HALO, own, far)
                acc = here if acc is None else jnp.where(lane >= start, here, acc)
            field[ex + t] = jnp.where(lane < GROUP * edge.places, acc, 0.0)

    def pool_yz(v):
        v = v + jnp.where(odd_row, up_y(v), dn_y(v))
        return v + jnp.where(odd_lane, up_z(v), dn_z(v))

    def walk(load, ref, lo, hi, emit):
        def one(i, v, gx, gx_next):
            gy = FY[i] * (v - up_y(v))
            gz = FZ[i] * (v - up_z(v))
            emit(i, v, (gx - gx_next) + ((gy - dn_y(gy)) + (gz - dn_z(gz))))

        before, v = load(lo - 1), load(lo)
        gx = ref[lo] * (v - before)
        for i in range(lo, hi):
            after = load(i + 1)
            gx_next = ref[i + 1] * (after - v)
            one(i, v, gx, gx_next)
            v, gx = after, gx_next
        before, v = spin(load(ex + tiles - 1), GROUP), load(ex)
        first = gx = ref[ex] * (v - before)
        for t in range(tiles):
            i = ex + t
            if t < tiles - 1:
                after = load(i + 1)
                gx_next = ref[i + 1] * (after - v)
            else:
                after, gx_next = None, spin(first, -GROUP)
            one(i, v, gx, gx_next)
            v, gx = after, gx_next

    wait_all(1)

    def limit(dx, dy, dz):
        return e_out[...] if (dx, dy, dz) == (0, 0, 0) else e_in[code(dx, dy, dz)]

    for k, (a, z) in enumerate(zip(tables(limit), depths())):
        z_f, even_f = z.astype(f32), (z - z % 2).astype(f32)
        FL[k] = (z_f < a).astype(f32)
        F1[k] = (even_f < a).astype(f32)

    build_edges(1, C)
    every = list(range(ex)) + list(range(ex, ex + tiles))
    for i in every:
        c = C[i]
        if i != 0:
            before = spin(C[ex + tiles - 1], GROUP) if i == ex else C[i - 1]
            FX[i] = 0.5 * (before + c)
        FY[i] = 0.5 * (c + up_y(c))
        FZ[i] = 0.5 * (c + up_z(c))
    for i in list(range(1, ex - 1)) + list(range(ex, ex + tiles)):
        fy, fz = FY[i], FZ[i]
        after = spin(FX[ex], -GROUP) if i == ex + tiles - 1 else FX[i + 1]
        diagonal = (FX[i] + after) + (fy + dn_y(fy)) + (fz + dn_z(fz))
        fl = FL[flag_of(i)]
        INV[i] = OMEGA * fl / (diagonal + 1.0 - fl)
    pairs, edge_pairs = ex // 2, tiles // 2
    for q in range(pairs + edge_pairs):
        C1[q] = pool_yz(C[2 * q] + C[2 * q + 1]) * 0.125
    for q in list(range(1, pairs - 1)) + list(range(pairs, pairs + edge_pairs)):
        c = C1[q]
        before = spin(C1[pairs + edge_pairs - 1], GROUP) if q == pairs else C1[q - 1]
        after = spin(C1[pairs], -GROUP) if q == pairs + edge_pairs - 1 else C1[q + 1]
        diagonal = 3.0 * c + 0.5 * (
            (before + after) + (up_y(c, 2) + dn_y(c, 2)) + (up_z(c, 2) + dn_z(c, 2))
        )
        fl = F1[flag_of(2 * q)]
        IC[q] = OMEGA * fl / (4.0 * diagonal + 1.0 - fl)

    off = lane_y % GROUP
    slot0 = (lane_y // GROUP) * tiles

    def core_edge(t, lo_off, hi_off):
        slot = slot0 + t
        low = (slot >= lo_x) & (slot < hi_x) & lo_off
        high = (slot >= ex + lo_x) & (slot < ex + hi_x) & hi_off
        return (low | high) & (lane_y < GROUP * edge.places)

    core_off = (off >= HALO) & (off < 2 * HALO)
    core_tiles = [core_edge(t, core_off, core_off) for t in range(tiles)]
    core_lanes = (lane_y >= HALO) & (lane_y < bz - HALO)

    flux_z = FZ[lo_x, :by]
    flux_y = FY[lo_x]
    for i in range(lo_x + 1, hi_x):
        flux_z = flux_z + FZ[i, :by]
        flux_y = flux_y + FY[i]
    fl = FL[1]
    fl_up, fl_core = up_y(fl), fl[:by]
    step = fl_core - up_z(fl)[:by]
    inner = jnp.where(lane_y >= 1, flux_z * (step * step), 0.0)
    none = jnp.logical_and(off < 0, off >= 0)
    low_face = [core_edge(t, off == HALO, none) for t in range(tiles)]
    high_face = [core_edge(t, none, off == 2 * HALO) for t in range(tiles)]
    sides = {}

    def put(d, alone, shared):
        sides[d] = (total(alone), total(shared))

    alone = FX[lo_x, :by] * fl_core
    put((-1, 0, 0), alone, alone * FL[0, :by])
    alone = FX[hi_x, :by] * fl_core
    put((1, 0, 0), alone, alone * FL[2, :by])
    alone = jnp.where(row == 0, flux_y * fl, 0.0)
    put((0, -1, 0), alone, alone * fl_up)
    alone = jnp.where(row == by, flux_y * fl_up, 0.0)
    put((0, 1, 0), alone, alone * fl)
    zeros = jnp.zeros((by, bz), f32)
    parts = [zeros] * 4
    for t in range(tiles):
        f_edge = FL[3 + edge.pattern_of[t]]
        f_here, f_up = f_edge[:by], up_z(f_edge)[:by]
        fz = FZ[ex + t, :by]
        a = jnp.where(low_face[t], fz * f_here, 0.0)
        b = jnp.where(high_face[t], fz * f_up, 0.0)
        parts = [parts[0] + a, parts[1] + a * f_up, parts[2] + b, parts[3] + b * f_here]
    put((0, 0, -1), parts[0], parts[1])
    put((0, 0, 1), parts[2], parts[3])

    scalars = 8
    width = late.shape[-1]
    base = scalars if width == bz else bz
    col = lax.broadcasted_iota(jnp.int32, (1, width), 1)
    diagonal = total(inner)
    late_row = jnp.zeros((1, width), f32)
    for (dx, dy, dz), (alone, shared) in sides.items():
        diagonal = diagonal + alone
        other = ((ix + dx) * ngy + iy + dy) * ngz + iz + dz
        valid = inside((dx, dy, dz))
        late_row = late_row - jnp.where((col == base + other) & valid, shared, 0.0)
    late_row = late_row + jnp.where(col == base + me, diagonal, 0.0)

    wait_all(0)
    build_edges(0, R)

    def sized(lo, hi):
        return list(range(lo, hi)) + list(range(ex, ex + tiles))

    def cycle(field, lo, hi, finish):
        even = (lo - 1) // 2 * 2
        stop = (hi + 2) // 2 * 2
        held = {}

        def first(i):
            return INV[i] * field[i]

        def coarse(i, v, lv):
            gap = FL[flag_of(i)] * (field[i] - lv)
            if i % 2 == 0:
                held[0] = (v, gap)
                return
            below = IC[i // 2] * pool_yz(held[0][1] + gap)
            for at, w in ((i - 1, held[0][0]), (i, v)):
                SEC[at] = w + FL[flag_of(at)] * below

        walk(first, FX, even, stop, coarse)
        walk(
            lambda i: SEC[i],
            FX,
            lo,
            hi,
            lambda i, v, lv: finish(i, v + INV[i] * (field[i] - lv)),
        )

    def solve(means):
        y_row = jnp.sum(inverse * means, axis=0, keepdims=True)
        y_col = jnp.sum(jnp.where(eye, y_row, 0.0), axis=1, keepdims=True)
        return y_row, y_col

    def block_row(dx, dy, dz):
        def near(at, step, count):
            return jnp.clip(at + step, 0, count - 1)

        b = (near(ix, dx, ngx) * ngy + near(iy, dy, ngy)) * ngz + near(iz, dz, ngz)
        return YB[pl.ds(b, 1)]

    def spread_blocks(y_col):
        YB[...] = jnp.broadcast_to(y_col, (n, bz))
        for k, v in enumerate(tables(block_row)):
            EY[k] = FL[k] * v

    cells = bx * by * bz
    collect(early, 0)
    m0_col = early[:, 0, 0:1]
    _, y_col = solve(m0_col * (1.0 / cells))
    spread_blocks(y_col)

    def keep_direction(i, v):
        D0[i] = v + EY[flag_of(i)]

    cycle(R, 4, ex - 4, keep_direction)

    sums = [[zeros, zeros] for _ in range(7)]

    def add(i, k, v):
        if i < ex:
            if lo_x <= i < hi_x:
                sums[k][0] = sums[k][0] + v()
        else:
            sums[k][1] = sums[k][1] + jnp.where(core_tiles[i - ex], v(), 0.0)

    def keep_image(i, v, lv):
        w = FL[flag_of(i)] * lv
        W[i] = w
        add(i, 0, lambda: R[i, :by] * v[:by])
        add(i, 1, lambda: w[:by] * v[:by])
        add(i, 2, lambda: w[:by])

    walk(lambda i: D0[i], FX, 5, ex - 5, keep_image)

    def keep_second(i, v):
        U[i] = v
        add(i, 3, lambda: W[i, :by] * v[:by])
        add(i, 4, lambda: R[i, :by] * v[:by])

    cycle(W, 7, ex - 7, keep_second)

    def keep_third(i, v, lv):
        q = FL[flag_of(i)] * lv
        Q[i] = q
        add(i, 5, lambda: q[:by] * v[:by])
        add(i, 6, lambda: q[:by])

    walk(lambda i: U[i], FX, lo_x, hi_x, keep_third)

    for k, (a, b) in enumerate(sums):
        part = total(jnp.where(core_lanes, a, 0.0) + b)
        late_row = jnp.where(col == k, part, late_row)
    late_out[...] = late_row
    late[pl.ds(me, 1)] = late_row[None]
    spread(late_out, late, 1)
    collect(late, 1)

    rows = late[:, 0, :]
    y_row, y_col = solve(rows[:, 2:3] * (1.0 / cells))
    spread_blocks(y_col)
    plain = jnp.sum(rows, axis=0, keepdims=True)
    weighted = jnp.sum(rows * y_col, axis=0, keepdims=True)

    def pick(line, k):
        return jnp.sum(line[:, k : k + 1], axis=(0, 1), keepdims=True)

    rz, dad = pick(plain, 0), pick(plain, 1)
    y_m0 = total(m0_col * y_col)
    w_u = pick(plain, 3) + pick(weighted, 2)
    r_u = pick(plain, 4) + y_m0
    u_q = (
        pick(plain, 5)
        + 2.0 * pick(weighted, 6)
        + total(weighted[:, base : base + n] * y_row)
    )
    alpha = rz / dad
    new = (rz - alpha * dad) + alpha * (alpha * w_u - r_u)
    beta = new / rz
    grow = 1.0 + beta
    dad1 = grow * grow * dad - 2.0 * alpha * grow * w_u + alpha * alpha * u_q
    alpha1 = new / dad1
    c1 = alpha + alpha1 * grow
    c2 = alpha * alpha1

    edges = {}

    def results(i, v, lv):
        fl = FL[flag_of(i)][:by]
        sol = c1 * D0[i, :by] - c2 * (U[i, :by] + v[:by])
        res = fl * R[i, :by] - c1 * W[i, :by] + c2 * (Q[i, :by] + fl * lv[:by])
        if i < ex:
            sol_ref[i - lo_x], res_ref[i - lo_x] = sol, res
        else:
            SEC[i, :by], D0[i, :by] = sol, res

    walk(lambda i: EY[flag_of(i)], FX, lo_x, hi_x, results)
    for x in range(bx):
        tl, jl = edge.place(lo_x + x, 0)
        th, jh = edge.place(lo_x + x, 1)
        for ref, held in ((sol_ref, SEC), (res_ref, D0)):
            low = spin(held[ex + tl, :by], -(GROUP * jl + HALO))
            high = spin(held[ex + th, :by], bz - HALO - (GROUP * jh + HALO))
            ref[x] = jnp.where(
                lane_y < HALO, low, jnp.where(lane_y >= bz - HALO, high, ref[x])
            )
    wait_sent(1)
    wait_sent(0)


def solution(mesh):
    counts = (mesh.shape["gx"], mesh.shape["gy"], mesh.shape["gz"])
    n = counts[0] * counts[1] * counts[2]

    def on_device(right_side, conductance, extents, coarse_factor):
        f32 = jnp.float32
        bx, by, bz = right_side.shape
        ex, ey = bx + 2 * HALO, by + 2 * HALO
        edge = Edge(bx, bz)
        slabs = ex + edge.tiles
        width = bz if n + 8 <= bz else bz + -(-n // 128) * 128
        vm = lambda *shape: pltpu.VMEM(shape, f32)
        field = vm(slabs, ey, bz)
        half = vm(slabs // 2, ey, bz)
        flags = vm(3 + len(edge.patterns), ey, bz)
        dma = pltpu.SemaphoreType.DMA
        scratch = [
            field,
            field,
            pltpu.VMEM(extents.shape, extents.dtype),
            pltpu.VMEM(coarse_factor.shape, coarse_factor.dtype),
            vm(1, bz),
            vm(27, 1, bz),
            vm(2, by, bz),
            vm(2, 2, 3, ey, bz),
            vm(1, bz),
            vm(n, 1, bz),
            vm(1, width),
            vm(n, 1, width),
            flags,
            flags,
            field,
            field,
            field,
            field,
            half,
            half,
            field,
            field,
            field,
            field,
            field,
            vm(n, bz),
            flags,
            dma((27,)),
            dma((27,)),
            dma((27,)),
            dma((27,)),
            dma((27,)),
            dma((27,)),
            dma((2,)),
            dma((2,)),
            dma((4,)),
        ]
        block = vm(bx, by, bz)
        whole = pl.BlockSpec(memory_space=pltpu.VMEM)
        outer = pl.BlockSpec(memory_space=pltpu.HBM)
        return pl.pallas_call(
            functools.partial(kernel, counts),
            out_shape=(block, block),
            in_specs=[outer, outer, outer, outer],
            out_specs=(whole, whole),
            scratch_shapes=scratch,
            compiler_params=pltpu.CompilerParams(
                collective_id=0, has_side_effects=True, vmem_limit_bytes=60000000
            ),
        )(right_side, conductance, extents, coarse_factor)

    in_specs = (P("gx", "gy", "gz"), P("gx", "gy", "gz"), P("gx", "gy", "gz"), P())
    out_specs = (P("gx", "gy", "gz"), P("gx", "gy", "gz"))
    return jax.shard_map(
        on_device, mesh=mesh, in_specs=in_specs, out_specs=out_specs, check_vma=False
    )
```

```python
import functools

import jax
import jax.numpy as jnp
from jax import lax
from jax.experimental import pallas as pl
from jax.experimental.pallas import tpu as pltpu
from jax.sharding import PartitionSpec as P

OMEGA = 0.8
HALO = 8
GROUP = 3 * HALO
SPAN = 16
MESH = pl.DeviceIdType.MESH
HIGH = lax.Precision.HIGHEST
DIRS = [
    (dx, dy, dz)
    for dx in (-1, 0, 1)
    for dy in (-1, 0, 1)
    for dz in (-1, 0, 1)
    if (dx, dy, dz) != (0, 0, 0)
]
DIRS.sort(key=lambda d: -sum(abs(a) for a in d))


def code(dx, dy, dz):
    return (dx + 1) * 9 + (dy + 1) * 3 + dz + 1


class Edge:
    def __init__(self, bx, bz):
        self.bx, self.ex = bx, bx + 2 * HALO
        self.places = bz // GROUP
        tiles = -(-2 * self.ex // self.places)
        self.tiles = tiles + tiles % 2
        self.patterns, self.pattern_of = [], []
        for t in range(self.tiles):
            key = tuple(
                None if s is None else (self.block(s[0])[0], s[1])
                for s in (self.slab(t, j) for j in range(self.places))
            )
            if key not in self.patterns:
                self.patterns.append(key)
            self.pattern_of.append(self.patterns.index(key))

    def slab(self, t, j):
        slot = t + self.tiles * j
        return None if slot >= 2 * self.ex else (slot % self.ex, slot // self.ex)

    def place(self, s, side):
        slot = s + self.ex * side
        return slot % self.tiles, slot // self.tiles

    def block(self, s):
        if s < HALO:
            return 0, self.bx - HALO + s
        if s < HALO + self.bx:
            return 1, s - HALO
        return 2, s - HALO - self.bx


def kernel(
    counts,
    rhs_hbm,
    cond_hbm,
    ext_hbm,
    factor_hbm,
    sol_ref,
    res_ref,
    R,
    C,
    ext_ref,
    factor_ref,
    e_out,
    e_in,
    z_out,
    z_in,
    early_out,
    early,
    late_out,
    late,
    FL,
    F1,
    FX,
    FY,
    FZ,
    INV,
    C1,
    IC,
    SEC,
    D0,
    W,
    U,
    Q,
    YB,
    EY,
    send_c,
    recv_c,
    send_r,
    recv_r,
    send_e,
    recv_e,
    send_g,
    recv_g,
    load_sem,
):
    ngx, ngy, ngz = counts
    n = ngx * ngy * ngz
    ix, iy, iz = lax.axis_index("gx"), lax.axis_index("gy"), lax.axis_index("gz")
    me = (ix * ngy + iy) * ngz + iz
    bx, by, bz = sol_ref.shape
    ex, ey = bx + 2 * HALO, by + 2 * HALO
    edge = Edge(bx, bz)
    tiles = edge.tiles
    f32 = jnp.float32
    lo_x, hi_x = HALO, HALO + bx

    def turned(at, step, count):
        moved = at + step
        return jnp.where(moved >= count, moved - count, moved)

    def everyone(act):
        if n <= 64:
            xs = [turned(ix, t, ngx) for t in range(ngx)]
            ys = [turned(iy, t, ngy) for t in range(ngy)]
            zs = [turned(iz, t, ngz) for t in range(ngz)]
            steps = [(a, b, c) for a in range(ngx) for b in range(ngy) for c in range(ngz)]
            steps.sort(
                key=lambda t: -sum(min(a, m - a) for a, m in zip(t, (ngx, ngy, ngz)))
            )
            for a, b, c in steps[:-1]:
                act((xs[a], ys[b], zs[c]))
        else:

            def one(t, carry):
                flat = (me + t) % n
                act((flat // (ngy * ngz), (flat // ngz) % ngy, flat % ngz))
                return carry

            lax.fori_loop(1, n, one, 0)

    core_x, core_y = pl.ds(lo_x, bx), pl.ds(0, by)
    loads = [
        pltpu.make_async_copy(src, dst, load_sem.at[k])
        for k, (src, dst) in enumerate(
            (
                (rhs_hbm, R.at[core_x, core_y]),
                (cond_hbm, C.at[core_x, core_y]),
                (ext_hbm, ext_ref),
                (factor_hbm, factor_ref),
            )
        )
    ]
    for load in loads:
        load.start()

    barrier = pltpu.get_barrier_semaphore()
    everyone(
        lambda device: pl.semaphore_signal(
            barrier, inc=1, device_id=device, device_id_type=MESH
        )
    )

    def inside(d):
        ok = None
        for at, step, count in zip((ix, iy, iz), d, counts):
            if step == 0:
                continue
            here = (at + step >= 0) & (at + step < count)
            ok = here if ok is None else ok & here
        return ok

    def x_from(dx):
        return pl.ds(bx, HALO) if dx == 1 else pl.ds(HALO, bx if dx == 0 else HALO)

    def x_into(dx):
        if dx == 0:
            return pl.ds(HALO, bx)
        return pl.ds(0, HALO) if dx == 1 else pl.ds(hi_x, HALO)

    def y_from(dy):
        return pl.ds(by - HALO, HALO) if dy == 1 else pl.ds(0, by if dy == 0 else HALO)

    def y_into(dy):
        if dy == 0:
            return pl.ds(0, by)
        return pl.ds(by + HALO, HALO) if dy == 1 else pl.ds(by, HALO)

    def landing(f, d):
        dx, dy, dz = d
        if dz != 0:
            return z_in.at[f, 1 if dz == 1 else 0, 1 - dx, y_into(dy)]
        return (R, C)[f].at[x_into(dx), y_into(dy)]

    def remote(src, dst, send, recv, d):
        return pltpu.make_async_remote_copy(
            src_ref=src,
            dst_ref=dst,
            send_sem=send,
            recv_sem=recv,
            device_id=(ix + d[0], iy + d[1], iz + d[2]),
            device_id_type=MESH,
        )

    def copies(f, d):
        dx, dy, dz = d
        k = code(*d)
        if dz != 0:
            src = z_out.at[f, y_from(dy)]
        else:
            src = (R, C)[f].at[x_from(dx), y_from(dy)]
        send, recv = ((send_r, recv_r), (send_c, recv_c))[f]
        out = [remote(src, landing(f, d), send.at[k], recv.at[k], d)]
        if f == 1:
            out.append(remote(e_out, e_in.at[code(-dx, -dy, -dz)], send_e.at[k], recv_e.at[k], d))
        return out

    def start_all(f):
        for d in DIRS:

            @pl.when(inside(d))
            def _():
                for c in copies(f, d):
                    c.start()

    def wait_all(f):
        for d in DIRS:

            @pl.when(inside(tuple(-a for a in d)))
            def _():
                for c in copies(f, d):
                    c.wait_recv()

    def wait_sent(f):
        for d in DIRS:

            @pl.when(inside(d))
            def _():
                for c in copies(f, d):
                    c.wait_send()

    for d in DIRS:

        @pl.when(jnp.logical_not(inside(tuple(-a for a in d))))
        def _():
            for f in (0, 1):
                ref = landing(f, d)
                ref[...] = jnp.zeros(ref.shape, f32)
            e_in[code(*(-a for a in d))] = jnp.zeros((1, bz), f32)

    lane = lax.broadcasted_iota(jnp.int32, (ey, bz), 1)
    row = lax.broadcasted_iota(jnp.int32, (ey, bz), 0)
    odd_lane, odd_row = lane % 2 == 1, row % 2 == 1
    lane_y = lane[:by]

    def up_y(v, k=1):
        return pltpu.roll(v, k, 0)

    def dn_y(v, k=1):
        return pltpu.roll(v, ey - k, 0)

    def spin(v, k):
        k = k % bz
        return v if k == 0 else pltpu.roll(v, k, 1)

    def up_z(v, k=1):
        return pltpu.roll(v, k, 1)

    def dn_z(v, k=1):
        return pltpu.roll(v, bz - k, 1)

    for load in loads[:3]:
        load.wait()
    own_limit = ext_ref[0].astype(f32)
    e_out[...] = jnp.broadcast_to(own_limit, (1, bz))
    for f, field in ((1, C), (0, R)):
        packed = jnp.zeros((by, bz), f32)
        for k in range(bx):
            moved = spin(field[lo_x + k, :by], 2 * HALO * k + HALO)
            packed = jnp.where(lane_y // (2 * HALO) == k, moved, packed)
        z_out[f] = packed

    def total(v):
        return jnp.sum(v, axis=(0, 1), keepdims=True)

    acc = R[lo_x, :by]
    for k in range(1, bx):
        acc = acc + R[lo_x + k, :by]
    m0 = total(jnp.where(lane_y.astype(f32) < own_limit, acc, 0.0))
    early_row = jnp.broadcast_to(m0, (1, bz))
    early_out[...] = early_row
    early[pl.ds(me, 1)] = early_row[None]

    def remote_row(out, into, base, device):
        return pltpu.make_async_remote_copy(
            src_ref=out,
            dst_ref=into.at[me],
            send_sem=send_g.at[base],
            recv_sem=recv_g.at[base],
            device_id=device,
            device_id_type=MESH,
        )

    def spread(out, into, base):
        everyone(lambda device: remote_row(out, into, base, device).start())

    def collect(into, base):
        part = into.at[pl.ds(0, n - 1)]
        pltpu.make_async_copy(part, part, recv_g.at[base]).wait()
        pltpu.make_async_copy(part, part, send_g.at[base]).wait()

    pl.semaphore_wait(barrier, n - 1)
    start_all(1)
    spread(early_out, early, 0)
    start_all(0)

    loads[3].wait()
    L = factor_ref[...].astype(f32)
    ri = lax.broadcasted_iota(jnp.int32, (n, n), 0)
    ci = lax.broadcasted_iota(jnp.int32, (n, n), 1)
    eye = ri == ci
    X = jnp.where(eye, 1.0 / jnp.where(eye, L, 1.0), 0.0)
    s = 1
    while s < n:
        pick = (ri // (2 * s) == ci // (2 * s)) & (ri % (2 * s) >= s) & (ci % (2 * s) < s)
        low = jnp.where(pick, L, 0.0)
        X = X - jnp.dot(
            X,
            jnp.dot(low, X, precision=HIGH, preferred_element_type=f32),
            precision=HIGH,
            preferred_element_type=f32,
        )
        s *= 2
    inverse = lax.dot_general(
        X, X, (((0,), (0,)), ((), ())), precision=HIGH, preferred_element_type=f32
    )

    one_lane = lax.broadcasted_iota(jnp.int32, (1, bz), 1)
    bands = ((0, by), (1, HALO), (-1, HALO))

    def tables(value):
        rows = {
            (dx, dy, dz): value(dx, dy, dz)
            for dx in (-1, 0, 1)
            for dy in (-1, 0, 1)
            for dz in (-1, 0, 1)
        }
        out = [
            jnp.concatenate(
                [jnp.broadcast_to(rows[dx, dy, 0], (count, bz)) for dy, count in bands], axis=0
            )
            for dx in (-1, 0, 1)
        ]
        for pattern in edge.patterns:
            parts = []
            for dy, count in bands:
                line = None
                for j, key in enumerate(pattern):
                    if key is None:
                        continue
                    dx, start = key[0] - 1, GROUP * j
                    if key[1] == 0:
                        here = jnp.where(
                            one_lane < start + HALO, rows[dx, dy, -1], rows[dx, dy, 0]
                        )
                    else:
                        here = jnp.where(
                            one_lane < start + 2 * HALO, rows[dx, dy, 0], rows[dx, dy, 1]
                        )
                    line = here if line is None else jnp.where(one_lane >= start, here, line)
                parts.append(jnp.broadcast_to(line, (count, bz)))
            out.append(jnp.concatenate(parts, axis=0))
        return out

    def depths():
        plain = one_lane
        out = [plain] * 3
        for pattern in edge.patterns:
            line = None
            for j, key in enumerate(pattern):
                off = one_lane - GROUP * j
                if key is None:
                    here = jnp.full((1, bz), bz, jnp.int32)
                elif key[1] == 0:
                    here = jnp.where(off < HALO, off + bz - HALO, off - HALO)
                else:
                    here = jnp.where(off < 2 * HALO, off + bz - 2 * HALO, off - 2 * HALO)
                line = here if line is None else jnp.where(off >= 0, here, line)
            line = jnp.where(one_lane >= GROUP * edge.places, bz, line)
            out.append(line)
        return out

    def flag_of(i):
        return edge.block(i)[0] if i < ex else 3 + edge.pattern_of[i - ex]

    def build_edges(f, field):
        for t in range(tiles):
            acc = None
            for j in range(edge.places):
                slab = edge.slab(t, j)
                start = GROUP * j
                if slab is None:
                    acc = jnp.where(lane >= start, 0.0, acc)
                    break
                s, side = slab
                which, k = edge.block(s)
                at = 2 * HALO * k
                if side == 0:
                    own = spin(field[s], start + HALO)
                    far = spin(z_in[f, 1, which], start - at)
                    here = jnp.where(lane < start + HALO, far, own)
                else:
                    own = spin(field[s], start + 2 * HALO - bz)
                    far = spin(z_in[f, 0, which], start + HALO - at)
                    here = jnp.where(lane < start + 2 * HALO, own, far)
                acc = here if acc is None else jnp.where(lane >= start, here, acc)
            field[ex + t] = jnp.where(lane < GROUP * edge.places, acc, 0.0)

    def pool_yz(v):
        v = v + jnp.where(odd_row, up_y(v), dn_y(v))
        return v + jnp.where(odd_lane, up_z(v), dn_z(v))

    def groups(lo, hi):
        out = []
        for a, b in ((lo, hi), (ex, ex + tiles)):
            at = a
            while at < b:
                stop = min(b, at + SPAN - (at - a) % SPAN)
                out.append(list(range(at, stop)))
                at = stop
        return out

    def around(i):
        last = ex + tiles - 1
        before = (last, GROUP) if i == ex else (i - 1, 0)
        after = (ex, -GROUP) if i == last else (i + 1, 0)
        return before, after

    def faces(load, group):
        v, turned_v = {}, {}
        for i in group:
            v[i] = load(i)
        for at, k in (around(group[0])[0], around(group[-1])[1]):
            turned_v[at, k] = v[at] if k == 0 and at in v else spin(load(at), k)
        up = {i: up_z(v[i]) for i in group}
        yield
        gz, dn = {}, {}
        for i in group:
            gz[i] = FZ[i] * (v[i] - up[i])
            dn[i] = dn_z(gz[i])
        yield
        out = {}
        (b, kb), _ = around(group[0])
        gx = FX[group[0]] * (v[group[0]] - turned_v[b, kb])
        for i in group:
            if i == group[-1]:
                a, ka = around(i)[1]
                after = turned_v[a, ka]
            else:
                after = v[i + 1]
            gx_next = FX[i + 1] * (after - v[i])
            gy = FY[i] * (v[i] - up_y(v[i]))
            out[i] = (v[i], (gx - gx_next) + ((gy - dn_y(gy)) + (gz[i] - dn[i])))
            gx = gx_next
        return out

    def reads(name, group):
        return {(name, i) for i in group} | {
            (name, around(group[0])[0][0]),
            (name, around(group[-1])[1][0]),
        }

    def run(items):
        done, open_items, at = set(), [], 0
        while at < len(items) or open_items:
            still = []
            for gen, gives in open_items:
                try:
                    next(gen)
                    still.append((gen, gives))
                except StopIteration:
                    done |= gives
            open_items = still
            if at < len(items) and items[at][1] <= done:
                gen, _, gives = items[at]
                at += 1
                try:
                    next(gen)
                    open_items.append((gen, gives))
                except StopIteration:
                    done |= gives

    wait_all(1)

    def limit(dx, dy, dz):
        return e_out[...] if (dx, dy, dz) == (0, 0, 0) else e_in[code(dx, dy, dz)]

    for k, (a, z) in enumerate(zip(tables(limit), depths())):
        z_f, even_f = z.astype(f32), (z - z % 2).astype(f32)
        FL[k] = (z_f < a).astype(f32)
        F1[k] = (even_f < a).astype(f32)

    build_edges(1, C)
    every = list(range(ex)) + list(range(ex, ex + tiles))
    for i in every:
        c = C[i]
        if i != 0:
            before = spin(C[ex + tiles - 1], GROUP) if i == ex else C[i - 1]
            FX[i] = 0.5 * (before + c)
        FY[i] = 0.5 * (c + up_y(c))
        FZ[i] = 0.5 * (c + up_z(c))
    FX[ex + tiles] = spin(FX[ex], -GROUP)
    for i in list(range(1, ex - 1)) + list(range(ex, ex + tiles)):
        fy, fz = FY[i], FZ[i]
        diagonal = (FX[i] + FX[i + 1]) + (fy + dn_y(fy)) + (fz + dn_z(fz))
        fl = FL[flag_of(i)]
        INV[i] = OMEGA * fl / (diagonal + 1.0 - fl)
    pairs, edge_pairs = ex // 2, tiles // 2
    for q in range(pairs + edge_pairs):
        C1[q] = pool_yz(C[2 * q] + C[2 * q + 1]) * 0.125
    for q in list(range(1, pairs - 1)) + list(range(pairs, pairs + edge_pairs)):
        c = C1[q]
        before = spin(C1[pairs + edge_pairs - 1], GROUP) if q == pairs else C1[q - 1]
        after = spin(C1[pairs], -GROUP) if q == pairs + edge_pairs - 1 else C1[q + 1]
        diagonal = 3.0 * c + 0.5 * (
            (before + after) + (up_y(c, 2) + dn_y(c, 2)) + (up_z(c, 2) + dn_z(c, 2))
        )
        fl = F1[flag_of(2 * q)]
        IC[q] = OMEGA * fl / (4.0 * diagonal + 1.0 - fl)

    off = lane_y % GROUP
    slot0 = (lane_y // GROUP) * tiles

    def core_edge(t, lo_off, hi_off):
        slot = slot0 + t
        low = (slot >= lo_x) & (slot < hi_x) & lo_off
        high = (slot >= ex + lo_x) & (slot < ex + hi_x) & hi_off
        return (low | high) & (lane_y < GROUP * edge.places)

    core_off = (off >= HALO) & (off < 2 * HALO)
    core_tiles = [core_edge(t, core_off, core_off) for t in range(tiles)]
    core_lanes = (lane_y >= HALO) & (lane_y < bz - HALO)

    flux_z = FZ[lo_x, :by]
    flux_y = FY[lo_x]
    for i in range(lo_x + 1, hi_x):
        flux_z = flux_z + FZ[i, :by]
        flux_y = flux_y + FY[i]
    fl = FL[1]
    fl_up, fl_core = up_y(fl), fl[:by]
    step = fl_core - up_z(fl)[:by]
    inner = jnp.where(lane_y >= 1, flux_z * (step * step), 0.0)
    none = jnp.logical_and(off < 0, off >= 0)
    low_face = [core_edge(t, off == HALO, none) for t in range(tiles)]
    high_face = [core_edge(t, none, off == 2 * HALO) for t in range(tiles)]
    sides = {}

    def put(d, alone, shared):
        sides[d] = (total(alone), total(shared))

    alone = FX[lo_x, :by] * fl_core
    put((-1, 0, 0), alone, alone * FL[0, :by])
    alone = FX[hi_x, :by] * fl_core
    put((1, 0, 0), alone, alone * FL[2, :by])
    alone = jnp.where(row == 0, flux_y * fl, 0.0)
    put((0, -1, 0), alone, alone * fl_up)
    alone = jnp.where(row == by, flux_y * fl_up, 0.0)
    put((0, 1, 0), alone, alone * fl)
    zeros = jnp.zeros((by, bz), f32)
    parts = [zeros] * 4
    for t in range(tiles):
        f_edge = FL[3 + edge.pattern_of[t]]
        f_here, f_up = f_edge[:by], up_z(f_edge)[:by]
        fz = FZ[ex + t, :by]
        a = jnp.where(low_face[t], fz * f_here, 0.0)
        b = jnp.where(high_face[t], fz * f_up, 0.0)
        parts = [parts[0] + a, parts[1] + a * f_up, parts[2] + b, parts[3] + b * f_here]
    put((0, 0, -1), parts[0], parts[1])
    put((0, 0, 1), parts[2], parts[3])

    scalars = 8
    width = late.shape[-1]
    base = scalars if width == bz else bz
    col = lax.broadcasted_iota(jnp.int32, (1, width), 1)
    diagonal = total(inner)
    late_row = jnp.zeros((1, width), f32)
    for (dx, dy, dz), (alone, shared) in sides.items():
        diagonal = diagonal + alone
        other = ((ix + dx) * ngy + iy + dy) * ngz + iz + dz
        valid = inside((dx, dy, dz))
        late_row = late_row - jnp.where((col == base + other) & valid, shared, 0.0)
    late_row = late_row + jnp.where(col == base + me, diagonal, 0.0)

    wait_all(0)
    build_edges(0, R)

    def solve(means):
        y_row = jnp.sum(inverse * means, axis=0, keepdims=True)
        y_col = jnp.sum(jnp.where(eye, y_row, 0.0), axis=1, keepdims=True)
        return y_row, y_col

    def block_row(dx, dy, dz):
        def near(at, step, count):
            return jnp.clip(at + step, 0, count - 1)

        b = (near(ix, dx, ngx) * ngy + near(iy, dy, ngy)) * ngz + near(iz, dz, ngz)
        return YB[pl.ds(b, 1)]

    def spread_blocks(y_col):
        YB[...] = jnp.broadcast_to(y_col, (n, bz))
        for k, v in enumerate(tables(block_row)):
            EY[k] = FL[k] * v

    cells = bx * by * bz
    collect(early, 0)
    m0_col = early[:, 0, 0:1]

    def first_solve():
        y_row = jnp.sum(inverse * (m0_col * (1.0 / cells)), axis=0, keepdims=True)
        yield
        y_col = jnp.sum(jnp.where(eye, y_row, 0.0), axis=1, keepdims=True)
        yield
        yield
        spread_blocks(y_col)

    items = [(first_solve(), set(), {"blocks"})]
    sums = [[zeros, zeros] for _ in range(7)]
    parts = {}

    def add(i, k, v):
        if i < ex:
            if lo_x <= i < hi_x:
                sums[k][0] = sums[k][0] + v
        else:
            sums[k][1] = sums[k][1] + jnp.where(core_tiles[i - ex], v, 0.0)

    def coarse(field, group):
        found = yield from faces(lambda i: INV[i] * field[i], group)
        pooled = {}
        for i in group[::2]:
            gap = FL[flag_of(i)] * (field[i] - found[i][1])
            gap = gap + FL[flag_of(i + 1)] * (field[i + 1] - found[i + 1][1])
            gap = gap + jnp.where(odd_row, up_y(gap), dn_y(gap))
            pooled[i] = (gap, up_z(gap), dn_z(gap))
        yield
        for i in group[::2]:
            gap, up, dn = pooled[i]
            below = IC[i // 2] * (gap + jnp.where(odd_lane, up, dn))
            for at in (i, i + 1):
                SEC[at] = found[at][0] + FL[flag_of(at)] * below

    def smooth(field, group, keep):
        found = yield from faces(lambda i: SEC[i], group)
        for i in group:
            v, lv = found[i]
            keep(i, v + INV[i] * (field[i] - lv))

    def image(load, group, keep):
        found = yield from faces(load, group)
        for i in group:
            keep(i, *found[i])

    def add_cycle(field, source, name, lo, hi, keep, extra):
        even, stop = (lo - 1) // 2 * 2, (hi + 2) // 2 * 2
        for group in groups(even, stop):
            needs = set() if source is None else reads(source, group)
            items.append((coarse(field, group), needs, {(name + "s", i) for i in group}))
        for group in groups(lo, hi):
            needs = reads(name + "s", group) | extra
            items.append((smooth(field, group, keep), needs, {(name, i) for i in group}))

    def keep_direction(i, v):
        D0[i] = v + EY[flag_of(i)]

    def keep_image(i, v, lv):
        w = FL[flag_of(i)] * lv
        W[i] = w
        add(i, 0, R[i, :by] * v[:by])
        add(i, 1, w[:by] * v[:by])
        add(i, 2, w[:by])

    def keep_second(i, v):
        U[i] = v
        add(i, 3, W[i, :by] * v[:by])
        add(i, 4, R[i, :by] * v[:by])

    def keep_third(i, v, lv):
        q = FL[flag_of(i)][:by] * lv[:by]
        Q[i, :by] = q
        add(i, 5, q * v[:by])
        add(i, 6, q)

    def gather_sums(which):
        for k in which:
            a, b = sums[k]
            parts[k] = total(jnp.where(core_lanes, a, 0.0) + b)
        yield

    def core_of(name):
        return {(name, i) for i in range(lo_x, hi_x)} | {(name, ex + t) for t in range(tiles)}

    add_cycle(R, None, "d", 4, ex - 4, keep_direction, {"blocks"})
    for group in groups(5, ex - 5):
        items.append(
            (image(lambda i: D0[i], group, keep_image), reads("d", group), {("w", i) for i in group})
        )
    add_cycle(W, "w", "u", 7, ex - 7, keep_second, set())
    items.append((gather_sums(range(3)), core_of("w"), set()))
    for group in groups(lo_x, hi_x):
        items.append(
            (image(lambda i: U[i], group, keep_third), reads("u", group), {("q", i) for i in group})
        )
    items.append((gather_sums(range(3, 5)), core_of("u"), set()))
    items.append((gather_sums(range(5, 7)), core_of("q"), set()))
    run(items)

    for k in range(7):
        late_row = jnp.where(col == k, parts[k], late_row)
    late_out[...] = late_row
    late[pl.ds(me, 1)] = late_row[None]
    spread(late_out, late, 1)
    collect(late, 1)

    rows = late[:, 0, :]
    y_row, y_col = solve(rows[:, 2:3] * (1.0 / cells))
    spread_blocks(y_col)
    plain = jnp.sum(rows, axis=0, keepdims=True)
    weighted = jnp.sum(rows * y_col, axis=0, keepdims=True)

    def pick(line, k):
        return jnp.sum(line[:, k : k + 1], axis=(0, 1), keepdims=True)

    rz, dad = pick(plain, 0), pick(plain, 1)
    y_m0 = total(m0_col * y_col)
    w_u = pick(plain, 3) + pick(weighted, 2)
    r_u = pick(plain, 4) + y_m0
    u_q = (
        pick(plain, 5)
        + 2.0 * pick(weighted, 6)
        + total(weighted[:, base : base + n] * y_row)
    )
    alpha = rz / dad
    new = (rz - alpha * dad) + alpha * (alpha * w_u - r_u)
    beta = new / rz
    grow = 1.0 + beta
    dad1 = grow * grow * dad - 2.0 * alpha * grow * w_u + alpha * alpha * u_q
    alpha1 = new / dad1
    c1 = alpha + alpha1 * grow
    c2 = alpha * alpha1

    def results(i, v, lv):
        fl = FL[flag_of(i)][:by]
        sol = c1 * D0[i, :by] - c2 * (U[i, :by] + v[:by])
        res = fl * R[i, :by] - c1 * W[i, :by] + c2 * (Q[i, :by] + fl * lv[:by])
        if i < ex:
            sol_ref[i - lo_x], res_ref[i - lo_x] = sol, res
        else:
            SEC[i, :by], INV[i, :by] = sol, res

    run(
        [
            (image(lambda i: EY[flag_of(i)], group, results), set(), set())
            for group in groups(lo_x, hi_x)
        ]
    )
    for x in range(bx):
        tl, jl = edge.place(lo_x + x, 0)
        th, jh = edge.place(lo_x + x, 1)
        for ref, held in ((sol_ref, SEC), (res_ref, INV)):
            low = spin(held[ex + tl, :by], -(GROUP * jl + HALO))
            high = spin(held[ex + th, :by], bz - HALO - (GROUP * jh + HALO))
            ref[x] = jnp.where(
                lane_y < HALO, low, jnp.where(lane_y >= bz - HALO, high, ref[x])
            )
    wait_sent(1)
    wait_sent(0)


def solution(mesh):
    counts = (mesh.shape["gx"], mesh.shape["gy"], mesh.shape["gz"])
    n = counts[0] * counts[1] * counts[2]

    def on_device(right_side, conductance, extents, coarse_factor):
        f32 = jnp.float32
        bx, by, bz = right_side.shape
        ex, ey = bx + 2 * HALO, by + 2 * HALO
        edge = Edge(bx, bz)
        slabs = ex + edge.tiles
        width = bz if n + 8 <= bz else bz + -(-n // 128) * 128
        vm = lambda *shape: pltpu.VMEM(shape, f32)
        field = vm(slabs, ey, bz)
        half = vm(slabs // 2, ey, bz)
        flags = vm(3 + len(edge.patterns), ey, bz)
        dma = pltpu.SemaphoreType.DMA
        scratch = [
            field,
            field,
            pltpu.VMEM(extents.shape, extents.dtype),
            pltpu.VMEM(coarse_factor.shape, coarse_factor.dtype),
            vm(1, bz),
            vm(27, 1, bz),
            vm(2, by, bz),
            vm(2, 2, 3, ey, bz),
            vm(1, bz),
            vm(n, 1, bz),
            vm(1, width),
            vm(n, 1, width),
            flags,
            flags,
            vm(slabs + 1, ey, bz),
            field,
            field,
            field,
            half,
            half,
            field,
            field,
            field,
            field,
            field,
            vm(n, bz),
            flags,
            dma((27,)),
            dma((27,)),
            dma((27,)),
            dma((27,)),
            dma((27,)),
            dma((27,)),
            dma((2,)),
            dma((2,)),
            dma((4,)),
        ]
        block = vm(bx, by, bz)
        whole = pl.BlockSpec(memory_space=pltpu.VMEM)
        outer = pl.BlockSpec(memory_space=pltpu.HBM)
        return pl.pallas_call(
            functools.partial(kernel, counts),
            out_shape=(block, block),
            in_specs=[outer, outer, outer, outer],
            out_specs=(whole, whole),
            scratch_shapes=scratch,
            compiler_params=pltpu.CompilerParams(
                collective_id=0, has_side_effects=True, vmem_limit_bytes=60000000
            ),
        )(right_side, conductance, extents, coarse_factor)

    in_specs = (P("gx", "gy", "gz"), P("gx", "gy", "gz"), P("gx", "gy", "gz"), P())
    out_specs = (P("gx", "gy", "gz"), P("gx", "gy", "gz"))
    return jax.shard_map(
        on_device, mesh=mesh, in_specs=in_specs, out_specs=out_specs, check_vma=False
    )
```

```python
import functools

import jax
import jax.numpy as jnp
from jax import lax
from jax.experimental import pallas as pl
from jax.experimental.pallas import tpu as pltpu
from jax.sharding import PartitionSpec as P

OMEGA = 0.8
HALO = 8
GROUP = 3 * HALO
SPAN = 16
MESH = pl.DeviceIdType.MESH
HIGH = lax.Precision.HIGHEST
DIRS = [
    (dx, dy, dz)
    for dx in (-1, 0, 1)
    for dy in (-1, 0, 1)
    for dz in (-1, 0, 1)
    if (dx, dy, dz) != (0, 0, 0)
]
DIRS.sort(key=lambda d: -sum(abs(a) for a in d))


def code(dx, dy, dz):
    return (dx + 1) * 9 + (dy + 1) * 3 + dz + 1


class Edge:
    def __init__(self, bx, bz):
        self.bx, self.ex = bx, bx + 2 * HALO
        self.places = bz // GROUP
        tiles = -(-2 * self.ex // self.places)
        self.tiles = tiles + tiles % 2
        self.patterns, self.pattern_of = [], []
        for t in range(self.tiles):
            key = tuple(
                None if s is None else (self.block(s[0])[0], s[1])
                for s in (self.slab(t, j) for j in range(self.places))
            )
            if key not in self.patterns:
                self.patterns.append(key)
            self.pattern_of.append(self.patterns.index(key))

    def slab(self, t, j):
        slot = t + self.tiles * j
        return None if slot >= 2 * self.ex else (slot % self.ex, slot // self.ex)

    def place(self, s, side):
        slot = s + self.ex * side
        return slot % self.tiles, slot // self.tiles

    def block(self, s):
        if s < HALO:
            return 0, self.bx - HALO + s
        if s < HALO + self.bx:
            return 1, s - HALO
        return 2, s - HALO - self.bx


def kernel(
    counts,
    rhs_hbm,
    cond_hbm,
    ext_hbm,
    factor_hbm,
    both_ref,
    R,
    C,
    ext_ref,
    factor_ref,
    e_out,
    e_in,
    z_out,
    z_in,
    early_out,
    early,
    late_out,
    late,
    FL,
    F1,
    FX,
    FY,
    FZ,
    INV,
    C1,
    IC,
    SEC,
    D0,
    W,
    U,
    Q,
    YB,
    EY,
    send_c,
    recv_c,
    send_r,
    recv_r,
    send_e,
    recv_e,
    send_g,
    recv_g,
    load_sem,
):
    sol_ref, res_ref = both_ref.at[0], both_ref.at[1]
    ngx, ngy, ngz = counts
    n = ngx * ngy * ngz
    ix, iy, iz = lax.axis_index("gx"), lax.axis_index("gy"), lax.axis_index("gz")
    me = (ix * ngy + iy) * ngz + iz
    bx, by, bz = sol_ref.shape
    ex, ey = bx + 2 * HALO, by + 2 * HALO
    edge = Edge(bx, bz)
    tiles = edge.tiles
    f32 = jnp.float32
    lo_x, hi_x = HALO, HALO + bx

    def turned(at, step, count):
        moved = at + step
        return jnp.where(moved >= count, moved - count, moved)

    def everyone(act):
        if n <= 64:
            xs = [turned(ix, t, ngx) for t in range(ngx)]
            ys = [turned(iy, t, ngy) for t in range(ngy)]
            zs = [turned(iz, t, ngz) for t in range(ngz)]
            steps = [(a, b, c) for a in range(ngx) for b in range(ngy) for c in range(ngz)]
            steps.sort(
                key=lambda t: -sum(min(a, m - a) for a, m in zip(t, (ngx, ngy, ngz)))
            )
            for a, b, c in steps[:-1]:
                act((xs[a], ys[b], zs[c]))
        else:

            def one(t, carry):
                flat = (me + t) % n
                act((flat // (ngy * ngz), (flat // ngz) % ngy, flat % ngz))
                return carry

            lax.fori_loop(1, n, one, 0)

    core_x, core_y = pl.ds(lo_x, bx), pl.ds(0, by)
    loads = [
        pltpu.make_async_copy(src, dst, load_sem.at[k])
        for k, (src, dst) in enumerate(
            (
                (rhs_hbm, R.at[core_x, core_y]),
                (cond_hbm, C.at[core_x, core_y]),
                (ext_hbm, ext_ref),
                (factor_hbm, factor_ref),
            )
        )
    ]
    for load in loads:
        load.start()

    barrier = pltpu.get_barrier_semaphore()
    everyone(
        lambda device: pl.semaphore_signal(
            barrier, inc=1, device_id=device, device_id_type=MESH
        )
    )

    def inside(d):
        ok = None
        for at, step, count in zip((ix, iy, iz), d, counts):
            if step == 0:
                continue
            here = (at + step >= 0) & (at + step < count)
            ok = here if ok is None else ok & here
        return ok

    def x_from(dx):
        return pl.ds(bx, HALO) if dx == 1 else pl.ds(HALO, bx if dx == 0 else HALO)

    def x_into(dx):
        if dx == 0:
            return pl.ds(HALO, bx)
        return pl.ds(0, HALO) if dx == 1 else pl.ds(hi_x, HALO)

    def y_from(dy):
        return pl.ds(by - HALO, HALO) if dy == 1 else pl.ds(0, by if dy == 0 else HALO)

    def y_into(dy):
        if dy == 0:
            return pl.ds(0, by)
        return pl.ds(by + HALO, HALO) if dy == 1 else pl.ds(by, HALO)

    def landing(f, d):
        dx, dy, dz = d
        if dz != 0:
            return z_in.at[f, 1 if dz == 1 else 0, 1 - dx, y_into(dy)]
        return (R, C)[f].at[x_into(dx), y_into(dy)]

    def remote(src, dst, send, recv, d):
        return pltpu.make_async_remote_copy(
            src_ref=src,
            dst_ref=dst,
            send_sem=send,
            recv_sem=recv,
            device_id=(ix + d[0], iy + d[1], iz + d[2]),
            device_id_type=MESH,
        )

    def copies(f, d):
        dx, dy, dz = d
        k = code(*d)
        if dz != 0:
            src = z_out.at[f, y_from(dy)]
        else:
            src = (R, C)[f].at[x_from(dx), y_from(dy)]
        send, recv = ((send_r, recv_r), (send_c, recv_c))[f]
        out = [remote(src, landing(f, d), send.at[k], recv.at[k], d)]
        if f == 1:
            out.append(remote(e_out, e_in.at[code(-dx, -dy, -dz)], send_e.at[k], recv_e.at[k], d))
        return out

    odd = ix % 2 == 1

    def corner(d):
        return d[0] != 0 and d[1] != 0 and d[2] == 0

    def when_sent(f, act):
        for d in DIRS:

            @pl.when(inside(d))
            def _():
                values, *flags = copies(f, d)
                for c in flags:
                    act(c)
                if not corner(d):
                    act(values)
                    return

                if d[0] == 1:
                    act(values)
                    return

                @pl.when(jnp.logical_not(odd))
                def _():
                    act(values)

    def relayed(f, dy):
        field, k = (R, C)[f], code(-1, dy, 0)
        send, recv = ((send_r, recv_r), (send_c, recv_c))[f]
        return remote(
            field.at[x_from(-1), y_into(dy)],
            field.at[x_into(-1), y_into(dy)],
            send.at[k],
            recv.at[k],
            (-1, 0, 0),
        )

    def start_all(f):
        when_sent(f, lambda c: c.start())

    def relay(f):
        for dy in (-1, 1):

            @pl.when(inside((0, -dy, 0)) & odd)
            def _():
                for c in copies(f, (0, dy, 0)):
                    c.wait_recv()
                relayed(f, dy).start()

    def wait_all(f):
        for d in DIRS:
            ok = inside(tuple(-a for a in d))

            @pl.when(ok & jnp.logical_not(odd) if d[0] == 0 and d[2] == 0 else ok)
            def _():
                for c in copies(f, d):
                    c.wait_recv()

    def wait_sent(f):
        when_sent(f, lambda c: c.wait_send())
        for dy in (-1, 1):

            @pl.when(inside((0, -dy, 0)) & odd)
            def _():
                relayed(f, dy).wait_send()

    for d in DIRS:

        @pl.when(jnp.logical_not(inside(tuple(-a for a in d))))
        def _():
            for f in (0, 1):
                ref = landing(f, d)
                ref[...] = jnp.zeros(ref.shape, f32)
            e_in[code(*(-a for a in d))] = jnp.zeros((1, bz), f32)

    lane = lax.broadcasted_iota(jnp.int32, (ey, bz), 1)
    row = lax.broadcasted_iota(jnp.int32, (ey, bz), 0)
    odd_lane, odd_row = lane % 2 == 1, row % 2 == 1
    lane_y = lane[:by]

    def up_y(v, k=1):
        return pltpu.roll(v, k, 0)

    def dn_y(v, k=1):
        return pltpu.roll(v, ey - k, 0)

    def spin(v, k):
        k = k % bz
        return v if k == 0 else pltpu.roll(v, k, 1)

    def up_z(v, k=1):
        return pltpu.roll(v, k, 1)

    def dn_z(v, k=1):
        return pltpu.roll(v, bz - k, 1)

    for load in loads[:3]:
        load.wait()
    own_limit = ext_ref[0].astype(f32)
    e_out[...] = jnp.broadcast_to(own_limit, (1, bz))
    for f, field in ((1, C), (0, R)):
        packed = jnp.zeros((by, bz), f32)
        for k in range(bx):
            moved = spin(field[lo_x + k, :by], 2 * HALO * k + HALO)
            packed = jnp.where(lane_y // (2 * HALO) == k, moved, packed)
        z_out[f] = packed

    def total(v):
        return jnp.sum(v, axis=(0, 1), keepdims=True)

    acc = R[lo_x, :by]
    for k in range(1, bx):
        acc = acc + R[lo_x + k, :by]
    m0 = total(jnp.where(lane_y.astype(f32) < own_limit, acc, 0.0))
    early_row = jnp.broadcast_to(m0, (1, bz))
    early_out[...] = early_row
    early[pl.ds(me, 1)] = early_row[None]

    def remote_row(out, into, base, device):
        return pltpu.make_async_remote_copy(
            src_ref=out,
            dst_ref=into.at[me],
            send_sem=send_g.at[base],
            recv_sem=recv_g.at[base],
            device_id=device,
            device_id_type=MESH,
        )

    def spread(out, into, base):
        everyone(lambda device: remote_row(out, into, base, device).start())

    def collect(into, base):
        part = into.at[pl.ds(0, n - 1)]
        pltpu.make_async_copy(part, part, recv_g.at[base]).wait()
        pltpu.make_async_copy(part, part, send_g.at[base]).wait()

    pl.semaphore_wait(barrier, n - 1)
    start_all(1)
    spread(early_out, early, 0)
    start_all(0)

    loads[3].wait()
    L = factor_ref[...].astype(f32)
    ri = lax.broadcasted_iota(jnp.int32, (n, n), 0)
    ci = lax.broadcasted_iota(jnp.int32, (n, n), 1)
    eye = ri == ci
    X = jnp.where(eye, 1.0 / jnp.where(eye, L, 1.0), 0.0)
    s = 1
    while s < n:
        pick = (ri // (2 * s) == ci // (2 * s)) & (ri % (2 * s) >= s) & (ci % (2 * s) < s)
        low = jnp.where(pick, L, 0.0)
        X = X - jnp.dot(
            X,
            jnp.dot(low, X, precision=HIGH, preferred_element_type=f32),
            precision=HIGH,
            preferred_element_type=f32,
        )
        s *= 2
    inverse = lax.dot_general(
        X, X, (((0,), (0,)), ((), ())), precision=HIGH, preferred_element_type=f32
    )

    one_lane = lax.broadcasted_iota(jnp.int32, (1, bz), 1)
    bands = ((0, by), (1, HALO), (-1, HALO))

    def tables(value):
        rows = {
            (dx, dy, dz): value(dx, dy, dz)
            for dx in (-1, 0, 1)
            for dy in (-1, 0, 1)
            for dz in (-1, 0, 1)
        }
        out = [
            jnp.concatenate(
                [jnp.broadcast_to(rows[dx, dy, 0], (count, bz)) for dy, count in bands], axis=0
            )
            for dx in (-1, 0, 1)
        ]
        for pattern in edge.patterns:
            parts = []
            for dy, count in bands:
                line = None
                for j, key in enumerate(pattern):
                    if key is None:
                        continue
                    dx, start = key[0] - 1, GROUP * j
                    if key[1] == 0:
                        here = jnp.where(
                            one_lane < start + HALO, rows[dx, dy, -1], rows[dx, dy, 0]
                        )
                    else:
                        here = jnp.where(
                            one_lane < start + 2 * HALO, rows[dx, dy, 0], rows[dx, dy, 1]
                        )
                    line = here if line is None else jnp.where(one_lane >= start, here, line)
                parts.append(jnp.broadcast_to(line, (count, bz)))
            out.append(jnp.concatenate(parts, axis=0))
        return out

    def depths():
        plain = one_lane
        out = [plain] * 3
        for pattern in edge.patterns:
            line = None
            for j, key in enumerate(pattern):
                off = one_lane - GROUP * j
                if key is None:
                    here = jnp.full((1, bz), bz, jnp.int32)
                elif key[1] == 0:
                    here = jnp.where(off < HALO, off + bz - HALO, off - HALO)
                else:
                    here = jnp.where(off < 2 * HALO, off + bz - 2 * HALO, off - 2 * HALO)
                line = here if line is None else jnp.where(off >= 0, here, line)
            line = jnp.where(one_lane >= GROUP * edge.places, bz, line)
            out.append(line)
        return out

    def flag_of(i):
        return edge.block(i)[0] if i < ex else 3 + edge.pattern_of[i - ex]

    def build_edges(f, field):
        for t in range(tiles):
            acc = None
            for j in range(edge.places):
                slab = edge.slab(t, j)
                start = GROUP * j
                if slab is None:
                    acc = jnp.where(lane >= start, 0.0, acc)
                    break
                s, side = slab
                which, k = edge.block(s)
                at = 2 * HALO * k
                if side == 0:
                    own = spin(field[s], start + HALO)
                    far = spin(z_in[f, 1, which], start - at)
                    here = jnp.where(lane < start + HALO, far, own)
                else:
                    own = spin(field[s], start + 2 * HALO - bz)
                    far = spin(z_in[f, 0, which], start + HALO - at)
                    here = jnp.where(lane < start + 2 * HALO, own, far)
                acc = here if acc is None else jnp.where(lane >= start, here, acc)
            field[ex + t] = jnp.where(lane < GROUP * edge.places, acc, 0.0)

    def pool_yz(v):
        v = v + jnp.where(odd_row, up_y(v), dn_y(v))
        return v + jnp.where(odd_lane, up_z(v), dn_z(v))

    def groups(lo, hi):
        out = []
        for a, b in ((lo, hi), (ex, ex + tiles)):
            at = a
            while at < b:
                stop = min(b, at + SPAN - (at - a) % SPAN)
                out.append(list(range(at, stop)))
                at = stop
        return out

    def around(i):
        last = ex + tiles - 1
        before = (last, GROUP) if i == ex else (i - 1, 0)
        after = (ex, -GROUP) if i == last else (i + 1, 0)
        return before, after

    def faces(load, group):
        v, turned_v = {}, {}
        for i in group:
            v[i] = load(i)
        for at, k in (around(group[0])[0], around(group[-1])[1]):
            turned_v[at, k] = v[at] if k == 0 and at in v else spin(load(at), k)
        up = {i: up_z(v[i]) for i in group}
        yield
        gz, dn = {}, {}
        for i in group:
            gz[i] = FZ[i] * (v[i] - up[i])
            dn[i] = dn_z(gz[i])
        yield
        out = {}
        (b, kb), _ = around(group[0])
        gx = FX[group[0]] * (v[group[0]] - turned_v[b, kb])
        for i in group:
            if i == group[-1]:
                a, ka = around(i)[1]
                after = turned_v[a, ka]
            else:
                after = v[i + 1]
            gx_next = FX[i + 1] * (after - v[i])
            gy = FY[i] * (v[i] - up_y(v[i]))
            out[i] = (v[i], (gx - gx_next) + ((gy - dn_y(gy)) + (gz[i] - dn[i])))
            gx = gx_next
        return out

    def reads(name, group):
        return {(name, i) for i in group} | {
            (name, around(group[0])[0][0]),
            (name, around(group[-1])[1][0]),
        }

    def run(items):
        done, open_items, at = set(), [], 0
        while at < len(items) or open_items:
            still = []
            for gen, gives in open_items:
                try:
                    next(gen)
                    still.append((gen, gives))
                except StopIteration:
                    done |= gives
            open_items = still
            if at < len(items) and items[at][1] <= done:
                gen, _, gives = items[at]
                at += 1
                try:
                    next(gen)
                    open_items.append((gen, gives))
                except StopIteration:
                    done |= gives

    relay(1)
    wait_all(1)
    relay(0)

    def limit(dx, dy, dz):
        return e_out[...] if (dx, dy, dz) == (0, 0, 0) else e_in[code(dx, dy, dz)]

    for k, (a, z) in enumerate(zip(tables(limit), depths())):
        z_f, even_f = z.astype(f32), (z - z % 2).astype(f32)
        FL[k] = (z_f < a).astype(f32)
        F1[k] = (even_f < a).astype(f32)

    build_edges(1, C)
    every = list(range(ex)) + list(range(ex, ex + tiles))
    for i in every:
        c = C[i]
        if i != 0:
            before = spin(C[ex + tiles - 1], GROUP) if i == ex else C[i - 1]
            FX[i] = 0.5 * (before + c)
        FY[i] = 0.5 * (c + up_y(c))
        FZ[i] = 0.5 * (c + up_z(c))
    FX[ex + tiles] = spin(FX[ex], -GROUP)
    for i in list(range(1, ex - 1)) + list(range(ex, ex + tiles)):
        fy, fz = FY[i], FZ[i]
        diagonal = (FX[i] + FX[i + 1]) + (fy + dn_y(fy)) + (fz + dn_z(fz))
        fl = FL[flag_of(i)]
        INV[i] = OMEGA * fl / (diagonal + 1.0 - fl)
    pairs, edge_pairs = ex // 2, tiles // 2
    for q in range(pairs + edge_pairs):
        C1[q] = pool_yz(C[2 * q] + C[2 * q + 1]) * 0.125
    for q in list(range(1, pairs - 1)) + list(range(pairs, pairs + edge_pairs)):
        c = C1[q]
        before = spin(C1[pairs + edge_pairs - 1], GROUP) if q == pairs else C1[q - 1]
        after = spin(C1[pairs], -GROUP) if q == pairs + edge_pairs - 1 else C1[q + 1]
        diagonal = 3.0 * c + 0.5 * (
            (before + after) + (up_y(c, 2) + dn_y(c, 2)) + (up_z(c, 2) + dn_z(c, 2))
        )
        fl = F1[flag_of(2 * q)]
        IC[q] = OMEGA * fl / (4.0 * diagonal + 1.0 - fl)

    off = lane_y % GROUP
    slot0 = (lane_y // GROUP) * tiles

    def core_edge(t, lo_off, hi_off):
        slot = slot0 + t
        low = (slot >= lo_x) & (slot < hi_x) & lo_off
        high = (slot >= ex + lo_x) & (slot < ex + hi_x) & hi_off
        return (low | high) & (lane_y < GROUP * edge.places)

    core_off = (off >= HALO) & (off < 2 * HALO)
    core_tiles = [core_edge(t, core_off, core_off) for t in range(tiles)]
    core_lanes = (lane_y >= HALO) & (lane_y < bz - HALO)

    zeros = jnp.zeros((by, bz), f32)
    scalars = 8
    width = late.shape[-1]
    base = scalars if width == bz else bz
    col = lax.broadcasted_iota(jnp.int32, (1, width), 1)
    coupling = {}

    def couple():
        flux_z = FZ[lo_x, :by]
        flux_y = FY[lo_x]
        for i in range(lo_x + 1, hi_x):
            flux_z = flux_z + FZ[i, :by]
            flux_y = flux_y + FY[i]
        fl = FL[1]
        fl_up, fl_core = up_y(fl), fl[:by]
        step = fl_core - up_z(fl)[:by]
        inner = jnp.where(lane_y >= 1, flux_z * (step * step), 0.0)
        none = jnp.logical_and(off < 0, off >= 0)
        low_face = [core_edge(t, off == HALO, none) for t in range(tiles)]
        high_face = [core_edge(t, none, off == 2 * HALO) for t in range(tiles)]
        sides = {}

        def put(d, alone, shared):
            sides[d] = (total(alone), total(shared))

        alone = FX[lo_x, :by] * fl_core
        put((-1, 0, 0), alone, alone * FL[0, :by])
        alone = FX[hi_x, :by] * fl_core
        put((1, 0, 0), alone, alone * FL[2, :by])
        alone = jnp.where(row == 0, flux_y * fl, 0.0)
        put((0, -1, 0), alone, alone * fl_up)
        alone = jnp.where(row == by, flux_y * fl_up, 0.0)
        put((0, 1, 0), alone, alone * fl)
        parts = [zeros] * 4
        for t in range(tiles):
            f_edge = FL[3 + edge.pattern_of[t]]
            f_here, f_up = f_edge[:by], up_z(f_edge)[:by]
            fz = FZ[ex + t, :by]
            a = jnp.where(low_face[t], fz * f_here, 0.0)
            b = jnp.where(high_face[t], fz * f_up, 0.0)
            parts = [parts[0] + a, parts[1] + a * f_up, parts[2] + b, parts[3] + b * f_here]
        put((0, 0, -1), parts[0], parts[1])
        put((0, 0, 1), parts[2], parts[3])

        inner_sum = total(inner)
        yield
        yield
        diagonal = inner_sum
        late_row = jnp.zeros((1, width), f32)
        for (dx, dy, dz), (alone, shared) in sides.items():
            diagonal = diagonal + alone
            other = ((ix + dx) * ngy + iy + dy) * ngz + iz + dz
            valid = inside((dx, dy, dz))
            late_row = late_row - jnp.where((col == base + other) & valid, shared, 0.0)
        late_row = late_row + jnp.where(col == base + me, diagonal, 0.0)
        coupling[0] = late_row

    wait_all(0)
    build_edges(0, R)

    def solve(means):
        y_row = jnp.sum(inverse * means, axis=0, keepdims=True)
        y_col = jnp.sum(jnp.where(eye, y_row, 0.0), axis=1, keepdims=True)
        return y_row, y_col

    def block_row(dx, dy, dz):
        def near(at, step, count):
            return jnp.clip(at + step, 0, count - 1)

        b = (near(ix, dx, ngx) * ngy + near(iy, dy, ngy)) * ngz + near(iz, dz, ngz)
        return YB[pl.ds(b, 1)]

    def spread_blocks(y_col):
        YB[...] = jnp.broadcast_to(y_col, (n, bz))
        for k, v in enumerate(tables(block_row)):
            EY[k] = FL[k] * v

    cells = bx * by * bz
    collect(early, 0)
    m0_col = early[:, 0, 0:1]

    def first_solve():
        y_row = jnp.sum(inverse * (m0_col * (1.0 / cells)), axis=0, keepdims=True)
        yield
        y_col = jnp.sum(jnp.where(eye, y_row, 0.0), axis=1, keepdims=True)
        yield
        yield
        spread_blocks(y_col)

    items = [(first_solve(), set(), {"blocks"})]
    sums = [[zeros, zeros] for _ in range(7)]
    parts = {}

    def add(i, k, v):
        if i < ex:
            if lo_x <= i < hi_x:
                sums[k][0] = sums[k][0] + v
        else:
            sums[k][1] = sums[k][1] + jnp.where(core_tiles[i - ex], v, 0.0)

    def coarse(field, group):
        found = yield from faces(lambda i: INV[i] * field[i], group)
        pooled = {}
        for i in group[::2]:
            gap = FL[flag_of(i)] * (field[i] - found[i][1])
            gap = gap + FL[flag_of(i + 1)] * (field[i + 1] - found[i + 1][1])
            gap = gap + jnp.where(odd_row, up_y(gap), dn_y(gap))
            pooled[i] = (gap, up_z(gap), dn_z(gap))
        yield
        for i in group[::2]:
            gap, up, dn = pooled[i]
            below = IC[i // 2] * (gap + jnp.where(odd_lane, up, dn))
            for at in (i, i + 1):
                SEC[at] = found[at][0] + FL[flag_of(at)] * below

    def smooth(field, group, keep):
        found = yield from faces(lambda i: SEC[i], group)
        for i in group:
            v, lv = found[i]
            keep(i, v + INV[i] * (field[i] - lv))

    def image(load, group, keep):
        found = yield from faces(load, group)
        for i in group:
            keep(i, *found[i])

    def add_cycle(field, source, name, lo, hi, keep, extra):
        even, stop = (lo - 1) // 2 * 2, (hi + 2) // 2 * 2
        for group in groups(even, stop):
            needs = set() if source is None else reads(source, group)
            items.append((coarse(field, group), needs, {(name + "s", i) for i in group}))
        for group in groups(lo, hi):
            needs = reads(name + "s", group) | extra
            items.append((smooth(field, group, keep), needs, {(name, i) for i in group}))

    def keep_direction(i, v):
        D0[i] = v + EY[flag_of(i)]

    def keep_image(i, v, lv):
        w = FL[flag_of(i)] * lv
        W[i] = w
        add(i, 0, R[i, :by] * v[:by])
        add(i, 1, w[:by] * v[:by])
        add(i, 2, w[:by])

    def keep_second(i, v):
        U[i] = v
        add(i, 3, W[i, :by] * v[:by])
        add(i, 4, R[i, :by] * v[:by])

    def keep_third(i, v, lv):
        q = FL[flag_of(i)][:by] * lv[:by]
        Q[i, :by] = q
        add(i, 5, q * v[:by])
        add(i, 6, q)

    def gather_sums(which):
        for k in which:
            a, b = sums[k]
            parts[k] = total(jnp.where(core_lanes, a, 0.0) + b)
        yield

    def core_of(name):
        return {(name, i) for i in range(lo_x, hi_x)} | {(name, ex + t) for t in range(tiles)}

    add_cycle(R, None, "d", 4, ex - 4, keep_direction, {"blocks"})
    for group in groups(5, ex - 5):
        items.append(
            (image(lambda i: D0[i], group, keep_image), reads("d", group), {("w", i) for i in group})
        )
    add_cycle(W, "w", "u", 7, ex - 7, keep_second, set())
    items.append((couple(), set(), set()))
    items.append((gather_sums(range(3)), core_of("w"), set()))
    for group in groups(lo_x, hi_x):
        items.append(
            (image(lambda i: U[i], group, keep_third), reads("u", group), {("q", i) for i in group})
        )
    items.append((gather_sums(range(3, 5)), core_of("u"), set()))
    items.append((gather_sums(range(5, 7)), core_of("q"), set()))
    run(items)

    late_row = coupling[0]
    for k in range(7):
        late_row = jnp.where(col == k, parts[k], late_row)
    late_out[...] = late_row
    late[pl.ds(me, 1)] = late_row[None]
    spread(late_out, late, 1)
    wait_sent(1)
    wait_sent(0)
    collect(late, 1)

    rows = late[:, 0, :]
    y_row, y_col = solve(rows[:, 2:3] * (1.0 / cells))
    spread_blocks(y_col)
    plain = jnp.sum(rows, axis=0, keepdims=True)
    weighted = jnp.sum(rows * y_col, axis=0, keepdims=True)

    def pick(line, k):
        return jnp.sum(line[:, k : k + 1], axis=(0, 1), keepdims=True)

    rz, dad = pick(plain, 0), pick(plain, 1)
    y_m0 = total(m0_col * y_col)
    w_u = pick(plain, 3) + pick(weighted, 2)
    r_u = pick(plain, 4) + y_m0
    u_q = (
        pick(plain, 5)
        + 2.0 * pick(weighted, 6)
        + total(weighted[:, base : base + n] * y_row)
    )
    alpha = rz / dad
    new = (rz - alpha * dad) + alpha * (alpha * w_u - r_u)
    beta = new / rz
    grow = 1.0 + beta
    dad1 = grow * grow * dad - 2.0 * alpha * grow * w_u + alpha * alpha * u_q
    alpha1 = new / dad1
    c1 = alpha + alpha1 * grow
    c2 = alpha * alpha1

    def results(i, v, lv):
        fl = FL[flag_of(i)][:by]
        sol = c1 * D0[i, :by] - c2 * (U[i, :by] + v[:by])
        res = fl * R[i, :by] - c1 * W[i, :by] + c2 * (Q[i, :by] + fl * lv[:by])
        if i < ex:
            sol_ref[i - lo_x], res_ref[i - lo_x] = sol, res
        else:
            SEC[i, :by], INV[i, :by] = sol, res

    run(
        [
            (image(lambda i: EY[flag_of(i)], group, results), set(), set())
            for group in groups(lo_x, hi_x)
        ]
    )
    for x in range(bx):
        tl, jl = edge.place(lo_x + x, 0)
        th, jh = edge.place(lo_x + x, 1)
        for ref, held in ((sol_ref, SEC), (res_ref, INV)):
            low = spin(held[ex + tl, :by], -(GROUP * jl + HALO))
            high = spin(held[ex + th, :by], bz - HALO - (GROUP * jh + HALO))
            ref[x] = jnp.where(
                lane_y < HALO, low, jnp.where(lane_y >= bz - HALO, high, ref[x])
            )


def solution(mesh):
    counts = (mesh.shape["gx"], mesh.shape["gy"], mesh.shape["gz"])
    n = counts[0] * counts[1] * counts[2]

    def on_device(right_side, conductance, extents, coarse_factor):
        f32 = jnp.float32
        bx, by, bz = right_side.shape
        ex, ey = bx + 2 * HALO, by + 2 * HALO
        edge = Edge(bx, bz)
        slabs = ex + edge.tiles
        width = bz if n + 8 <= bz else bz + -(-n // 128) * 128
        vm = lambda *shape: pltpu.VMEM(shape, f32)
        field = vm(slabs, ey, bz)
        half = vm(slabs // 2, ey, bz)
        flags = vm(3 + len(edge.patterns), ey, bz)
        dma = pltpu.SemaphoreType.DMA
        scratch = [
            field,
            field,
            pltpu.VMEM(extents.shape, extents.dtype),
            pltpu.VMEM(coarse_factor.shape, coarse_factor.dtype),
            vm(1, bz),
            vm(27, 1, bz),
            vm(2, by, bz),
            vm(2, 2, 3, ey, bz),
            vm(1, bz),
            vm(n, 1, bz),
            vm(1, width),
            vm(n, 1, width),
            flags,
            flags,
            vm(slabs + 1, ey, bz),
            field,
            field,
            field,
            half,
            half,
            field,
            field,
            field,
            field,
            field,
            vm(n, bz),
            flags,
            dma((27,)),
            dma((27,)),
            dma((27,)),
            dma((27,)),
            dma((27,)),
            dma((27,)),
            dma((2,)),
            dma((2,)),
            dma((4,)),
        ]
        whole = pl.BlockSpec(memory_space=pltpu.VMEM)
        outer = pl.BlockSpec(memory_space=pltpu.HBM)
        both = pl.pallas_call(
            functools.partial(kernel, counts),
            out_shape=vm(2, bx, by, bz),
            in_specs=[outer, outer, outer, outer],
            out_specs=whole,
            scratch_shapes=scratch,
            compiler_params=pltpu.CompilerParams(
                collective_id=0, has_side_effects=True, vmem_limit_bytes=60000000
            ),
        )(right_side, conductance, extents, coarse_factor)
        return both[0], both[1]

    in_specs = (P("gx", "gy", "gz"), P("gx", "gy", "gz"), P("gx", "gy", "gz"), P())
    out_specs = (P("gx", "gy", "gz"), P("gx", "gy", "gz"))
    return jax.shard_map(
        on_device, mesh=mesh, in_specs=in_specs, out_specs=out_specs, check_vma=False
    )
```

```python
import functools

import jax
import jax.numpy as jnp
from jax import lax
from jax.experimental import pallas as pl
from jax.experimental.pallas import tpu as pltpu
from jax.sharding import PartitionSpec as P

OMEGA = 0.8
HALO = 8
GROUP = 3 * HALO
SPAN = 24
WIDE = 12
EDGES = 2
MESH = pl.DeviceIdType.MESH
HIGH = lax.Precision.HIGHEST
DIRS = [
    (dx, dy, dz)
    for dx in (-1, 0, 1)
    for dy in (-1, 0, 1)
    for dz in (-1, 0, 1)
    if (dx, dy, dz) != (0, 0, 0)
]
DIRS.sort(key=lambda d: -sum(abs(a) for a in d))


def code(dx, dy, dz):
    return (dx + 1) * 9 + (dy + 1) * 3 + dz + 1


class Edge:
    def __init__(self, bx, bz):
        self.bx, self.ex = bx, bx + 2 * HALO
        self.places = bz // GROUP
        tiles = -(-2 * self.ex // self.places)
        self.tiles = tiles + tiles % 2
        self.patterns, self.pattern_of = [], []
        for t in range(self.tiles):
            key = tuple(
                None if s is None else (self.block(s[0])[0], s[1])
                for s in (self.slab(t, j) for j in range(self.places))
            )
            if key not in self.patterns:
                self.patterns.append(key)
            self.pattern_of.append(self.patterns.index(key))

    def slab(self, t, j):
        slot = t + self.tiles * j
        return None if slot >= 2 * self.ex else (slot % self.ex, slot // self.ex)

    def place(self, s, side):
        slot = s + self.ex * side
        return slot % self.tiles, slot // self.tiles

    def block(self, s):
        if s < HALO:
            return 0, self.bx - HALO + s
        if s < HALO + self.bx:
            return 1, s - HALO
        return 2, s - HALO - self.bx


def kernel(
    counts,
    rhs_hbm,
    cond_hbm,
    ext_hbm,
    factor_hbm,
    both_ref,
    R,
    C,
    ext_ref,
    factor_ref,
    e_out,
    e_in,
    z_out,
    z_in,
    early_out,
    early,
    late_out,
    late,
    FL,
    F1,
    FX,
    FY,
    FZ,
    INV,
    C1,
    IC,
    SEC,
    D0,
    W,
    U,
    Q,
    YB,
    EY,
    send_c,
    recv_c,
    send_r,
    recv_r,
    send_e,
    recv_e,
    send_g,
    recv_g,
    load_sem,
):
    sol_ref, res_ref = both_ref.at[0], both_ref.at[1]
    ngx, ngy, ngz = counts
    n = ngx * ngy * ngz
    ix, iy, iz = lax.axis_index("gx"), lax.axis_index("gy"), lax.axis_index("gz")
    me = (ix * ngy + iy) * ngz + iz
    bx, by, bz = sol_ref.shape
    ex, ey = bx + 2 * HALO, by + 2 * HALO
    edge = Edge(bx, bz)
    tiles = edge.tiles
    f32 = jnp.float32
    lo_x, hi_x = HALO, HALO + bx

    def turned(at, step, count):
        moved = at + step
        return jnp.where(moved >= count, moved - count, moved)

    def everyone(act):
        if n <= 64:
            xs = [turned(ix, t, ngx) for t in range(ngx)]
            ys = [turned(iy, t, ngy) for t in range(ngy)]
            zs = [turned(iz, t, ngz) for t in range(ngz)]
            steps = [(a, b, c) for a in range(ngx) for b in range(ngy) for c in range(ngz)]
            steps.sort(
                key=lambda t: -sum(min(a, m - a) for a, m in zip(t, (ngx, ngy, ngz)))
            )
            for a, b, c in steps[:-1]:
                act((xs[a], ys[b], zs[c]))
        else:

            def one(t, carry):
                flat = (me + t) % n
                act((flat // (ngy * ngz), (flat // ngz) % ngy, flat % ngz))
                return carry

            lax.fori_loop(1, n, one, 0)

    core_x, core_y = pl.ds(lo_x, bx), pl.ds(0, by)
    loads = [
        pltpu.make_async_copy(src, dst, load_sem.at[k])
        for k, (src, dst) in enumerate(
            (
                (rhs_hbm, R.at[core_x, core_y]),
                (cond_hbm, C.at[core_x, core_y]),
                (ext_hbm, ext_ref),
                (factor_hbm, factor_ref),
            )
        )
    ]
    for load in loads:
        load.start()

    barrier = pltpu.get_barrier_semaphore()
    everyone(
        lambda device: pl.semaphore_signal(
            barrier, inc=1, device_id=device, device_id_type=MESH
        )
    )

    def inside(d):
        ok = None
        for at, step, count in zip((ix, iy, iz), d, counts):
            if step == 0:
                continue
            here = (at + step >= 0) & (at + step < count)
            ok = here if ok is None else ok & here
        return ok

    def x_from(dx):
        return pl.ds(bx, HALO) if dx == 1 else pl.ds(HALO, bx if dx == 0 else HALO)

    def x_into(dx):
        if dx == 0:
            return pl.ds(HALO, bx)
        return pl.ds(0, HALO) if dx == 1 else pl.ds(hi_x, HALO)

    def y_from(dy):
        return pl.ds(by - HALO, HALO) if dy == 1 else pl.ds(0, by if dy == 0 else HALO)

    def y_into(dy):
        if dy == 0:
            return pl.ds(0, by)
        return pl.ds(by + HALO, HALO) if dy == 1 else pl.ds(by, HALO)

    def landing(f, d):
        dx, dy, dz = d
        if dz != 0:
            return z_in.at[f, 1 if dz == 1 else 0, 1 - dx, y_into(dy)]
        return (R, C)[f].at[x_into(dx), y_into(dy)]

    def remote(src, dst, send, recv, d):
        return pltpu.make_async_remote_copy(
            src_ref=src,
            dst_ref=dst,
            send_sem=send,
            recv_sem=recv,
            device_id=(ix + d[0], iy + d[1], iz + d[2]),
            device_id_type=MESH,
        )

    def copies(f, d):
        dx, dy, dz = d
        k = code(*d)
        if dz != 0:
            src = z_out.at[f, y_from(dy)]
        else:
            src = (R, C)[f].at[x_from(dx), y_from(dy)]
        send, recv = ((send_r, recv_r), (send_c, recv_c))[f]
        out = [remote(src, landing(f, d), send.at[k], recv.at[k], d)]
        if f == 1:
            out.append(remote(e_out, e_in.at[code(-dx, -dy, -dz)], send_e.at[k], recv_e.at[k], d))
        return out

    odd = ix % 2 == 1

    def corner(d):
        return d[0] != 0 and d[1] != 0 and d[2] == 0

    def when_sent(f, act):
        for d in DIRS:

            @pl.when(inside(d))
            def _():
                values, *flags = copies(f, d)
                for c in flags:
                    act(c)
                if not corner(d):
                    act(values)
                    return

                if d[0] == 1:
                    act(values)
                    return

                @pl.when(jnp.logical_not(odd))
                def _():
                    act(values)

    def relayed(f, dy):
        field, k = (R, C)[f], code(-1, dy, 0)
        send, recv = ((send_r, recv_r), (send_c, recv_c))[f]
        return remote(
            field.at[x_from(-1), y_into(dy)],
            field.at[x_into(-1), y_into(dy)],
            send.at[k],
            recv.at[k],
            (-1, 0, 0),
        )

    def start_all(f):
        when_sent(f, lambda c: c.start())

    def relay(f):
        for dy in (-1, 1):

            @pl.when(inside((0, -dy, 0)) & odd)
            def _():
                for c in copies(f, (0, dy, 0)):
                    c.wait_recv()
                relayed(f, dy).start()

    def wait_all(f):
        for d in DIRS:
            ok = inside(tuple(-a for a in d))

            @pl.when(ok & jnp.logical_not(odd) if d[0] == 0 and d[2] == 0 else ok)
            def _():
                for c in copies(f, d):
                    c.wait_recv()

    def wait_sent(f):
        when_sent(f, lambda c: c.wait_send())
        for dy in (-1, 1):

            @pl.when(inside((0, -dy, 0)) & odd)
            def _():
                relayed(f, dy).wait_send()

    for d in DIRS:

        @pl.when(jnp.logical_not(inside(tuple(-a for a in d))))
        def _():
            for f in (0, 1):
                ref = landing(f, d)
                ref[...] = jnp.zeros(ref.shape, f32)
            e_in[code(*(-a for a in d))] = jnp.zeros((1, bz), f32)

    lane = lax.broadcasted_iota(jnp.int32, (ey, bz), 1)
    row = lax.broadcasted_iota(jnp.int32, (ey, bz), 0)
    odd_lane = lane % 2 == 1
    odd_row = (row % 2 == 1).reshape(ey // 8, 8, bz)
    lane_y = lane[:by]

    def up_y(v, k=1):
        return pltpu.roll(v, k, 0)

    def dn_y(v, k=1):
        return pltpu.roll(v, ey - k, 0)

    def spin(v, k):
        k = k % bz
        return v if k == 0 else pltpu.roll(v, k, 1)

    def up_z(v, k=1):
        return pltpu.roll(v, k, 1)

    def dn_z(v, k=1):
        return pltpu.roll(v, bz - k, 1)

    for load in loads[:3]:
        load.wait()
    own_limit = ext_ref[0].astype(f32)
    e_out[...] = jnp.broadcast_to(own_limit, (1, bz))
    for f, field in ((1, C), (0, R)):
        packed = jnp.zeros((by, bz), f32)
        for k in range(bx):
            moved = spin(field[lo_x + k, :by], 2 * HALO * k + HALO)
            packed = jnp.where(lane_y // (2 * HALO) == k, moved, packed)
        z_out[f] = packed

    def total(v):
        return jnp.sum(v, axis=(0, 1), keepdims=True)

    acc = R[lo_x, :by]
    for k in range(1, bx):
        acc = acc + R[lo_x + k, :by]
    m0 = total(jnp.where(lane_y.astype(f32) < own_limit, acc, 0.0))
    early_row = jnp.broadcast_to(m0, (1, bz))
    early_out[...] = early_row
    early[pl.ds(me, 1)] = early_row[None]

    def remote_row(out, into, base, device):
        return pltpu.make_async_remote_copy(
            src_ref=out,
            dst_ref=into.at[me],
            send_sem=send_g.at[base],
            recv_sem=recv_g.at[base],
            device_id=device,
            device_id_type=MESH,
        )

    def spread(out, into, base):
        everyone(lambda device: remote_row(out, into, base, device).start())

    def collect(into, base):
        part = into.at[pl.ds(0, n - 1)]
        pltpu.make_async_copy(part, part, recv_g.at[base]).wait()

    def spread_done(into, base):
        part = into.at[pl.ds(0, n - 1)]
        pltpu.make_async_copy(part, part, send_g.at[base]).wait()

    pl.semaphore_wait(barrier, n - 1)
    start_all(1)
    spread(early_out, early, 0)
    start_all(0)

    loads[3].wait()
    L = factor_ref[...].astype(f32)
    ri = lax.broadcasted_iota(jnp.int32, (n, n), 0)
    ci = lax.broadcasted_iota(jnp.int32, (n, n), 1)
    eye = ri == ci
    X = jnp.where(eye, 1.0 / jnp.where(eye, L, 1.0), 0.0)
    s = 1
    while s < n:
        pick = (ri // (2 * s) == ci // (2 * s)) & (ri % (2 * s) >= s) & (ci % (2 * s) < s)
        low = jnp.where(pick, L, 0.0)
        X = X - jnp.dot(
            X,
            jnp.dot(low, X, precision=HIGH, preferred_element_type=f32),
            precision=HIGH,
            preferred_element_type=f32,
        )
        s *= 2
    inverse = lax.dot_general(
        X, X, (((0,), (0,)), ((), ())), precision=HIGH, preferred_element_type=f32
    )

    one_lane = lax.broadcasted_iota(jnp.int32, (1, bz), 1)
    bands = ((0, by), (1, HALO), (-1, HALO))

    def tables(value):
        rows = {
            (dx, dy, dz): value(dx, dy, dz)
            for dx in (-1, 0, 1)
            for dy in (-1, 0, 1)
            for dz in (-1, 0, 1)
        }
        out = [
            jnp.concatenate(
                [jnp.broadcast_to(rows[dx, dy, 0], (count, bz)) for dy, count in bands], axis=0
            )
            for dx in (-1, 0, 1)
        ]
        for pattern in edge.patterns:
            parts = []
            for dy, count in bands:
                line = None
                for j, key in enumerate(pattern):
                    if key is None:
                        continue
                    dx, start = key[0] - 1, GROUP * j
                    if key[1] == 0:
                        here = jnp.where(
                            one_lane < start + HALO, rows[dx, dy, -1], rows[dx, dy, 0]
                        )
                    else:
                        here = jnp.where(
                            one_lane < start + 2 * HALO, rows[dx, dy, 0], rows[dx, dy, 1]
                        )
                    line = here if line is None else jnp.where(one_lane >= start, here, line)
                parts.append(jnp.broadcast_to(line, (count, bz)))
            out.append(jnp.concatenate(parts, axis=0))
        return out

    def depths():
        plain = one_lane
        out = [plain] * 3
        for pattern in edge.patterns:
            line = None
            for j, key in enumerate(pattern):
                off = one_lane - GROUP * j
                if key is None:
                    here = jnp.full((1, bz), bz, jnp.int32)
                elif key[1] == 0:
                    here = jnp.where(off < HALO, off + bz - HALO, off - HALO)
                else:
                    here = jnp.where(off < 2 * HALO, off + bz - 2 * HALO, off - 2 * HALO)
                line = here if line is None else jnp.where(off >= 0, here, line)
            line = jnp.where(one_lane >= GROUP * edge.places, bz, line)
            out.append(line)
        return out

    def flag_of(i):
        return edge.block(i)[0] if i < ex else 3 + edge.pattern_of[i - ex]

    def build_edges(f, field, group):
        moved = {}
        for t in group:
            for j in range(edge.places):
                slab = edge.slab(t, j)
                if slab is None:
                    continue
                s, side = slab
                which, k = edge.block(s)
                start, at = GROUP * j, 2 * HALO * k
                if side == 0:
                    own = spin(field[s], start + HALO)
                    far = spin(z_in[f, 1, which], start - at)
                else:
                    own = spin(field[s], start + 2 * HALO - bz)
                    far = spin(z_in[f, 0, which], start + HALO - at)
                moved[t, j] = own, far
        yield
        for t in group:
            acc = None
            for j in range(edge.places):
                start = GROUP * j
                if (t, j) not in moved:
                    acc = jnp.where(lane >= start, 0.0, acc)
                    break
                own, far = moved[t, j]
                if edge.slab(t, j)[1] == 0:
                    here = jnp.where(lane < start + HALO, far, own)
                else:
                    here = jnp.where(lane < start + 2 * HALO, own, far)
                acc = here if acc is None else jnp.where(lane >= start, here, acc)
            field[ex + t] = jnp.where(lane < GROUP * edge.places, acc, 0.0)

    def pair_y(v):
        rows = v.reshape(ey // 8, 8, bz)
        swapped = jnp.where(odd_row, pltpu.roll(rows, 1, 1), pltpu.roll(rows, 7, 1))
        return (rows + swapped).reshape(ey, bz)

    def groups(lo, hi, span=SPAN):
        out = []
        for a, b in ((lo, hi), (ex, ex + tiles)):
            at = a
            while at < b:
                stop = min(b, at + span)
                out.append(list(range(at, stop)))
                at = stop
        return out

    def around(i):
        last = ex + tiles - 1
        before = (last, GROUP) if i == ex else (i - 1, 0)
        after = (ex, -GROUP) if i == last else (i + 1, 0)
        return before, after

    def faces(load, group):
        v, turned_v = {}, {}
        for i in group:
            v[i] = load(i)
        for at, k in (around(group[0])[0], around(group[-1])[1]):
            turned_v[at, k] = v[at] if k == 0 and at in v else spin(load(at), k)
        up = {i: up_z(v[i]) for i in group}
        yield
        gz, dn = {}, {}
        for i in group:
            gz[i] = FZ[i] * (v[i] - up[i])
            dn[i] = dn_z(gz[i])
        yield
        out = {}
        (b, kb), _ = around(group[0])
        gx = FX[group[0]] * (v[group[0]] - turned_v[b, kb])
        for i in group:
            if i == group[-1]:
                a, ka = around(i)[1]
                after = turned_v[a, ka]
            else:
                after = v[i + 1]
            gx_next = FX[i + 1] * (after - v[i])
            gy = FY[i] * (v[i] - up_y(v[i]))
            out[i] = (v[i], (gx - gx_next) + ((gy - dn_y(gy)) + (gz[i] - dn[i])))
            gx = gx_next
        return out

    def reads(name, group):
        return {(name, i) for i in group} | {
            (name, around(group[0])[0][0]),
            (name, around(group[-1])[1][0]),
        }

    def run(items):
        done, open_items, at = set(), [], 0
        while at < len(items) or open_items:
            still = []
            for gen, gives in open_items:
                try:
                    next(gen)
                    still.append((gen, gives))
                except StopIteration:
                    done |= gives
            open_items = still
            if not open_items and at < len(items):
                assert items[at][1] <= done, items[at][1] - done
            if at < len(items) and items[at][1] <= done:
                gen, _, gives = items[at]
                at += 1
                try:
                    next(gen)
                    open_items.append((gen, gives))
                except StopIteration:
                    done |= gives

    relay(1)
    wait_all(1)
    relay(0)

    def limit(dx, dy, dz):
        return e_out[...] if (dx, dy, dz) == (0, 0, 0) else e_in[code(dx, dy, dz)]

    for k, (a, z) in enumerate(zip(tables(limit), depths())):
        z_f, even_f = z.astype(f32), (z - z % 2).astype(f32)
        FL[k] = (z_f < a).astype(f32)
        F1[k] = (even_f < a).astype(f32)

    items = []
    pairs, edge_pairs = ex // 2, tiles // 2
    last_pair = pairs + edge_pairs - 1

    def make_faces(group):
        up = {i: up_z(C[i]) for i in group}
        (b, kb), _ = around(group[0])
        before = None if group[0] == 0 else spin(C[b], kb)
        yield
        for i in group:
            c = C[i]
            if before is not None:
                FX[i] = 0.5 * (before + c)
            before = c
            FY[i] = 0.5 * (c + up_y(c))
            FZ[i] = 0.5 * (c + up[i])

    def make_wrap():
        around_face = spin(FX[ex], -GROUP)
        yield
        FX[ex + tiles] = around_face

    def make_inverse(group):
        dn = {i: dn_z(FZ[i]) for i in group}
        yield
        for i in group:
            fy = FY[i]
            diagonal = (FX[i] + FX[i + 1]) + (fy + dn_y(fy)) + (FZ[i] + dn[i])
            fl = FL[flag_of(i)]
            INV[i] = OMEGA * fl / (diagonal + 1.0 - fl)

    def make_pooled(group):
        pooled = {}
        for q in group:
            v = pair_y(C[2 * q] + C[2 * q + 1])
            pooled[q] = v, up_z(v), dn_z(v)
        yield
        for q in group:
            v, up, dn = pooled[q]
            C1[q] = (v + jnp.where(odd_lane, up, dn)) * 0.125

    def beside(q):
        before = (last_pair, GROUP) if q == pairs else (q - 1, 0)
        after = (pairs, -GROUP) if q == last_pair else (q + 1, 0)
        return before, after

    def make_coarse_inverse(group):
        found = {}
        for q in group:
            c = C1[q]
            (b, kb), (a, ka) = beside(q)
            found[q] = up_z(c, 2), dn_z(c, 2), spin(C1[b], kb), spin(C1[a], ka)
        yield
        for q in group:
            c = C1[q]
            up, dn, before, after = found[q]
            diagonal = 3.0 * c + 0.5 * ((before + after) + (up_y(c, 2) + dn_y(c, 2)) + (up + dn))
            fl = F1[flag_of(2 * q)]
            IC[q] = OMEGA * fl / (4.0 * diagonal + 1.0 - fl)

    def cut(lo, hi, span):
        return [list(range(a, min(hi, a + span))) for a in range(lo, hi, span)]

    def named(name, these):
        return {(name, i) for i in these}

    def face_items(lo, hi, needs):
        return [
            (make_faces(g), needs if lo < ex else named("c", range(tiles)), named("f", g))
            for g in cut(lo, hi, WIDE)
        ]

    def inverse_items(lo, hi):
        return [
            (make_inverse(g), named("f", g + [g[-1] + 1]), named("i", g)) for g in cut(lo, hi, WIDE)
        ]

    def pooled_items(lo, hi):
        needs = set() if lo < pairs else named("c", range(tiles))
        return [(make_pooled(g), needs, named("p", g)) for g in cut(lo, hi, WIDE // 2)]

    def coarse_items(lo, hi):
        return [
            (
                make_coarse_inverse(g),
                named("p", [at for q in g for at, _ in beside(q)] + g),
                named("n", g),
            )
            for g in cut(lo, hi, WIDE // 2)
        ]

    def edge_items(f, name):
        field = (R, C)[f]
        return [
            (build_edges(f, field, g), set() if f else {"arrived"}, named(name, g))
            for g in cut(0, tiles, EDGES)
        ]

    def mixed(*lists):
        out, lists = [], [list(x) for x in lists]
        while any(lists):
            for x in lists:
                if x:
                    out.append(x.pop(0))
        return out

    def arrive():
        wait_all(0)
        yield

    items += mixed(
        edge_items(1, "c"),
        face_items(0, ex, set()) + inverse_items(1, ex - 1),
        pooled_items(0, pairs) + coarse_items(1, pairs - 1),
    )
    items.append((arrive(), set(), {"arrived"}))
    items += mixed(
        edge_items(0, "r"),
        face_items(ex, ex + tiles, None)
        + [(make_wrap(), named("f", [ex]), named("f", [ex + tiles]))]
        + inverse_items(ex, ex + tiles),
        pooled_items(pairs, pairs + edge_pairs) + coarse_items(pairs, pairs + edge_pairs),
    )

    off = lane_y % GROUP
    slot0 = (lane_y // GROUP) * tiles

    def core_edge(t, lo_off, hi_off):
        slot = slot0 + t
        low = (slot >= lo_x) & (slot < hi_x) & lo_off
        high = (slot >= ex + lo_x) & (slot < ex + hi_x) & hi_off
        return (low | high) & (lane_y < GROUP * edge.places)

    core_off = (off >= HALO) & (off < 2 * HALO)
    core_tiles = [core_edge(t, core_off, core_off) for t in range(tiles)]
    core_lanes = (lane_y >= HALO) & (lane_y < bz - HALO)

    zeros = jnp.zeros((by, bz), f32)
    scalars = 8
    width = late.shape[-1]
    base = scalars if width == bz else bz
    col = lax.broadcasted_iota(jnp.int32, (1, width), 1)
    coupling = {}

    def couple():
        flux_z = FZ[lo_x, :by]
        flux_y = FY[lo_x]
        for i in range(lo_x + 1, hi_x):
            flux_z = flux_z + FZ[i, :by]
            flux_y = flux_y + FY[i]
        fl = FL[1]
        fl_up, fl_core = up_y(fl), fl[:by]
        step = fl_core - up_z(fl)[:by]
        inner = jnp.where(lane_y >= 1, flux_z * (step * step), 0.0)
        none = jnp.logical_and(off < 0, off >= 0)
        low_face = [core_edge(t, off == HALO, none) for t in range(tiles)]
        high_face = [core_edge(t, none, off == 2 * HALO) for t in range(tiles)]
        sides = {}

        def put(d, alone, shared):
            sides[d] = (total(alone), total(shared))

        alone = FX[lo_x, :by] * fl_core
        put((-1, 0, 0), alone, alone * FL[0, :by])
        alone = FX[hi_x, :by] * fl_core
        put((1, 0, 0), alone, alone * FL[2, :by])
        alone = jnp.where(row == 0, flux_y * fl, 0.0)
        put((0, -1, 0), alone, alone * fl_up)
        alone = jnp.where(row == by, flux_y * fl_up, 0.0)
        put((0, 1, 0), alone, alone * fl)
        parts = [zeros] * 4
        for t in range(tiles):
            f_edge = FL[3 + edge.pattern_of[t]]
            f_here, f_up = f_edge[:by], up_z(f_edge)[:by]
            fz = FZ[ex + t, :by]
            a = jnp.where(low_face[t], fz * f_here, 0.0)
            b = jnp.where(high_face[t], fz * f_up, 0.0)
            parts = [parts[0] + a, parts[1] + a * f_up, parts[2] + b, parts[3] + b * f_here]
        put((0, 0, -1), parts[0], parts[1])
        put((0, 0, 1), parts[2], parts[3])

        inner_sum = total(inner)
        yield
        yield
        diagonal = inner_sum
        late_row = jnp.zeros((1, width), f32)
        for (dx, dy, dz), (alone, shared) in sides.items():
            diagonal = diagonal + alone
            other = ((ix + dx) * ngy + iy + dy) * ngz + iz + dz
            valid = inside((dx, dy, dz))
            late_row = late_row - jnp.where((col == base + other) & valid, shared, 0.0)
        late_row = late_row + jnp.where(col == base + me, diagonal, 0.0)
        coupling[0] = late_row


    def solve(means):
        y_row = jnp.sum(inverse * means, axis=0, keepdims=True)
        y_col = jnp.sum(jnp.where(eye, y_row, 0.0), axis=1, keepdims=True)
        return y_row, y_col

    def block_row(dx, dy, dz):
        def near(at, step, count):
            return jnp.clip(at + step, 0, count - 1)

        b = (near(ix, dx, ngx) * ngy + near(iy, dy, ngy)) * ngz + near(iz, dz, ngz)
        return YB[pl.ds(b, 1)]

    def spread_blocks(y_col):
        YB[...] = jnp.broadcast_to(y_col, (n, bz))
        for k, v in enumerate(tables(block_row)):
            EY[k] = FL[k] * v

    cells = bx * by * bz

    def first_solve():
        collect(early, 0)
        m0_col = early[:, 0, 0:1]
        yield
        y_row = jnp.sum(inverse * (m0_col * (1.0 / cells)), axis=0, keepdims=True)
        yield
        y_col = jnp.sum(jnp.where(eye, y_row, 0.0), axis=1, keepdims=True)
        yield
        yield
        spread_blocks(y_col)

    items.append((first_solve(), set(), {"blocks"}))
    sums = [[zeros, zeros] for _ in range(7)]
    parts = {}

    def add(i, k, v):
        if i < ex:
            if lo_x <= i < hi_x:
                sums[k][0] = sums[k][0] + v
        else:
            sums[k][1] = sums[k][1] + jnp.where(core_tiles[i - ex], v, 0.0)

    def coarse(field, group):
        found = yield from faces(lambda i: INV[i] * field[i], group)
        pooled = {}
        for i in group[::2]:
            gap = FL[flag_of(i)] * (field[i] - found[i][1])
            gap = gap + FL[flag_of(i + 1)] * (field[i + 1] - found[i + 1][1])
            gap = pair_y(gap)
            pooled[i] = (gap, up_z(gap), dn_z(gap))
        yield
        for i in group[::2]:
            gap, up, dn = pooled[i]
            below = IC[i // 2] * (gap + jnp.where(odd_lane, up, dn))
            for at in (i, i + 1):
                SEC[at] = found[at][0] + FL[flag_of(at)] * below

    def smooth(field, group, keep):
        found = yield from faces(lambda i: SEC[i], group)
        for i in group:
            v, lv = found[i]
            keep(i, v + INV[i] * (field[i] - lv))

    def image(load, group, keep):
        found = yield from faces(load, group)
        for i in group:
            keep(i, *found[i])

    def add_cycle(field, source, name, lo, hi, keep, extra):
        even, stop = (lo - 1) // 2 * 2, (hi + 2) // 2 * 2
        for group in groups(even, stop):
            if source is None:
                needs = {(k, at) for k in "fi" for _, at in reads("i", group)}
                needs |= named("n", [i // 2 for i in group]) | {"arrived"}
                needs |= named("r", range(tiles)) if group[0] >= ex else set()
            else:
                needs = reads(source, group)
            items.append((coarse(field, group), needs, {(name + "s", i) for i in group}))
        for group in groups(lo, hi):
            needs = reads(name + "s", group) | extra
            items.append((smooth(field, group, keep), needs, {(name, i) for i in group}))

    def keep_direction(i, v):
        D0[i] = v + EY[flag_of(i)]

    def keep_image(i, v, lv):
        w = FL[flag_of(i)] * lv
        W[i] = w
        add(i, 0, R[i, :by] * v[:by])
        add(i, 1, w[:by] * v[:by])
        add(i, 2, w[:by])

    def keep_second(i, v):
        U[i] = v
        add(i, 3, W[i, :by] * v[:by])
        add(i, 4, R[i, :by] * v[:by])

    def keep_third(i, v, lv):
        q = FL[flag_of(i)][:by] * lv[:by]
        Q[i, :by] = q
        add(i, 5, q * v[:by])
        add(i, 6, q)

    def gather_sums(which):
        for k in which:
            a, b = sums[k]
            parts[k] = total(jnp.where(core_lanes, a, 0.0) + b)
        yield

    def core_of(name):
        return {(name, i) for i in range(lo_x, hi_x)} | {(name, ex + t) for t in range(tiles)}

    add_cycle(R, None, "d", 4, ex - 4, keep_direction, {"blocks"})
    for group in groups(5, ex - 5):
        items.append(
            (image(lambda i: D0[i], group, keep_image), reads("d", group), {("w", i) for i in group})
        )
    add_cycle(W, "w", "u", 7, ex - 7, keep_second, set())
    items.append((couple(), set(), set()))
    items.append((gather_sums(range(3)), core_of("w"), set()))
    for group in groups(lo_x, hi_x):
        items.append(
            (image(lambda i: U[i], group, keep_third), reads("u", group), {("q", i) for i in group})
        )
    items.append((gather_sums(range(3, 5)), core_of("u"), set()))
    items.append((gather_sums(range(5, 7)), core_of("q"), set()))
    run(items)

    late_row = coupling[0]
    for k in range(7):
        late_row = jnp.where(col == k, parts[k], late_row)
    late_row = jnp.where(col == 7, m0, late_row)
    late_out[...] = late_row
    late[pl.ds(me, 1)] = late_row[None]
    spread(late_out, late, 1)
    wait_sent(1)
    wait_sent(0)
    collect(late, 1)

    rows = late[:, 0, :]
    y_row, y_col = solve(rows[:, 2:3] * (1.0 / cells))
    spread_blocks(y_col)
    plain = jnp.sum(rows, axis=0, keepdims=True)
    weighted = jnp.sum(rows * y_col, axis=0, keepdims=True)

    def pick(line, k):
        return jnp.sum(line[:, k : k + 1], axis=(0, 1), keepdims=True)

    rz, dad = pick(plain, 0), pick(plain, 1)
    w_u = pick(plain, 3) + pick(weighted, 2)
    r_u = pick(plain, 4) + pick(weighted, 7)
    u_q = (
        pick(plain, 5)
        + 2.0 * pick(weighted, 6)
        + total(weighted[:, base : base + n] * y_row)
    )
    alpha = rz / dad
    new = (rz - alpha * dad) + alpha * (alpha * w_u - r_u)
    beta = new / rz
    grow = 1.0 + beta
    dad1 = grow * grow * dad - 2.0 * alpha * grow * w_u + alpha * alpha * u_q
    alpha1 = new / dad1
    c1 = alpha + alpha1 * grow
    c2 = alpha * alpha1

    def results(i, v, lv):
        fl = FL[flag_of(i)][:by]
        sol = c1 * D0[i, :by] - c2 * (U[i, :by] + v[:by])
        res = fl * R[i, :by] - c1 * W[i, :by] + c2 * (Q[i, :by] + fl * lv[:by])
        if i < ex:
            sol_ref[i - lo_x], res_ref[i - lo_x] = sol, res
        else:
            SEC[i, :by], INV[i, :by] = sol, res

    run(
        [
            (image(lambda i: EY[flag_of(i)], group, results), set(), set())
            for group in groups(lo_x, hi_x)
        ]
    )
    for x in range(bx):
        tl, jl = edge.place(lo_x + x, 0)
        th, jh = edge.place(lo_x + x, 1)
        for ref, held in ((sol_ref, SEC), (res_ref, INV)):
            low = spin(held[ex + tl, :by], -(GROUP * jl + HALO))
            high = spin(held[ex + th, :by], bz - HALO - (GROUP * jh + HALO))
            ref[x] = jnp.where(
                lane_y < HALO, low, jnp.where(lane_y >= bz - HALO, high, ref[x])
            )
    spread_done(early, 0)
    spread_done(late, 1)


def solution(mesh):
    counts = (mesh.shape["gx"], mesh.shape["gy"], mesh.shape["gz"])
    n = counts[0] * counts[1] * counts[2]

    def on_device(right_side, conductance, extents, coarse_factor):
        f32 = jnp.float32
        bx, by, bz = right_side.shape
        ex, ey = bx + 2 * HALO, by + 2 * HALO
        edge = Edge(bx, bz)
        slabs = ex + edge.tiles
        width = bz if n + 8 <= bz else bz + -(-n // 128) * 128
        vm = lambda *shape: pltpu.VMEM(shape, f32)
        field = vm(slabs, ey, bz)
        half = vm(slabs // 2, ey, bz)
        flags = vm(3 + len(edge.patterns), ey, bz)
        dma = pltpu.SemaphoreType.DMA
        scratch = [
            field,
            field,
            pltpu.VMEM(extents.shape, extents.dtype),
            pltpu.VMEM(coarse_factor.shape, coarse_factor.dtype),
            vm(1, bz),
            vm(27, 1, bz),
            vm(2, by, bz),
            vm(2, 2, 3, ey, bz),
            vm(1, bz),
            vm(n, 1, bz),
            vm(1, width),
            vm(n, 1, width),
            flags,
            flags,
            vm(slabs + 1, ey, bz),
            field,
            field,
            field,
            half,
            half,
            field,
            field,
            field,
            field,
            field,
            vm(n, bz),
            flags,
            dma((27,)),
            dma((27,)),
            dma((27,)),
            dma((27,)),
            dma((27,)),
            dma((27,)),
            dma((2,)),
            dma((2,)),
            dma((4,)),
        ]
        whole = pl.BlockSpec(memory_space=pltpu.VMEM)
        outer = pl.BlockSpec(memory_space=pltpu.HBM)
        both = pl.pallas_call(
            functools.partial(kernel, counts),
            out_shape=vm(2, bx, by, bz),
            in_specs=[outer, outer, outer, outer],
            out_specs=whole,
            scratch_shapes=scratch,
            compiler_params=pltpu.CompilerParams(
                collective_id=0, has_side_effects=True, vmem_limit_bytes=60000000
            ),
        )(right_side, conductance, extents, coarse_factor)
        return both[0], both[1]

    in_specs = (P("gx", "gy", "gz"), P("gx", "gy", "gz"), P("gx", "gy", "gz"), P())
    out_specs = (P("gx", "gy", "gz"), P("gx", "gy", "gz"))
    return jax.shard_map(
        on_device, mesh=mesh, in_specs=in_specs, out_specs=out_specs, check_vma=False
    )
```

```python
import functools

import jax
import jax.numpy as jnp
from jax import lax
from jax.experimental import pallas as pl
from jax.experimental.pallas import tpu as pltpu
from jax.sharding import PartitionSpec as P

OMEGA = 0.8
HALO = 8
GROUP = 3 * HALO
SPAN = 24
WIDE = 12
EDGES = 2
MESH = pl.DeviceIdType.MESH
HIGH = lax.Precision.HIGHEST
DIRS = [
    (dx, dy, dz)
    for dx in (-1, 0, 1)
    for dy in (-1, 0, 1)
    for dz in (-1, 0, 1)
    if (dx, dy, dz) != (0, 0, 0)
]
DIRS.sort(key=lambda d: -sum(abs(a) for a in d))


def code(dx, dy, dz):
    return (dx + 1) * 9 + (dy + 1) * 3 + dz + 1


class Edge:
    def __init__(self, bx, bz):
        self.bx, self.ex = bx, bx + 2 * HALO
        self.places = bz // GROUP
        tiles = -(-2 * self.ex // self.places)
        self.tiles = tiles + tiles % 2
        self.patterns, self.pattern_of = [], []
        for t in range(self.tiles):
            key = tuple(
                None if s is None else (self.block(s[0])[0], s[1])
                for s in (self.slab(t, j) for j in range(self.places))
            )
            if key not in self.patterns:
                self.patterns.append(key)
            self.pattern_of.append(self.patterns.index(key))

    def slab(self, t, j):
        slot = t + self.tiles * j
        return None if slot >= 2 * self.ex else (slot % self.ex, slot // self.ex)

    def place(self, s, side):
        slot = s + self.ex * side
        return slot % self.tiles, slot // self.tiles

    def block(self, s):
        if s < HALO:
            return 0, self.bx - HALO + s
        if s < HALO + self.bx:
            return 1, s - HALO
        return 2, s - HALO - self.bx


def kernel(
    counts,
    rhs_hbm,
    cond_hbm,
    ext_hbm,
    factor_hbm,
    both_ref,
    R,
    C,
    ext_ref,
    factor_ref,
    e_out,
    e_in,
    z_out,
    z_in,
    early_out,
    early,
    late_out,
    late,
    FL,
    F1,
    FX,
    FY,
    FZ,
    INV,
    C1,
    IC,
    SEC,
    D0,
    W,
    U,
    Q,
    YB,
    EY,
    send_c,
    recv_c,
    send_r,
    recv_r,
    send_e,
    recv_e,
    send_g,
    recv_g,
    load_sem,
):
    sol_ref, res_ref = both_ref.at[0], both_ref.at[1]
    ngx, ngy, ngz = counts
    n = ngx * ngy * ngz
    ix, iy, iz = lax.axis_index("gx"), lax.axis_index("gy"), lax.axis_index("gz")
    me = (ix * ngy + iy) * ngz + iz
    bx, by, bz = sol_ref.shape
    ex, ey = bx + 2 * HALO, by + 2 * HALO
    edge = Edge(bx, bz)
    tiles = edge.tiles
    f32 = jnp.float32
    lo_x, hi_x = HALO, HALO + bx

    def turned(at, step, count):
        moved = at + step
        return jnp.where(moved >= count, moved - count, moved)

    def everyone(act):
        if n <= 64:
            xs = [turned(ix, t, ngx) for t in range(ngx)]
            ys = [turned(iy, t, ngy) for t in range(ngy)]
            zs = [turned(iz, t, ngz) for t in range(ngz)]
            steps = [(a, b, c) for a in range(ngx) for b in range(ngy) for c in range(ngz)]
            steps.sort(
                key=lambda t: -sum(min(a, m - a) for a, m in zip(t, (ngx, ngy, ngz)))
            )
            for a, b, c in steps[:-1]:
                act((xs[a], ys[b], zs[c]))
        else:

            def one(t, carry):
                flat = (me + t) % n
                act((flat // (ngy * ngz), (flat // ngz) % ngy, flat % ngz))
                return carry

            lax.fori_loop(1, n, one, 0)

    core_x, core_y = pl.ds(lo_x, bx), pl.ds(0, by)
    loads = [
        pltpu.make_async_copy(src, dst, load_sem.at[k])
        for k, (src, dst) in enumerate(
            (
                (rhs_hbm, R.at[core_x, core_y]),
                (cond_hbm, C.at[core_x, core_y]),
                (ext_hbm, ext_ref),
                (factor_hbm, factor_ref),
            )
        )
    ]
    for load in loads:
        load.start()

    barrier = pltpu.get_barrier_semaphore()
    everyone(
        lambda device: pl.semaphore_signal(
            barrier, inc=1, device_id=device, device_id_type=MESH
        )
    )

    def inside(d):
        ok = None
        for at, step, count in zip((ix, iy, iz), d, counts):
            if step == 0:
                continue
            here = (at + step >= 0) & (at + step < count)
            ok = here if ok is None else ok & here
        return ok

    def x_from(dx):
        return pl.ds(bx, HALO) if dx == 1 else pl.ds(HALO, bx if dx == 0 else HALO)

    def x_into(dx):
        if dx == 0:
            return pl.ds(HALO, bx)
        return pl.ds(0, HALO) if dx == 1 else pl.ds(hi_x, HALO)

    def y_from(dy):
        return pl.ds(by - HALO, HALO) if dy == 1 else pl.ds(0, by if dy == 0 else HALO)

    def y_into(dy):
        if dy == 0:
            return pl.ds(0, by)
        return pl.ds(by + HALO, HALO) if dy == 1 else pl.ds(by, HALO)

    def landing(f, d):
        dx, dy, dz = d
        if dz != 0:
            return z_in.at[f, 1 if dz == 1 else 0, 1 - dx, y_into(dy)]
        return (R, C)[f].at[x_into(dx), y_into(dy)]

    def remote(src, dst, send, recv, d):
        return pltpu.make_async_remote_copy(
            src_ref=src,
            dst_ref=dst,
            send_sem=send,
            recv_sem=recv,
            device_id=(ix + d[0], iy + d[1], iz + d[2]),
            device_id_type=MESH,
        )

    def copies(f, d):
        dx, dy, dz = d
        k = code(*d)
        if dz != 0:
            src = z_out.at[f, y_from(dy)]
        else:
            src = (R, C)[f].at[x_from(dx), y_from(dy)]
        send, recv = ((send_r, recv_r), (send_c, recv_c))[f]
        out = [remote(src, landing(f, d), send.at[k], recv.at[k], d)]
        if f == 1:
            out.append(remote(e_out, e_in.at[code(-dx, -dy, -dz)], send_e.at[k], recv_e.at[k], d))
        return out

    odd = ix % 2 == 1

    def corner(d):
        return d[0] != 0 and d[1] != 0 and d[2] == 0

    def when_sent(f, act):
        for d in DIRS:

            @pl.when(inside(d))
            def _():
                values, *flags = copies(f, d)
                for c in flags:
                    act(c)
                if not corner(d):
                    act(values)
                    return

                if d[0] == 1:
                    act(values)
                    return

                @pl.when(jnp.logical_not(odd))
                def _():
                    act(values)

    def relayed(f, dy):
        field, k = (R, C)[f], code(-1, dy, 0)
        send, recv = ((send_r, recv_r), (send_c, recv_c))[f]
        return remote(
            field.at[x_from(-1), y_into(dy)],
            field.at[x_into(-1), y_into(dy)],
            send.at[k],
            recv.at[k],
            (-1, 0, 0),
        )

    def start_all(f):
        when_sent(f, lambda c: c.start())

    def relay(f):
        for dy in (-1, 1):

            @pl.when(inside((0, -dy, 0)) & odd)
            def _():
                for c in copies(f, (0, dy, 0)):
                    c.wait_recv()
                relayed(f, dy).start()

    def wait_all(f):
        for d in DIRS:
            ok = inside(tuple(-a for a in d))

            @pl.when(ok & jnp.logical_not(odd) if d[0] == 0 and d[2] == 0 else ok)
            def _():
                for c in copies(f, d):
                    c.wait_recv()

    def wait_sent(f):
        when_sent(f, lambda c: c.wait_send())
        for dy in (-1, 1):

            @pl.when(inside((0, -dy, 0)) & odd)
            def _():
                relayed(f, dy).wait_send()

    for d in DIRS:

        @pl.when(jnp.logical_not(inside(tuple(-a for a in d))))
        def _():
            for f in (0, 1):
                ref = landing(f, d)
                ref[...] = jnp.zeros(ref.shape, f32)
            e_in[code(*(-a for a in d))] = jnp.zeros((1, bz), f32)

    lane = lax.broadcasted_iota(jnp.int32, (ey, bz), 1)
    row = lax.broadcasted_iota(jnp.int32, (ey, bz), 0)
    odd_lane = lane % 2 == 1
    odd_row = (row % 2 == 1).reshape(ey // 8, 8, bz)
    lane_y = lane[:by]

    def up_y(v, k=1):
        return pltpu.roll(v, k, 0)

    def dn_y(v, k=1):
        return pltpu.roll(v, ey - k, 0)

    def spin(v, k):
        k = k % bz
        return v if k == 0 else pltpu.roll(v, k, 1)

    def up_z(v, k=1):
        return pltpu.roll(v, k, 1)

    def dn_z(v, k=1):
        return pltpu.roll(v, bz - k, 1)

    for load in loads[:3]:
        load.wait()
    own_limit = ext_ref[0].astype(f32)
    e_out[...] = jnp.broadcast_to(own_limit, (1, bz))
    for f, field in ((1, C), (0, R)):
        packed = jnp.zeros((by, bz), f32)
        for k in range(bx):
            moved = spin(field[lo_x + k, :by], 2 * HALO * k + HALO)
            packed = jnp.where(lane_y // (2 * HALO) == k, moved, packed)
        z_out[f] = packed

    def total(v):
        return jnp.sum(v, axis=(0, 1), keepdims=True)

    acc = R[lo_x, :by]
    for k in range(1, bx):
        acc = acc + R[lo_x + k, :by]
    m0 = total(jnp.where(lane_y.astype(f32) < own_limit, acc, 0.0))
    early_row = jnp.broadcast_to(m0, (1, bz))
    early_out[...] = early_row
    early[pl.ds(me, 1)] = early_row[None]

    def remote_row(out, into, base, device):
        return pltpu.make_async_remote_copy(
            src_ref=out,
            dst_ref=into.at[me],
            send_sem=send_g.at[base],
            recv_sem=recv_g.at[base],
            device_id=device,
            device_id_type=MESH,
        )

    def spread(out, into, base):
        everyone(lambda device: remote_row(out, into, base, device).start())

    def collect(into, base):
        part = into.at[pl.ds(0, n - 1)]
        pltpu.make_async_copy(part, part, recv_g.at[base]).wait()

    def spread_done(into, base):
        part = into.at[pl.ds(0, n - 1)]
        pltpu.make_async_copy(part, part, send_g.at[base]).wait()

    pl.semaphore_wait(barrier, n - 1)
    start_all(1)
    spread(early_out, early, 0)
    start_all(0)

    loads[3].wait()
    L = factor_ref[...].astype(f32)
    ri = lax.broadcasted_iota(jnp.int32, (n, n), 0)
    ci = lax.broadcasted_iota(jnp.int32, (n, n), 1)
    eye = ri == ci
    X = jnp.where(eye, 1.0 / jnp.where(eye, L, 1.0), 0.0)
    s = 1
    while s < n:
        pick = (ri // (2 * s) == ci // (2 * s)) & (ri % (2 * s) >= s) & (ci % (2 * s) < s)
        low = jnp.where(pick, L, 0.0)
        X = X - jnp.dot(
            X,
            jnp.dot(low, X, precision=HIGH, preferred_element_type=f32),
            precision=HIGH,
            preferred_element_type=f32,
        )
        s *= 2
    inverse = lax.dot_general(
        X, X, (((0,), (0,)), ((), ())), precision=HIGH, preferred_element_type=f32
    )

    one_lane = lax.broadcasted_iota(jnp.int32, (1, bz), 1)
    bands = ((0, by), (1, HALO), (-1, HALO))

    def tables(value):
        rows = {
            (dx, dy, dz): value(dx, dy, dz)
            for dx in (-1, 0, 1)
            for dy in (-1, 0, 1)
            for dz in (-1, 0, 1)
        }
        out = [
            jnp.concatenate(
                [jnp.broadcast_to(rows[dx, dy, 0], (count, bz)) for dy, count in bands], axis=0
            )
            for dx in (-1, 0, 1)
        ]
        for pattern in edge.patterns:
            parts = []
            for dy, count in bands:
                line = None
                for j, key in enumerate(pattern):
                    if key is None:
                        continue
                    dx, start = key[0] - 1, GROUP * j
                    if key[1] == 0:
                        here = jnp.where(
                            one_lane < start + HALO, rows[dx, dy, -1], rows[dx, dy, 0]
                        )
                    else:
                        here = jnp.where(
                            one_lane < start + 2 * HALO, rows[dx, dy, 0], rows[dx, dy, 1]
                        )
                    line = here if line is None else jnp.where(one_lane >= start, here, line)
                parts.append(jnp.broadcast_to(line, (count, bz)))
            out.append(jnp.concatenate(parts, axis=0))
        return out

    def depths():
        plain = one_lane
        out = [plain] * 3
        for pattern in edge.patterns:
            line = None
            for j, key in enumerate(pattern):
                off = one_lane - GROUP * j
                if key is None:
                    here = jnp.full((1, bz), bz, jnp.int32)
                elif key[1] == 0:
                    here = jnp.where(off < HALO, off + bz - HALO, off - HALO)
                else:
                    here = jnp.where(off < 2 * HALO, off + bz - 2 * HALO, off - 2 * HALO)
                line = here if line is None else jnp.where(off >= 0, here, line)
            line = jnp.where(one_lane >= GROUP * edge.places, bz, line)
            out.append(line)
        return out

    def flag_of(i):
        return edge.block(i)[0] if i < ex else 3 + edge.pattern_of[i - ex]

    def build_edges(f, field, group):
        moved = {}
        for t in group:
            for j in range(edge.places):
                slab = edge.slab(t, j)
                if slab is None:
                    continue
                s, side = slab
                which, k = edge.block(s)
                start, at = GROUP * j, 2 * HALO * k
                if side == 0:
                    own = spin(field[s], start + HALO)
                    far = spin(z_in[f, 1, which], start - at)
                else:
                    own = spin(field[s], start + 2 * HALO - bz)
                    far = spin(z_in[f, 0, which], start + HALO - at)
                moved[t, j] = own, far
        yield
        for t in group:
            acc = None
            for j in range(edge.places):
                start = GROUP * j
                if (t, j) not in moved:
                    acc = jnp.where(lane >= start, 0.0, acc)
                    break
                own, far = moved[t, j]
                if edge.slab(t, j)[1] == 0:
                    here = jnp.where(lane < start + HALO, far, own)
                else:
                    here = jnp.where(lane < start + 2 * HALO, own, far)
                acc = here if acc is None else jnp.where(lane >= start, here, acc)
            field[ex + t] = jnp.where(lane < GROUP * edge.places, acc, 0.0)

    def pair_y(v):
        rows = v.reshape(ey // 8, 8, bz)
        swapped = jnp.where(odd_row, pltpu.roll(rows, 1, 1), pltpu.roll(rows, 7, 1))
        return (rows + swapped).reshape(ey, bz)

    def groups(lo, hi, span=SPAN):
        out = []
        for a, b in ((lo, hi), (ex, ex + tiles)):
            at = a
            while at < b:
                stop = min(b, at + span)
                out.append(list(range(at, stop)))
                at = stop
        return out

    def around(i):
        last = ex + tiles - 1
        before = (last, GROUP) if i == ex else (i - 1, 0)
        after = (ex, -GROUP) if i == last else (i + 1, 0)
        return before, after

    def faces(load, group):
        v, turned_v = {}, {}
        for i in group:
            v[i] = load(i)
        for at, k in (around(group[0])[0], around(group[-1])[1]):
            turned_v[at, k] = v[at] if k == 0 and at in v else spin(load(at), k)
        up = {i: up_z(v[i]) for i in group}
        yield
        gz, dn = {}, {}
        for i in group:
            gz[i] = FZ[i] * (v[i] - up[i])
            dn[i] = dn_z(gz[i])
        yield
        out = {}
        (b, kb), _ = around(group[0])
        gx = FX[group[0]] * (v[group[0]] - turned_v[b, kb])
        for i in group:
            if i == group[-1]:
                a, ka = around(i)[1]
                after = turned_v[a, ka]
            else:
                after = v[i + 1]
            gx_next = FX[i + 1] * (after - v[i])
            gy = FY[i] * (v[i] - up_y(v[i]))
            out[i] = (v[i], (gx - gx_next) + ((gy - dn_y(gy)) + (gz[i] - dn[i])))
            gx = gx_next
        return out

    def reads(name, group):
        return {(name, i) for i in group} | {
            (name, around(group[0])[0][0]),
            (name, around(group[-1])[1][0]),
        }

    def run(items):
        done, open_items, at = set(), [], 0
        while at < len(items) or open_items:
            still = []
            for gen, gives in open_items:
                try:
                    next(gen)
                    still.append((gen, gives))
                except StopIteration:
                    done |= gives
            open_items = still
            if not open_items and at < len(items):
                assert items[at][1] <= done, items[at][1] - done
            if at < len(items) and items[at][1] <= done:
                gen, _, gives = items[at]
                at += 1
                try:
                    next(gen)
                    open_items.append((gen, gives))
                except StopIteration:
                    done |= gives

    relay(1)
    wait_all(1)
    relay(0)

    def limit(dx, dy, dz):
        return e_out[...] if (dx, dy, dz) == (0, 0, 0) else e_in[code(dx, dy, dz)]

    for k, (a, z) in enumerate(zip(tables(limit), depths())):
        z_f, even_f = z.astype(f32), (z - z % 2).astype(f32)
        FL[k] = (z_f < a).astype(f32)
        F1[k] = (even_f < a).astype(f32)

    items = []
    pairs, edge_pairs = ex // 2, tiles // 2
    last_pair = pairs + edge_pairs - 1

    def make_faces(group):
        up = {i: up_z(C[i]) for i in group}
        (b, kb), _ = around(group[0])
        before = None if group[0] == 0 else spin(C[b], kb)
        yield
        for i in group:
            c = C[i]
            if before is not None:
                FX[i] = 0.5 * (before + c)
            before = c
            FY[i] = 0.5 * (c + up_y(c))
            FZ[i] = 0.5 * (c + up[i])

    def make_wrap():
        around_face = spin(FX[ex], -GROUP)
        yield
        FX[ex + tiles] = around_face

    def make_inverse(group):
        dn = {i: dn_z(FZ[i]) for i in group}
        yield
        for i in group:
            fy = FY[i]
            diagonal = (FX[i] + FX[i + 1]) + (fy + dn_y(fy)) + (FZ[i] + dn[i])
            fl = FL[flag_of(i)]
            INV[i] = OMEGA * fl / (diagonal + 1.0 - fl)

    def make_pooled(group):
        pooled = {}
        for q in group:
            v = pair_y(C[2 * q] + C[2 * q + 1])
            pooled[q] = v, up_z(v), dn_z(v)
        yield
        for q in group:
            v, up, dn = pooled[q]
            C1[q] = (v + jnp.where(odd_lane, up, dn)) * 0.125

    def beside(q):
        before = (last_pair, GROUP) if q == pairs else (q - 1, 0)
        after = (pairs, -GROUP) if q == last_pair else (q + 1, 0)
        return before, after

    def make_coarse_inverse(group):
        found = {}
        for q in group:
            c = C1[q]
            (b, kb), (a, ka) = beside(q)
            found[q] = up_z(c, 2), dn_z(c, 2), spin(C1[b], kb), spin(C1[a], ka)
        yield
        for q in group:
            c = C1[q]
            up, dn, before, after = found[q]
            diagonal = 3.0 * c + 0.5 * ((before + after) + (up_y(c, 2) + dn_y(c, 2)) + (up + dn))
            fl = F1[flag_of(2 * q)]
            IC[q] = OMEGA * fl / (4.0 * diagonal + 1.0 - fl)

    def cut(lo, hi, span):
        return [list(range(a, min(hi, a + span))) for a in range(lo, hi, span)]

    def named(name, these):
        return {(name, i) for i in these}

    def face_items(lo, hi, needs):
        return [
            (make_faces(g), needs if lo < ex else named("c", range(tiles)), named("f", g))
            for g in cut(lo, hi, WIDE)
        ]

    def inverse_items(lo, hi):
        return [
            (make_inverse(g), named("f", g + [g[-1] + 1]), named("i", g)) for g in cut(lo, hi, WIDE)
        ]

    def pooled_items(lo, hi):
        needs = set() if lo < pairs else named("c", range(tiles))
        return [(make_pooled(g), needs, named("p", g)) for g in cut(lo, hi, WIDE // 2)]

    def coarse_items(lo, hi):
        return [
            (
                make_coarse_inverse(g),
                named("p", [at for q in g for at, _ in beside(q)] + g),
                named("n", g),
            )
            for g in cut(lo, hi, WIDE // 2)
        ]

    def edge_items(f, name):
        field = (R, C)[f]
        return [
            (build_edges(f, field, g), set() if f else {"arrived"}, named(name, g))
            for g in cut(0, tiles, EDGES)
        ]

    def mixed(*lists):
        out, lists = [], [list(x) for x in lists]
        while any(lists):
            for x in lists:
                if x:
                    out.append(x.pop(0))
        return out

    def arrive():
        wait_all(0)
        yield

    items += mixed(
        edge_items(1, "c"),
        face_items(0, ex, set()) + inverse_items(1, ex - 1),
        pooled_items(0, pairs) + coarse_items(1, pairs - 1),
    )
    items.append((arrive(), set(), {"arrived"}))
    items += mixed(
        edge_items(0, "r"),
        face_items(ex, ex + tiles, None)
        + [(make_wrap(), named("f", [ex]), named("f", [ex + tiles]))]
        + inverse_items(ex, ex + tiles),
        pooled_items(pairs, pairs + edge_pairs) + coarse_items(pairs, pairs + edge_pairs),
    )

    off = lane_y % GROUP
    slot0 = (lane_y // GROUP) * tiles

    def core_edge(t, lo_off, hi_off):
        slot = slot0 + t
        low = (slot >= lo_x) & (slot < hi_x) & lo_off
        high = (slot >= ex + lo_x) & (slot < ex + hi_x) & hi_off
        return (low | high) & (lane_y < GROUP * edge.places)

    core_off = (off >= HALO) & (off < 2 * HALO)
    core_tiles = [core_edge(t, core_off, core_off) for t in range(tiles)]
    core_lanes = (lane_y >= HALO) & (lane_y < bz - HALO)

    zeros = jnp.zeros((by, bz), f32)
    scalars = 8
    width = late.shape[-1]
    base = scalars if width == bz else bz
    col = lax.broadcasted_iota(jnp.int32, (1, width), 1)
    coupling = {}

    def couple():
        flux_z = FZ[lo_x, :by]
        flux_y = FY[lo_x]
        for i in range(lo_x + 1, hi_x):
            flux_z = flux_z + FZ[i, :by]
            flux_y = flux_y + FY[i]
        fl = FL[1]
        fl_up, fl_core = up_y(fl), fl[:by]
        step = fl_core - up_z(fl)[:by]
        inner = jnp.where(lane_y >= 1, flux_z * (step * step), 0.0)
        none = jnp.logical_and(off < 0, off >= 0)
        low_face = [core_edge(t, off == HALO, none) for t in range(tiles)]
        high_face = [core_edge(t, none, off == 2 * HALO) for t in range(tiles)]
        sides = {}

        def put(d, alone, shared):
            sides[d] = (total(alone), total(shared))

        alone = FX[lo_x, :by] * fl_core
        put((-1, 0, 0), alone, alone * FL[0, :by])
        alone = FX[hi_x, :by] * fl_core
        put((1, 0, 0), alone, alone * FL[2, :by])
        alone = jnp.where(row == 0, flux_y * fl, 0.0)
        put((0, -1, 0), alone, alone * fl_up)
        alone = jnp.where(row == by, flux_y * fl_up, 0.0)
        put((0, 1, 0), alone, alone * fl)
        parts = [zeros] * 4
        for t in range(tiles):
            f_edge = FL[3 + edge.pattern_of[t]]
            f_here, f_up = f_edge[:by], up_z(f_edge)[:by]
            fz = FZ[ex + t, :by]
            a = jnp.where(low_face[t], fz * f_here, 0.0)
            b = jnp.where(high_face[t], fz * f_up, 0.0)
            parts = [parts[0] + a, parts[1] + a * f_up, parts[2] + b, parts[3] + b * f_here]
        put((0, 0, -1), parts[0], parts[1])
        put((0, 0, 1), parts[2], parts[3])

        inner_sum = total(inner)
        yield
        yield
        diagonal = inner_sum
        late_row = jnp.zeros((1, width), f32)
        for (dx, dy, dz), (alone, shared) in sides.items():
            diagonal = diagonal + alone
            other = ((ix + dx) * ngy + iy + dy) * ngz + iz + dz
            valid = inside((dx, dy, dz))
            late_row = late_row - jnp.where((col == base + other) & valid, shared, 0.0)
        late_row = late_row + jnp.where(col == base + me, diagonal, 0.0)
        coupling[0] = late_row


    def solve(means):
        y_row = jnp.sum(inverse * means, axis=0, keepdims=True)
        y_col = jnp.sum(jnp.where(eye, y_row, 0.0), axis=1, keepdims=True)
        return y_row, y_col

    def block_row(dx, dy, dz):
        def near(at, step, count):
            return jnp.clip(at + step, 0, count - 1)

        b = (near(ix, dx, ngx) * ngy + near(iy, dy, ngy)) * ngz + near(iz, dz, ngz)
        return YB[pl.ds(b, 1)]

    def spread_blocks(y_col):
        YB[...] = jnp.broadcast_to(y_col, (n, bz))
        for k, v in enumerate(tables(block_row)):
            EY[k] = FL[k] * v

    cells = bx * by * bz

    def first_solve():
        collect(early, 0)
        m0_col = early[:, 0, 0:1]
        yield
        y_row = jnp.sum(inverse * (m0_col * (1.0 / cells)), axis=0, keepdims=True)
        yield
        y_col = jnp.sum(jnp.where(eye, y_row, 0.0), axis=1, keepdims=True)
        yield
        yield
        spread_blocks(y_col)

    sums = [[zeros, zeros] for _ in range(7)]
    parts = {}

    def add(i, k, v):
        if i < ex:
            if lo_x <= i < hi_x:
                sums[k][0] = sums[k][0] + v
        else:
            sums[k][1] = sums[k][1] + jnp.where(core_tiles[i - ex], v, 0.0)

    def coarse(field, group):
        found = yield from faces(lambda i: INV[i] * field[i], group)
        pooled = {}
        for i in group[::2]:
            gap = FL[flag_of(i)] * (field[i] - found[i][1])
            gap = gap + FL[flag_of(i + 1)] * (field[i + 1] - found[i + 1][1])
            gap = pair_y(gap)
            pooled[i] = (gap, up_z(gap), dn_z(gap))
        yield
        for i in group[::2]:
            gap, up, dn = pooled[i]
            below = IC[i // 2] * (gap + jnp.where(odd_lane, up, dn))
            for at in (i, i + 1):
                SEC[at] = found[at][0] + FL[flag_of(at)] * below

    def smooth(field, group, keep):
        found = yield from faces(lambda i: SEC[i], group)
        for i in group:
            v, lv = found[i]
            keep(i, v + INV[i] * (field[i] - lv))

    def image(load, group, keep):
        found = yield from faces(load, group)
        for i in group:
            keep(i, *found[i])

    def add_cycle(field, source, name, lo, hi, keep, extra):
        even, stop = (lo - 1) // 2 * 2, (hi + 2) // 2 * 2
        for group in groups(even, stop):
            if source is None:
                needs = {(k, at) for k in "fi" for _, at in reads("i", group)}
                needs |= named("n", [i // 2 for i in group]) | {"arrived"}
                needs |= named("r", range(tiles)) if group[0] >= ex else set()
            else:
                needs = reads(source, group)
            items.append((coarse(field, group), needs, {(name + "s", i) for i in group}))
        for group in groups(lo, hi):
            needs = reads(name + "s", group)
            if extra and group[0] >= ex:
                items.append(extra)
                extra = None
            items.append((smooth(field, group, keep), needs, {(name, i) for i in group}))

    def keep_direction(i, v):
        U[i] = v

    def keep_image(i, v, lv):
        w = FL[flag_of(i)] * lv
        W[i] = w
        if lo_x <= i < hi_x or i >= ex:
            D0[i] = v
        add(i, 0, R[i, :by] * v[:by])
        add(i, 1, w[:by] * v[:by])
        add(i, 2, w[:by])

    def keep_second(i, v):
        U[i] = v
        add(i, 3, W[i, :by] * v[:by])
        add(i, 4, R[i, :by] * v[:by])

    def keep_third(i, v, lv):
        q = FL[flag_of(i)][:by] * lv[:by]
        Q[i, :by] = q
        add(i, 5, q * v[:by])
        add(i, 6, q)

    def gather_sums(which):
        for k in which:
            a, b = sums[k]
            parts[k] = total(jnp.where(core_lanes, a, 0.0) + b)
        yield

    def core_of(name):
        return {(name, i) for i in range(lo_x, hi_x)} | {(name, ex + t) for t in range(tiles)}

    add_cycle(R, None, "d", 4, ex - 4, keep_direction, (first_solve(), set(), {"blocks"}))
    for group in groups(5, ex - 5):
        items.append(
            (image(lambda i: U[i] + EY[flag_of(i)], group, keep_image), reads("d", group) | {"blocks"}, {("w", i) for i in group})
        )
    add_cycle(W, "w", "u", 7, ex - 7, keep_second, None)
    items.append((couple(), set(), set()))
    items.append((gather_sums(range(3)), core_of("w"), set()))
    for group in groups(lo_x, hi_x):
        items.append(
            (image(lambda i: U[i], group, keep_third), reads("u", group), {("q", i) for i in group})
        )
    items.append((gather_sums(range(3, 5)), core_of("u"), set()))
    items.append((gather_sums(range(5, 7)), core_of("q"), set()))
    run(items)

    late_row = coupling[0]
    for k in range(7):
        late_row = jnp.where(col == k, parts[k], late_row)
    late_row = jnp.where(col == 7, m0, late_row)
    compact = base + 2 * n <= width
    if compact:
        late_row = jnp.where(col == base + n + me, parts[2], late_row)
    late_out[...] = late_row
    late[pl.ds(me, 1)] = late_row[None]
    spread(late_out, late, 1)
    if compact:
        spot = lax.broadcasted_iota(jnp.int32, (n, width), 1)
        owner = lax.broadcasted_iota(jnp.int32, (n, width), 0)
        own_lane = spot == base + owner
        placed = jnp.dot(
            inverse,
            (spot == base + n + owner).astype(f32),
            precision=HIGH,
            preferred_element_type=f32,
        )
    wait_sent(1)
    wait_sent(0)
    collect(late, 1)

    rows = late[:, 0, :]
    plain = jnp.sum(rows, axis=0, keepdims=True)
    if compact:
        y_col = jnp.sum(placed * plain, axis=1, keepdims=True) * (1.0 / cells)
    else:
        y_row, y_col = solve(rows[:, 2:3] * (1.0 / cells))
    spread_blocks(y_col)
    weighted = jnp.sum(rows * y_col, axis=0, keepdims=True)
    if compact:
        y_line = jnp.sum(jnp.where(own_lane, y_col, 0.0), axis=0, keepdims=True)
        quadratic = total(weighted * y_line)
    else:
        quadratic = total(weighted[:, base : base + n] * y_row)

    def pick(line, k):
        return jnp.sum(line[:, k : k + 1], axis=(0, 1), keepdims=True)

    rz, dad = pick(plain, 0), pick(plain, 1)
    w_u = pick(plain, 3) + pick(weighted, 2)
    r_u = pick(plain, 4) + pick(weighted, 7)
    u_q = (
        pick(plain, 5)
        + 2.0 * pick(weighted, 6)
        + quadratic
    )
    alpha, per_rz = rz / dad, 1.0 / rz
    new = (rz - alpha * dad) + alpha * (alpha * w_u - r_u)
    beta = new * per_rz
    grow = 1.0 + beta
    dad1 = grow * grow * dad - 2.0 * alpha * grow * w_u + alpha * alpha * u_q
    alpha1 = new / dad1
    c1 = alpha + alpha1 * grow
    c2 = alpha * alpha1

    def results(i, v, lv):
        fl = FL[flag_of(i)][:by]
        sol = c1 * D0[i, :by] - c2 * (U[i, :by] + v[:by])
        res = fl * R[i, :by] - c1 * W[i, :by] + c2 * (Q[i, :by] + fl * lv[:by])
        if i < ex:
            sol_ref[i - lo_x], res_ref[i - lo_x] = sol, res
        else:
            SEC[i, :by], INV[i, :by] = sol, res

    run(
        [
            (image(lambda i: EY[flag_of(i)], group, results), set(), set())
            for group in groups(lo_x, hi_x)
        ]
    )
    for x in range(bx):
        tl, jl = edge.place(lo_x + x, 0)
        th, jh = edge.place(lo_x + x, 1)
        for ref, held in ((sol_ref, SEC), (res_ref, INV)):
            low = spin(held[ex + tl, :by], -(GROUP * jl + HALO))
            high = spin(held[ex + th, :by], bz - HALO - (GROUP * jh + HALO))
            ref[x] = jnp.where(
                lane_y < HALO, low, jnp.where(lane_y >= bz - HALO, high, ref[x])
            )
    spread_done(early, 0)
    spread_done(late, 1)


def solution(mesh):
    counts = (mesh.shape["gx"], mesh.shape["gy"], mesh.shape["gz"])
    n = counts[0] * counts[1] * counts[2]

    def on_device(right_side, conductance, extents, coarse_factor):
        f32 = jnp.float32
        bx, by, bz = right_side.shape
        ex, ey = bx + 2 * HALO, by + 2 * HALO
        edge = Edge(bx, bz)
        slabs = ex + edge.tiles
        width = bz if n + 8 <= bz else bz + -(-n // 128) * 128
        vm = lambda *shape: pltpu.VMEM(shape, f32)
        field = vm(slabs, ey, bz)
        half = vm(slabs // 2, ey, bz)
        flags = vm(3 + len(edge.patterns), ey, bz)
        dma = pltpu.SemaphoreType.DMA
        scratch = [
            field,
            field,
            pltpu.VMEM(extents.shape, extents.dtype),
            pltpu.VMEM(coarse_factor.shape, coarse_factor.dtype),
            vm(1, bz),
            vm(27, 1, bz),
            vm(2, by, bz),
            vm(2, 2, 3, ey, bz),
            vm(1, bz),
            vm(n, 1, bz),
            vm(1, width),
            vm(n, 1, width),
            flags,
            flags,
            vm(slabs + 1, ey, bz),
            field,
            field,
            field,
            half,
            half,
            field,
            field,
            field,
            field,
            field,
            vm(n, bz),
            flags,
            dma((27,)),
            dma((27,)),
            dma((27,)),
            dma((27,)),
            dma((27,)),
            dma((27,)),
            dma((2,)),
            dma((2,)),
            dma((4,)),
        ]
        whole = pl.BlockSpec(memory_space=pltpu.VMEM)
        outer = pl.BlockSpec(memory_space=pltpu.HBM)
        both = pl.pallas_call(
            functools.partial(kernel, counts),
            out_shape=vm(2, bx, by, bz),
            in_specs=[outer, outer, outer, outer],
            out_specs=whole,
            scratch_shapes=scratch,
            compiler_params=pltpu.CompilerParams(
                collective_id=0, has_side_effects=True, vmem_limit_bytes=60000000
            ),
        )(right_side, conductance, extents, coarse_factor)
        return both[0], both[1]

    in_specs = (P("gx", "gy", "gz"), P("gx", "gy", "gz"), P("gx", "gy", "gz"), P())
    out_specs = (P("gx", "gy", "gz"), P("gx", "gy", "gz"))
    return jax.shard_map(
        on_device, mesh=mesh, in_specs=in_specs, out_specs=out_specs, check_vma=False
    )
```

```python
import functools

import jax
import jax.numpy as jnp
from jax import lax
from jax.experimental import pallas as pl
from jax.experimental.pallas import tpu as pltpu
from jax.sharding import PartitionSpec as P

OMEGA = 0.8
HALO = 8
GROUP = 3 * HALO
SPAN = 24
WIDE = 12
EDGES = 2
MESH = pl.DeviceIdType.MESH
HIGH = lax.Precision.HIGHEST
DIRS = [
    (dx, dy, dz)
    for dx in (-1, 0, 1)
    for dy in (-1, 0, 1)
    for dz in (-1, 0, 1)
    if (dx, dy, dz) != (0, 0, 0)
]
DIRS.sort(key=lambda d: -sum(abs(a) for a in d))


def code(dx, dy, dz):
    return (dx + 1) * 9 + (dy + 1) * 3 + dz + 1


class Edge:
    def __init__(self, bx, bz):
        self.bx, self.ex = bx, bx + 2 * HALO
        self.places = bz // GROUP
        tiles = -(-2 * self.ex // self.places)
        self.tiles = tiles + tiles % 2
        self.patterns, self.pattern_of = [], []
        for t in range(self.tiles):
            key = tuple(
                None if s is None else (self.block(s[0])[0], s[1])
                for s in (self.slab(t, j) for j in range(self.places))
            )
            if key not in self.patterns:
                self.patterns.append(key)
            self.pattern_of.append(self.patterns.index(key))

    def slab(self, t, j):
        slot = t + self.tiles * j
        return None if slot >= 2 * self.ex else (slot % self.ex, slot // self.ex)

    def place(self, s, side):
        slot = s + self.ex * side
        return slot % self.tiles, slot // self.tiles

    def block(self, s):
        if s < HALO:
            return 0, self.bx - HALO + s
        if s < HALO + self.bx:
            return 1, s - HALO
        return 2, s - HALO - self.bx


def kernel(
    counts,
    rhs_hbm,
    cond_hbm,
    ext_hbm,
    factor_hbm,
    both_ref,
    R,
    C,
    ext_ref,
    factor_ref,
    e_out,
    e_in,
    z_out,
    z_in,
    early_out,
    early,
    late_out,
    late,
    FL,
    F1,
    FX,
    FY,
    FZ,
    INV,
    C1,
    IC,
    SEC,
    D0,
    W,
    U,
    Q,
    YB,
    EY,
    send_c,
    recv_c,
    send_r,
    recv_r,
    send_e,
    recv_e,
    send_g,
    recv_g,
    load_sem,
):
    sol_ref, res_ref = both_ref.at[0], both_ref.at[1]
    ngx, ngy, ngz = counts
    n = ngx * ngy * ngz
    ix, iy, iz = lax.axis_index("gx"), lax.axis_index("gy"), lax.axis_index("gz")
    me = (ix * ngy + iy) * ngz + iz
    bx, by, bz = sol_ref.shape
    ex, ey = bx + 2 * HALO, by + 2 * HALO
    edge = Edge(bx, bz)
    tiles = edge.tiles
    f32 = jnp.float32
    lo_x, hi_x = HALO, HALO + bx

    def turned(at, step, count):
        moved = at + step
        return jnp.where(moved >= count, moved - count, moved)

    def everyone(act):
        if n <= 64:
            xs = [turned(ix, t, ngx) for t in range(ngx)]
            ys = [turned(iy, t, ngy) for t in range(ngy)]
            zs = [turned(iz, t, ngz) for t in range(ngz)]
            steps = [(a, b, c) for a in range(ngx) for b in range(ngy) for c in range(ngz)]
            steps.sort(
                key=lambda t: -sum(min(a, m - a) for a, m in zip(t, (ngx, ngy, ngz)))
            )
            for a, b, c in steps[:-1]:
                act((xs[a], ys[b], zs[c]))
        else:

            def one(t, carry):
                flat = (me + t) % n
                act((flat // (ngy * ngz), (flat // ngz) % ngy, flat % ngz))
                return carry

            lax.fori_loop(1, n, one, 0)

    core_x, core_y = pl.ds(lo_x, bx), pl.ds(0, by)
    loads = [
        pltpu.make_async_copy(src, dst, load_sem.at[k])
        for k, (src, dst) in enumerate(
            (
                (rhs_hbm, R.at[core_x, core_y]),
                (cond_hbm, C.at[core_x, core_y]),
                (ext_hbm, ext_ref),
                (factor_hbm, factor_ref),
            )
        )
    ]
    for load in loads:
        load.start()

    barrier = pltpu.get_barrier_semaphore()
    everyone(
        lambda device: pl.semaphore_signal(
            barrier, inc=1, device_id=device, device_id_type=MESH
        )
    )

    def inside(d):
        ok = None
        for at, step, count in zip((ix, iy, iz), d, counts):
            if step == 0:
                continue
            here = (at + step >= 0) & (at + step < count)
            ok = here if ok is None else ok & here
        return ok

    def x_from(dx):
        return pl.ds(bx, HALO) if dx == 1 else pl.ds(HALO, bx if dx == 0 else HALO)

    def x_into(dx):
        if dx == 0:
            return pl.ds(HALO, bx)
        return pl.ds(0, HALO) if dx == 1 else pl.ds(hi_x, HALO)

    def y_from(dy):
        return pl.ds(by - HALO, HALO) if dy == 1 else pl.ds(0, by if dy == 0 else HALO)

    def y_into(dy):
        if dy == 0:
            return pl.ds(0, by)
        return pl.ds(by + HALO, HALO) if dy == 1 else pl.ds(by, HALO)

    def landing(f, d):
        dx, dy, dz = d
        if dz != 0:
            return z_in.at[f, 1 if dz == 1 else 0, 1 - dx, y_into(dy)]
        return (R, C)[f].at[x_into(dx), y_into(dy)]

    def remote(src, dst, send, recv, d):
        return pltpu.make_async_remote_copy(
            src_ref=src,
            dst_ref=dst,
            send_sem=send,
            recv_sem=recv,
            device_id=(ix + d[0], iy + d[1], iz + d[2]),
            device_id_type=MESH,
        )

    def copies(f, d):
        dx, dy, dz = d
        k = code(*d)
        if dz != 0:
            src = z_out.at[f, y_from(dy)]
        else:
            src = (R, C)[f].at[x_from(dx), y_from(dy)]
        send, recv = ((send_r, recv_r), (send_c, recv_c))[f]
        out = [remote(src, landing(f, d), send.at[k], recv.at[k], d)]
        if f == 1:
            out.append(remote(e_out, e_in.at[code(-dx, -dy, -dz)], send_e.at[k], recv_e.at[k], d))
        return out

    odd = ix % 2 == 1

    def corner(d):
        return d[0] != 0 and d[1] != 0 and d[2] == 0

    def when_sent(f, act):
        for d in DIRS:

            @pl.when(inside(d))
            def _():
                values, *flags = copies(f, d)
                for c in flags:
                    act(c)
                if not corner(d):
                    act(values)
                    return

                if d[0] == 1:
                    act(values)
                    return

                @pl.when(jnp.logical_not(odd))
                def _():
                    act(values)

    def relayed(f, dy):
        field, k = (R, C)[f], code(-1, dy, 0)
        send, recv = ((send_r, recv_r), (send_c, recv_c))[f]
        return remote(
            field.at[x_from(-1), y_into(dy)],
            field.at[x_into(-1), y_into(dy)],
            send.at[k],
            recv.at[k],
            (-1, 0, 0),
        )

    def start_all(f):
        when_sent(f, lambda c: c.start())

    def relay(f):
        for dy in (-1, 1):

            @pl.when(inside((0, -dy, 0)) & odd)
            def _():
                for c in copies(f, (0, dy, 0)):
                    c.wait_recv()
                relayed(f, dy).start()

    def wait_all(f):
        for d in DIRS:
            ok = inside(tuple(-a for a in d))

            @pl.when(ok & jnp.logical_not(odd) if d[0] == 0 and d[2] == 0 else ok)
            def _():
                for c in copies(f, d):
                    c.wait_recv()

    def wait_sent(f):
        when_sent(f, lambda c: c.wait_send())
        for dy in (-1, 1):

            @pl.when(inside((0, -dy, 0)) & odd)
            def _():
                relayed(f, dy).wait_send()

    for d in DIRS:

        @pl.when(jnp.logical_not(inside(tuple(-a for a in d))))
        def _():
            for f in (0, 1):
                ref = landing(f, d)
                ref[...] = jnp.zeros(ref.shape, f32)
            e_in[code(*(-a for a in d))] = jnp.zeros((1, bz), f32)

    lane = lax.broadcasted_iota(jnp.int32, (ey, bz), 1)
    row = lax.broadcasted_iota(jnp.int32, (ey, bz), 0)
    odd_lane = lane % 2 == 1
    odd_row = (row % 2 == 1).reshape(ey // 8, 8, bz)
    lane_y = lane[:by]

    def up_y(v, k=1):
        return pltpu.roll(v, k, 0)

    def dn_y(v, k=1):
        return pltpu.roll(v, ey - k, 0)

    def spin(v, k):
        k = k % bz
        return v if k == 0 else pltpu.roll(v, k, 1)

    def up_z(v, k=1):
        return pltpu.roll(v, k, 1)

    def dn_z(v, k=1):
        return pltpu.roll(v, bz - k, 1)

    for load in loads[:3]:
        load.wait()
    own_limit = ext_ref[0].astype(f32)
    e_out[...] = jnp.broadcast_to(own_limit, (1, bz))
    for f, field in ((1, C), (0, R)):
        packed = jnp.zeros((by, bz), f32)
        for k in range(bx):
            moved = spin(field[lo_x + k, :by], 2 * HALO * k + HALO)
            packed = jnp.where(lane_y // (2 * HALO) == k, moved, packed)
        z_out[f] = packed

    def total(v):
        return jnp.sum(v, axis=(0, 1), keepdims=True)

    acc = R[lo_x, :by]
    for k in range(1, bx):
        acc = acc + R[lo_x + k, :by]
    m0 = total(jnp.where(lane_y.astype(f32) < own_limit, acc, 0.0))
    early_row = jnp.broadcast_to(m0, (1, bz))
    early_out[...] = early_row
    early[pl.ds(me, 1)] = early_row[None]

    def remote_row(out, into, base, device):
        return pltpu.make_async_remote_copy(
            src_ref=out,
            dst_ref=into.at[me],
            send_sem=send_g.at[base],
            recv_sem=recv_g.at[base],
            device_id=device,
            device_id_type=MESH,
        )

    def spread(out, into, base):
        everyone(lambda device: remote_row(out, into, base, device).start())

    def collect(into, base):
        part = into.at[pl.ds(0, n - 1)]
        pltpu.make_async_copy(part, part, recv_g.at[base]).wait()

    def spread_done(into, base):
        part = into.at[pl.ds(0, n - 1)]
        pltpu.make_async_copy(part, part, send_g.at[base]).wait()

    pl.semaphore_wait(barrier, n - 1)
    start_all(1)
    spread(early_out, early, 0)
    start_all(0)

    loads[3].wait()
    L = factor_ref[...].astype(f32)
    ri = lax.broadcasted_iota(jnp.int32, (n, n), 0)
    ci = lax.broadcasted_iota(jnp.int32, (n, n), 1)
    eye = ri == ci
    X = jnp.where(eye, 1.0 / jnp.where(eye, L, 1.0), 0.0)
    s = 1
    while s < n:
        pick = (ri // (2 * s) == ci // (2 * s)) & (ri % (2 * s) >= s) & (ci % (2 * s) < s)
        low = jnp.where(pick, L, 0.0)
        X = X - jnp.dot(
            X,
            jnp.dot(low, X, precision=HIGH, preferred_element_type=f32),
            precision=HIGH,
            preferred_element_type=f32,
        )
        s *= 2
    inverse = lax.dot_general(
        X, X, (((0,), (0,)), ((), ())), precision=HIGH, preferred_element_type=f32
    )

    one_lane = lax.broadcasted_iota(jnp.int32, (1, bz), 1)
    bands = ((0, by), (1, HALO), (-1, HALO))

    def tables(value):
        rows = {
            (dx, dy, dz): value(dx, dy, dz)
            for dx in (-1, 0, 1)
            for dy in (-1, 0, 1)
            for dz in (-1, 0, 1)
        }
        out = [
            jnp.concatenate(
                [jnp.broadcast_to(rows[dx, dy, 0], (count, bz)) for dy, count in bands], axis=0
            )
            for dx in (-1, 0, 1)
        ]
        for pattern in edge.patterns:
            parts = []
            for dy, count in bands:
                line = None
                for j, key in enumerate(pattern):
                    if key is None:
                        continue
                    dx, start = key[0] - 1, GROUP * j
                    if key[1] == 0:
                        here = jnp.where(
                            one_lane < start + HALO, rows[dx, dy, -1], rows[dx, dy, 0]
                        )
                    else:
                        here = jnp.where(
                            one_lane < start + 2 * HALO, rows[dx, dy, 0], rows[dx, dy, 1]
                        )
                    line = here if line is None else jnp.where(one_lane >= start, here, line)
                parts.append(jnp.broadcast_to(line, (count, bz)))
            out.append(jnp.concatenate(parts, axis=0))
        return out

    def depths():
        plain = one_lane
        out = [plain] * 3
        for pattern in edge.patterns:
            line = None
            for j, key in enumerate(pattern):
                off = one_lane - GROUP * j
                if key is None:
                    here = jnp.full((1, bz), bz, jnp.int32)
                elif key[1] == 0:
                    here = jnp.where(off < HALO, off + bz - HALO, off - HALO)
                else:
                    here = jnp.where(off < 2 * HALO, off + bz - 2 * HALO, off - 2 * HALO)
                line = here if line is None else jnp.where(off >= 0, here, line)
            line = jnp.where(one_lane >= GROUP * edge.places, bz, line)
            out.append(line)
        return out

    def flag_of(i):
        return edge.block(i)[0] if i < ex else 3 + edge.pattern_of[i - ex]

    def build_edges(f, field, group):
        moved = {}
        for t in group:
            for j in range(edge.places):
                slab = edge.slab(t, j)
                if slab is None:
                    continue
                s, side = slab
                if f == 0 and s in (0, ex - 1):
                    moved[t, j] = None
                    continue
                which, k = edge.block(s)
                start, at = GROUP * j, 2 * HALO * k
                if side == 0:
                    own = spin(field[s], start + HALO)
                    far = spin(z_in[f, 1, which], start - at)
                else:
                    own = spin(field[s], start + 2 * HALO - bz)
                    far = spin(z_in[f, 0, which], start + HALO - at)
                moved[t, j] = own, far
        yield
        for t in group:
            acc = None
            for j in range(edge.places):
                start = GROUP * j
                if (t, j) not in moved:
                    acc = jnp.where(lane >= start, 0.0, acc)
                    break
                own, far = moved[t, j] or (0.0, 0.0)
                if edge.slab(t, j)[1] == 0:
                    here = jnp.where(lane < start + HALO, far, own)
                else:
                    here = jnp.where(lane < start + 2 * HALO, own, far)
                acc = here if acc is None else jnp.where(lane >= start, here, acc)
            field[ex + t] = jnp.where(lane < GROUP * edge.places, acc, 0.0)

    def pair_y(v):
        rows = v.reshape(ey // 8, 8, bz)
        swapped = jnp.where(odd_row, pltpu.roll(rows, 1, 1), pltpu.roll(rows, 7, 1))
        return (rows + swapped).reshape(ey, bz)

    def groups(lo, hi, span=SPAN):
        out = []
        for a, b in ((lo, hi), (ex, ex + tiles)):
            at = a
            while at < b:
                stop = min(b, at + span)
                out.append(list(range(at, stop)))
                at = stop
        return out

    def around(i):
        last = ex + tiles - 1
        before = (last, GROUP) if i == ex else (i - 1, 0)
        after = (ex, -GROUP) if i == last else (i + 1, 0)
        return before, after

    def faces(load, group):
        v, turned_v = {}, {}
        for i in group:
            v[i] = load(i)
        for at, k in (around(group[0])[0], around(group[-1])[1]):
            turned_v[at, k] = v[at] if k == 0 and at in v else spin(load(at), k)
        up = {i: up_z(v[i]) for i in group}
        yield
        gz, dn = {}, {}
        for i in group:
            gz[i] = FZ[i] * (v[i] - up[i])
            dn[i] = dn_z(gz[i])
        yield
        out = {}
        (b, kb), _ = around(group[0])
        gx = FX[group[0]] * (v[group[0]] - turned_v[b, kb])
        for i in group:
            if i == group[-1]:
                a, ka = around(i)[1]
                after = turned_v[a, ka]
            else:
                after = v[i + 1]
            gx_next = FX[i + 1] * (after - v[i])
            gy = FY[i] * (v[i] - up_y(v[i]))
            out[i] = (v[i], (gx - gx_next) + ((gy - dn_y(gy)) + (gz[i] - dn[i])))
            gx = gx_next
        return out

    def reads(name, group):
        return {(name, i) for i in group} | {
            (name, around(group[0])[0][0]),
            (name, around(group[-1])[1][0]),
        }

    def run(items):
        done, open_items, at = set(), [], 0
        while at < len(items) or open_items:
            still = []
            for gen, gives in open_items:
                try:
                    next(gen)
                    still.append((gen, gives))
                except StopIteration:
                    done |= gives
            open_items = still
            if not open_items and at < len(items):
                assert items[at][1] <= done, items[at][1] - done
            if at < len(items) and items[at][1] <= done:
                gen, _, gives = items[at]
                at += 1
                try:
                    next(gen)
                    open_items.append((gen, gives))
                except StopIteration:
                    done |= gives

    relay(1)
    wait_all(1)
    relay(0)

    def limit(dx, dy, dz):
        return e_out[...] if (dx, dy, dz) == (0, 0, 0) else e_in[code(dx, dy, dz)]

    for k, (a, z) in enumerate(zip(tables(limit), depths())):
        z_f, even_f = z.astype(f32), (z - z % 2).astype(f32)
        FL[k] = (z_f < a).astype(f32)
        F1[k] = (even_f < a).astype(f32)

    items = []
    pairs, edge_pairs = ex // 2, tiles // 2
    last_pair = pairs + edge_pairs - 1

    def make_faces(group):
        up = {i: up_z(C[i]) for i in group}
        (b, kb), _ = around(group[0])
        before = None if group[0] == 0 else spin(C[b], kb)
        yield
        for i in group:
            c = C[i]
            if before is not None:
                FX[i] = 0.5 * (before + c)
            before = c
            FY[i] = 0.5 * (c + up_y(c))
            FZ[i] = 0.5 * (c + up[i])

    def make_wrap():
        around_face = spin(FX[ex], -GROUP)
        yield
        FX[ex + tiles] = around_face

    def make_inverse(group):
        dn = {i: dn_z(FZ[i]) for i in group}
        yield
        for i in group:
            fy = FY[i]
            diagonal = (FX[i] + FX[i + 1]) + (fy + dn_y(fy)) + (FZ[i] + dn[i])
            fl = FL[flag_of(i)]
            INV[i] = OMEGA * fl / (diagonal + 1.0 - fl)

    def make_pooled(group):
        pooled = {}
        for q in group:
            v = pair_y(C[2 * q] + C[2 * q + 1])
            pooled[q] = v, up_z(v), dn_z(v)
        yield
        for q in group:
            v, up, dn = pooled[q]
            C1[q] = (v + jnp.where(odd_lane, up, dn)) * 0.125

    def beside(q):
        before = (last_pair, GROUP) if q == pairs else (q - 1, 0)
        after = (pairs, -GROUP) if q == last_pair else (q + 1, 0)
        return before, after

    def make_coarse_inverse(group):
        found = {}
        for q in group:
            c = C1[q]
            (b, kb), (a, ka) = beside(q)
            found[q] = up_z(c, 2), dn_z(c, 2), spin(C1[b], kb), spin(C1[a], ka)
        yield
        for q in group:
            c = C1[q]
            up, dn, before, after = found[q]
            diagonal = 3.0 * c + 0.5 * ((before + after) + (up_y(c, 2) + dn_y(c, 2)) + (up + dn))
            fl = F1[flag_of(2 * q)]
            IC[q] = OMEGA * fl / (4.0 * diagonal + 1.0 - fl)

    def cut(lo, hi, span):
        return [list(range(a, min(hi, a + span))) for a in range(lo, hi, span)]

    def named(name, these):
        return {(name, i) for i in these}

    def face_items(lo, hi, needs):
        return [
            (make_faces(g), needs if lo < ex else named("c", range(tiles)), named("f", g))
            for g in cut(lo, hi, WIDE)
        ]

    def inverse_items(lo, hi):
        return [
            (make_inverse(g), named("f", g + [g[-1] + 1]), named("i", g)) for g in cut(lo, hi, WIDE)
        ]

    def pooled_items(lo, hi):
        needs = set() if lo < pairs else named("c", range(tiles))
        return [(make_pooled(g), needs, named("p", g)) for g in cut(lo, hi, WIDE // 2)]

    def coarse_items(lo, hi):
        return [
            (
                make_coarse_inverse(g),
                named("p", [at for q in g for at, _ in beside(q)] + g),
                named("n", g),
            )
            for g in cut(lo, hi, WIDE // 2)
        ]

    def edge_items(f, name):
        field = (R, C)[f]
        return [
            (build_edges(f, field, g), set() if f else {"arrived"}, named(name, g))
            for g in cut(0, tiles, EDGES)
        ]

    def mixed(*lists):
        out, lists = [], [list(x) for x in lists]
        while any(lists):
            for x in lists:
                if x:
                    out.append(x.pop(0))
        return out

    def arrive():
        wait_all(0)
        yield

    items += mixed(
        edge_items(1, "c"),
        face_items(0, ex, set()) + inverse_items(1, ex - 1),
        pooled_items(0, pairs) + coarse_items(1, pairs - 1),
    )
    items.append((arrive(), set(), {"arrived"}))
    items += mixed(
        edge_items(0, "r"),
        face_items(ex, ex + tiles, None)
        + [(make_wrap(), named("f", [ex]), named("f", [ex + tiles]))]
        + inverse_items(ex, ex + tiles),
        pooled_items(pairs, pairs + edge_pairs) + coarse_items(pairs, pairs + edge_pairs),
    )

    off = lane_y % GROUP
    slot0 = (lane_y // GROUP) * tiles

    def core_edge(t, lo_off, hi_off):
        slot = slot0 + t
        low = (slot >= lo_x) & (slot < hi_x) & lo_off
        high = (slot >= ex + lo_x) & (slot < ex + hi_x) & hi_off
        return (low | high) & (lane_y < GROUP * edge.places)

    core_off = (off >= HALO) & (off < 2 * HALO)
    core_tiles = [core_edge(t, core_off, core_off) for t in range(tiles)]
    core_lanes = (lane_y >= HALO) & (lane_y < bz - HALO)

    zeros = jnp.zeros((by, bz), f32)
    scalars = 8
    width = late.shape[-1]
    base = scalars if width == bz else bz
    col = lax.broadcasted_iota(jnp.int32, (1, width), 1)
    coupling = {}

    def couple():
        flux_z = FZ[lo_x, :by]
        flux_y = FY[lo_x]
        for i in range(lo_x + 1, hi_x):
            flux_z = flux_z + FZ[i, :by]
            flux_y = flux_y + FY[i]
        fl = FL[1]
        fl_up, fl_core = up_y(fl), fl[:by]
        step = fl_core - up_z(fl)[:by]
        inner = jnp.where(lane_y >= 1, flux_z * (step * step), 0.0)
        none = jnp.logical_and(off < 0, off >= 0)
        low_face = [core_edge(t, off == HALO, none) for t in range(tiles)]
        high_face = [core_edge(t, none, off == 2 * HALO) for t in range(tiles)]
        sides = {}

        def put(d, alone, shared):
            sides[d] = (total(alone), total(shared))

        alone = FX[lo_x, :by] * fl_core
        put((-1, 0, 0), alone, alone * FL[0, :by])
        alone = FX[hi_x, :by] * fl_core
        put((1, 0, 0), alone, alone * FL[2, :by])
        alone = jnp.where(row == 0, flux_y * fl, 0.0)
        put((0, -1, 0), alone, alone * fl_up)
        alone = jnp.where(row == by, flux_y * fl_up, 0.0)
        put((0, 1, 0), alone, alone * fl)
        parts = [zeros] * 4
        for t in range(tiles):
            f_edge = FL[3 + edge.pattern_of[t]]
            f_here, f_up = f_edge[:by], up_z(f_edge)[:by]
            fz = FZ[ex + t, :by]
            a = jnp.where(low_face[t], fz * f_here, 0.0)
            b = jnp.where(high_face[t], fz * f_up, 0.0)
            parts = [parts[0] + a, parts[1] + a * f_up, parts[2] + b, parts[3] + b * f_here]
        put((0, 0, -1), parts[0], parts[1])
        put((0, 0, 1), parts[2], parts[3])

        inner_sum = total(inner)
        yield
        yield
        diagonal = inner_sum
        late_row = jnp.zeros((1, width), f32)
        for (dx, dy, dz), (alone, shared) in sides.items():
            diagonal = diagonal + alone
            other = ((ix + dx) * ngy + iy + dy) * ngz + iz + dz
            valid = inside((dx, dy, dz))
            late_row = late_row - jnp.where((col == base + other) & valid, shared, 0.0)
        late_row = late_row + jnp.where(col == base + me, diagonal, 0.0)
        coupling[0] = late_row


    def solve(means):
        y_row = jnp.sum(inverse * means, axis=0, keepdims=True)
        y_col = jnp.sum(jnp.where(eye, y_row, 0.0), axis=1, keepdims=True)
        return y_row, y_col

    def block_row(dx, dy, dz):
        def near(at, step, count):
            return jnp.clip(at + step, 0, count - 1)

        b = (near(ix, dx, ngx) * ngy + near(iy, dy, ngy)) * ngz + near(iz, dz, ngz)
        return YB[pl.ds(b, 1)]

    def spread_blocks(y_col):
        YB[...] = jnp.broadcast_to(y_col, (n, bz))
        for k, v in enumerate(tables(block_row)):
            EY[k] = FL[k] * v

    cells = bx * by * bz

    def first_solve():
        collect(early, 0)
        m0_col = early[:, 0, 0:1]
        yield
        y_row = jnp.sum(inverse * (m0_col * (1.0 / cells)), axis=0, keepdims=True)
        yield
        y_col = jnp.sum(jnp.where(eye, y_row, 0.0), axis=1, keepdims=True)
        yield
        yield
        spread_blocks(y_col)

    sums = [[zeros, zeros] for _ in range(7)]
    parts = {}

    def add(i, k, v):
        if i < ex:
            if lo_x <= i < hi_x:
                sums[k][0] = sums[k][0] + v
        else:
            sums[k][1] = sums[k][1] + jnp.where(core_tiles[i - ex], v, 0.0)

    def coarse(field, group):
        found = yield from faces(lambda i: INV[i] * field[i], group)
        pooled = {}
        for i in group[::2]:
            gap = FL[flag_of(i)] * (field[i] - found[i][1])
            gap = gap + FL[flag_of(i + 1)] * (field[i + 1] - found[i + 1][1])
            gap = pair_y(gap)
            pooled[i] = (gap, up_z(gap), dn_z(gap))
        yield
        for i in group[::2]:
            gap, up, dn = pooled[i]
            below = IC[i // 2] * (gap + jnp.where(odd_lane, up, dn))
            for at in (i, i + 1):
                SEC[at] = found[at][0] + FL[flag_of(at)] * below

    def smooth(field, group, keep):
        found = yield from faces(lambda i: SEC[i], group)
        for i in group:
            v, lv = found[i]
            keep(i, v + INV[i] * (field[i] - lv))

    def image(load, group, keep):
        found = yield from faces(load, group)
        for i in group:
            keep(i, *found[i])

    def add_cycle(field, source, name, lo, hi, keep, extra):
        even, stop = (lo - 1) // 2 * 2, (hi + 2) // 2 * 2
        for group in groups(even, stop):
            if source is None:
                needs = {(k, at) for k in "fi" for _, at in reads("i", group)}
                needs |= named("n", [i // 2 for i in group]) | {"arrived"}
                needs |= named("r", range(tiles)) if group[0] >= ex else set()
            else:
                needs = reads(source, group)
            items.append((coarse(field, group), needs, {(name + "s", i) for i in group}))
        for group in groups(lo, hi):
            needs = reads(name + "s", group)
            if extra and group[0] >= ex:
                items.append(extra)
                extra = None
            items.append((smooth(field, group, keep), needs, {(name, i) for i in group}))

    def keep_direction(i, v):
        U[i] = v

    def keep_image(i, v, lv):
        w = FL[flag_of(i)] * lv
        W[i] = w
        if lo_x <= i < hi_x or i >= ex:
            D0[i] = v
        add(i, 0, R[i, :by] * v[:by])
        add(i, 1, w[:by] * v[:by])
        add(i, 2, w[:by])

    def keep_second(i, v):
        U[i] = v
        add(i, 3, W[i, :by] * v[:by])
        add(i, 4, R[i, :by] * v[:by])

    def keep_third(i, v, lv):
        q = FL[flag_of(i)][:by] * lv[:by]
        Q[i, :by] = q
        add(i, 5, q * v[:by])
        add(i, 6, q)

    def gather_sums(which):
        for k in which:
            a, b = sums[k]
            parts[k] = total(jnp.where(core_lanes, a, 0.0) + b)
        yield

    def core_of(name):
        return {(name, i) for i in range(lo_x, hi_x)} | {(name, ex + t) for t in range(tiles)}

    add_cycle(R, None, "d", 4, ex - 4, keep_direction, (first_solve(), set(), {"blocks"}))
    for group in groups(5, ex - 5):
        items.append(
            (image(lambda i: U[i] + EY[flag_of(i)], group, keep_image), reads("d", group) | {"blocks"}, {("w", i) for i in group})
        )
    add_cycle(W, "w", "u", 7, ex - 7, keep_second, None)
    items.append((couple(), set(), set()))
    items.append((gather_sums(range(3)), core_of("w"), set()))
    for group in groups(lo_x, hi_x):
        items.append(
            (image(lambda i: U[i], group, keep_third), reads("u", group), {("q", i) for i in group})
        )
    items.append((gather_sums(range(3, 5)), core_of("u"), set()))
    items.append((gather_sums(range(5, 7)), core_of("q"), set()))
    run(items)

    late_row = coupling[0]
    for k in range(7):
        late_row = jnp.where(col == k, parts[k], late_row)
    late_row = jnp.where(col == 7, m0, late_row)
    compact = base + 2 * n <= width
    if compact:
        late_row = jnp.where(col == base + n + me, parts[2], late_row)
    late_out[...] = late_row
    late[pl.ds(me, 1)] = late_row[None]
    spread(late_out, late, 1)
    if compact:
        spot = lax.broadcasted_iota(jnp.int32, (n, width), 1)
        owner = lax.broadcasted_iota(jnp.int32, (n, width), 0)
        own_lane = spot == base + owner
        placed = jnp.dot(
            inverse,
            (spot == base + n + owner).astype(f32),
            precision=HIGH,
            preferred_element_type=f32,
        )
    wait_sent(1)
    wait_sent(0)
    collect(late, 1)

    rows = late[:, 0, :]
    plain = jnp.sum(rows, axis=0, keepdims=True)
    if compact:
        y_col = jnp.sum(placed * plain, axis=1, keepdims=True) * (1.0 / cells)
    else:
        y_row, y_col = solve(rows[:, 2:3] * (1.0 / cells))
    spread_blocks(y_col)
    weighted = jnp.sum(rows * y_col, axis=0, keepdims=True)
    if compact:
        y_line = jnp.sum(jnp.where(own_lane, y_col, 0.0), axis=0, keepdims=True)
        quadratic = total(weighted * y_line)
    else:
        quadratic = total(weighted[:, base : base + n] * y_row)

    def pick(line, k):
        return jnp.sum(line[:, k : k + 1], axis=(0, 1), keepdims=True)

    rz, dad = pick(plain, 0), pick(plain, 1)
    w_u = pick(plain, 3) + pick(weighted, 2)
    r_u = pick(plain, 4) + pick(weighted, 7)
    u_q = (
        pick(plain, 5)
        + 2.0 * pick(weighted, 6)
        + quadratic
    )
    alpha, per_rz = rz / dad, 1.0 / rz
    new = (rz - alpha * dad) + alpha * (alpha * w_u - r_u)
    beta = new * per_rz
    grow = 1.0 + beta
    dad1 = grow * grow * dad - 2.0 * alpha * grow * w_u + alpha * alpha * u_q
    alpha1 = new / dad1
    c1 = alpha + alpha1 * grow
    c2 = alpha * alpha1

    def results(i, v, lv):
        fl = FL[flag_of(i)][:by]
        sol = c1 * D0[i, :by] - c2 * (U[i, :by] + v[:by])
        res = fl * R[i, :by] - c1 * W[i, :by] + c2 * (Q[i, :by] + fl * lv[:by])
        if i < ex:
            inner[i - lo_x] = sol, res
        else:
            SEC[i, :by], INV[i, :by] = sol, res

    inner = {}

    def turn_edges(xs):
        ends = {}
        for x in xs:
            tl, jl = edge.place(lo_x + x, 0)
            th, jh = edge.place(lo_x + x, 1)
            ends[x] = [
                (
                    spin(held[ex + tl, :by], -(GROUP * jl + HALO)),
                    spin(held[ex + th, :by], bz - HALO - (GROUP * jh + HALO)),
                )
                for held in (SEC, INV)
            ]
        yield
        for x in xs:
            for ref, whole, (low, high) in zip((sol_ref, res_ref), inner[x], ends[x]):
                whole = jnp.where(lane_y >= bz - HALO, high, whole)
                ref[x] = jnp.where(lane_y < HALO, low, whole)

    steps = [
        (image(lambda i: EY[flag_of(i)], group, results), set(), named("out", group))
        for group in reversed(groups(lo_x, hi_x))
    ]
    around_x = named("out", list(range(lo_x, hi_x)) + list(range(ex, ex + tiles)))
    steps += [(turn_edges(xs), around_x, set()) for xs in cut(0, bx, bx // 2)]
    run(steps)
    spread_done(early, 0)
    spread_done(late, 1)


def solution(mesh):
    counts = (mesh.shape["gx"], mesh.shape["gy"], mesh.shape["gz"])
    n = counts[0] * counts[1] * counts[2]

    def on_device(right_side, conductance, extents, coarse_factor):
        f32 = jnp.float32
        bx, by, bz = right_side.shape
        ex, ey = bx + 2 * HALO, by + 2 * HALO
        edge = Edge(bx, bz)
        slabs = ex + edge.tiles
        width = bz if n + 8 <= bz else bz + -(-n // 128) * 128
        vm = lambda *shape: pltpu.VMEM(shape, f32)
        field = vm(slabs, ey, bz)
        half = vm(slabs // 2, ey, bz)
        flags = vm(3 + len(edge.patterns), ey, bz)
        dma = pltpu.SemaphoreType.DMA
        scratch = [
            field,
            field,
            pltpu.VMEM(extents.shape, extents.dtype),
            pltpu.VMEM(coarse_factor.shape, coarse_factor.dtype),
            vm(1, bz),
            vm(27, 1, bz),
            vm(2, by, bz),
            vm(2, 2, 3, ey, bz),
            vm(1, bz),
            vm(n, 1, bz),
            vm(1, width),
            vm(n, 1, width),
            flags,
            flags,
            vm(slabs + 1, ey, bz),
            field,
            field,
            field,
            half,
            half,
            field,
            field,
            field,
            field,
            field,
            vm(n, bz),
            flags,
            dma((27,)),
            dma((27,)),
            dma((27,)),
            dma((27,)),
            dma((27,)),
            dma((27,)),
            dma((2,)),
            dma((2,)),
            dma((4,)),
        ]
        whole = pl.BlockSpec(memory_space=pltpu.VMEM)
        outer = pl.BlockSpec(memory_space=pltpu.HBM)
        both = pl.pallas_call(
            functools.partial(kernel, counts),
            out_shape=vm(2, bx, by, bz),
            in_specs=[outer, outer, outer, outer],
            out_specs=whole,
            scratch_shapes=scratch,
            compiler_params=pltpu.CompilerParams(
                collective_id=0, has_side_effects=True, vmem_limit_bytes=60000000
            ),
        )(right_side, conductance, extents, coarse_factor)
        return both[0], both[1]

    in_specs = (P("gx", "gy", "gz"), P("gx", "gy", "gz"), P("gx", "gy", "gz"), P())
    out_specs = (P("gx", "gy", "gz"), P("gx", "gy", "gz"))
    return jax.shard_map(
        on_device, mesh=mesh, in_specs=in_specs, out_specs=out_specs, check_vma=False
    )
```

```python
import functools

import jax
import jax.numpy as jnp
from jax import lax
from jax.experimental import pallas as pl
from jax.experimental.pallas import tpu as pltpu
from jax.sharding import PartitionSpec as P

OMEGA = 0.8
HALO = 8
GROUP = 3 * HALO
SPAN = 24
WIDE = 12
EDGES = 2
MESH = pl.DeviceIdType.MESH
HIGH = lax.Precision.HIGHEST
DIRS = [
    (dx, dy, dz)
    for dx in (-1, 0, 1)
    for dy in (-1, 0, 1)
    for dz in (-1, 0, 1)
    if (dx, dy, dz) != (0, 0, 0)
]
DIRS.sort(key=lambda d: -sum(abs(a) for a in d))


def code(dx, dy, dz):
    return (dx + 1) * 9 + (dy + 1) * 3 + dz + 1


class Edge:
    def __init__(self, bx, bz):
        self.bx, self.ex = bx, bx + 2 * HALO
        self.places = bz // GROUP
        tiles = -(-2 * self.ex // self.places)
        self.tiles = tiles + tiles % 2
        self.patterns, self.pattern_of = [], []
        for t in range(self.tiles):
            key = tuple(
                None if s is None else (self.block(s[0])[0], s[1])
                for s in (self.slab(t, j) for j in range(self.places))
            )
            if key not in self.patterns:
                self.patterns.append(key)
            self.pattern_of.append(self.patterns.index(key))

    def slab(self, t, j):
        slot = t + self.tiles * j
        return None if slot >= 2 * self.ex else (slot % self.ex, slot // self.ex)

    def place(self, s, side):
        slot = s + self.ex * side
        return slot % self.tiles, slot // self.tiles

    def block(self, s):
        if s < HALO:
            return 0, self.bx - HALO + s
        if s < HALO + self.bx:
            return 1, s - HALO
        return 2, s - HALO - self.bx


def kernel(
    counts,
    rhs_hbm,
    cond_hbm,
    ext_hbm,
    factor_hbm,
    both_ref,
    R,
    C,
    ext_ref,
    factor_ref,
    e_out,
    e_in,
    z_out,
    z_in,
    early_out,
    early,
    late_out,
    late,
    FL,
    F1,
    FX,
    FY,
    FZ,
    INV,
    C1,
    IC,
    SEC,
    D0,
    W,
    U,
    Q,
    YB,
    EY,
    send_c,
    recv_c,
    send_r,
    recv_r,
    send_e,
    recv_e,
    send_g,
    recv_g,
    load_sem,
):
    sol_ref, res_ref = both_ref.at[0], both_ref.at[1]
    ngx, ngy, ngz = counts
    n = ngx * ngy * ngz
    ix, iy, iz = lax.axis_index("gx"), lax.axis_index("gy"), lax.axis_index("gz")
    me = (ix * ngy + iy) * ngz + iz
    bx, by, bz = sol_ref.shape
    ex, ey = bx + 2 * HALO, by + 2 * HALO
    edge = Edge(bx, bz)
    tiles = edge.tiles
    f32 = jnp.float32
    lo_x, hi_x = HALO, HALO + bx

    def turned(at, step, count):
        moved = at + step
        return jnp.where(moved >= count, moved - count, moved)

    def everyone(act):
        if n <= 64:
            xs = [turned(ix, t, ngx) for t in range(ngx)]
            ys = [turned(iy, t, ngy) for t in range(ngy)]
            zs = [turned(iz, t, ngz) for t in range(ngz)]
            steps = [(a, b, c) for a in range(ngx) for b in range(ngy) for c in range(ngz)]
            steps.sort(
                key=lambda t: -sum(min(a, m - a) for a, m in zip(t, (ngx, ngy, ngz)))
            )
            for a, b, c in steps[:-1]:
                act((xs[a], ys[b], zs[c]))
        else:

            def one(t, carry):
                flat = (me + t) % n
                act((flat // (ngy * ngz), (flat // ngz) % ngy, flat % ngz))
                return carry

            lax.fori_loop(1, n, one, 0)

    core_x, core_y = pl.ds(lo_x, bx), pl.ds(0, by)
    loads = [
        pltpu.make_async_copy(src, dst, load_sem.at[k])
        for k, (src, dst) in enumerate(
            (
                (rhs_hbm, R.at[core_x, core_y]),
                (cond_hbm, C.at[core_x, core_y]),
                (ext_hbm, ext_ref),
                (factor_hbm, factor_ref),
            )
        )
    ]
    for load in loads:
        load.start()

    barrier = pltpu.get_barrier_semaphore()
    everyone(
        lambda device: pl.semaphore_signal(
            barrier, inc=1, device_id=device, device_id_type=MESH
        )
    )

    def inside(d):
        ok = None
        for at, step, count in zip((ix, iy, iz), d, counts):
            if step == 0:
                continue
            here = (at + step >= 0) & (at + step < count)
            ok = here if ok is None else ok & here
        return ok

    def x_from(dx):
        return pl.ds(bx, HALO) if dx == 1 else pl.ds(HALO, bx if dx == 0 else HALO)

    def x_into(dx):
        if dx == 0:
            return pl.ds(HALO, bx)
        return pl.ds(0, HALO) if dx == 1 else pl.ds(hi_x, HALO)

    def y_from(dy):
        return pl.ds(by - HALO, HALO) if dy == 1 else pl.ds(0, by if dy == 0 else HALO)

    def y_into(dy):
        if dy == 0:
            return pl.ds(0, by)
        return pl.ds(by + HALO, HALO) if dy == 1 else pl.ds(by, HALO)

    def landing(f, d):
        dx, dy, dz = d
        if dz != 0:
            return z_in.at[f, 1 if dz == 1 else 0, 1 - dx, y_into(dy)]
        return (R, C)[f].at[x_into(dx), y_into(dy)]

    def remote(src, dst, send, recv, d):
        return pltpu.make_async_remote_copy(
            src_ref=src,
            dst_ref=dst,
            send_sem=send,
            recv_sem=recv,
            device_id=(ix + d[0], iy + d[1], iz + d[2]),
            device_id_type=MESH,
        )

    def copies(f, d):
        dx, dy, dz = d
        k = code(*d)
        if dz != 0:
            src = z_out.at[f, y_from(dy)]
        else:
            src = (R, C)[f].at[x_from(dx), y_from(dy)]
        send, recv = ((send_r, recv_r), (send_c, recv_c))[f]
        out = [remote(src, landing(f, d), send.at[k], recv.at[k], d)]
        if f == 1:
            out.append(remote(e_out, e_in.at[code(-dx, -dy, -dz)], send_e.at[k], recv_e.at[k], d))
        return out

    odd = ix % 2 == 1

    def corner(d):
        return d[0] != 0 and d[1] != 0 and d[2] == 0

    def when_sent(f, act):
        for d in DIRS:

            @pl.when(inside(d))
            def _():
                values, *flags = copies(f, d)
                for c in flags:
                    act(c)
                if not corner(d):
                    act(values)
                    return

                if d[0] == 1:
                    act(values)
                    return

                @pl.when(jnp.logical_not(odd))
                def _():
                    act(values)

    def relayed(f, dy):
        field, k = (R, C)[f], code(-1, dy, 0)
        send, recv = ((send_r, recv_r), (send_c, recv_c))[f]
        return remote(
            field.at[x_from(-1), y_into(dy)],
            field.at[x_into(-1), y_into(dy)],
            send.at[k],
            recv.at[k],
            (-1, 0, 0),
        )

    def start_all(f):
        when_sent(f, lambda c: c.start())

    def relay(f):
        for dy in (-1, 1):

            @pl.when(inside((0, -dy, 0)) & odd)
            def _():
                for c in copies(f, (0, dy, 0)):
                    c.wait_recv()
                relayed(f, dy).start()

    def wait_all(f):
        for d in DIRS:
            ok = inside(tuple(-a for a in d))

            @pl.when(ok & jnp.logical_not(odd) if d[0] == 0 and d[2] == 0 else ok)
            def _():
                for c in copies(f, d):
                    c.wait_recv()

    def wait_sent(f):
        when_sent(f, lambda c: c.wait_send())
        for dy in (-1, 1):

            @pl.when(inside((0, -dy, 0)) & odd)
            def _():
                relayed(f, dy).wait_send()

    for d in DIRS:

        @pl.when(jnp.logical_not(inside(tuple(-a for a in d))))
        def _():
            for f in (0, 1):
                ref = landing(f, d)
                ref[...] = jnp.zeros(ref.shape, f32)
            e_in[code(*(-a for a in d))] = jnp.zeros((1, bz), f32)

    lane = lax.broadcasted_iota(jnp.int32, (ey, bz), 1)
    row = lax.broadcasted_iota(jnp.int32, (ey, bz), 0)
    odd_lane = lane % 2 == 1
    odd_row = (row % 2 == 1).reshape(ey // 8, 8, bz)
    lane_y = lane[:by]

    def up_y(v, k=1):
        return pltpu.roll(v, k, 0)

    def dn_y(v, k=1):
        return pltpu.roll(v, ey - k, 0)

    def spin(v, k):
        k = k % bz
        return v if k == 0 else pltpu.roll(v, k, 1)

    def up_z(v, k=1):
        return pltpu.roll(v, k, 1)

    def dn_z(v, k=1):
        return pltpu.roll(v, bz - k, 1)

    for load in loads[:3]:
        load.wait()
    own_limit = ext_ref[0].astype(f32)
    e_out[...] = jnp.broadcast_to(own_limit, (1, bz))
    for f, field in ((1, C), (0, R)):
        packed = jnp.zeros((by, bz), f32)
        for k in range(bx):
            moved = spin(field[lo_x + k, :by], 2 * HALO * k + HALO)
            packed = jnp.where(lane_y // (2 * HALO) == k, moved, packed)
        z_out[f] = packed

    def total(v):
        return jnp.sum(v, axis=(0, 1), keepdims=True)

    acc = R[lo_x, :by]
    for k in range(1, bx):
        acc = acc + R[lo_x + k, :by]
    m0 = total(jnp.where(lane_y.astype(f32) < own_limit, acc, 0.0))
    early_row = jnp.broadcast_to(m0, (1, bz))
    early_out[...] = early_row
    early[pl.ds(me, 1)] = early_row[None]

    def remote_row(out, into, base, device):
        return pltpu.make_async_remote_copy(
            src_ref=out,
            dst_ref=into.at[me],
            send_sem=send_g.at[base],
            recv_sem=recv_g.at[base],
            device_id=device,
            device_id_type=MESH,
        )

    def spread(out, into, base):
        everyone(lambda device: remote_row(out, into, base, device).start())

    def collect(into, base):
        part = into.at[pl.ds(0, n - 1)]
        pltpu.make_async_copy(part, part, recv_g.at[base]).wait()

    def spread_done(into, base):
        part = into.at[pl.ds(0, n - 1)]
        pltpu.make_async_copy(part, part, send_g.at[base]).wait()

    pl.semaphore_wait(barrier, n - 1)
    start_all(1)
    spread(early_out, early, 0)
    start_all(0)

    loads[3].wait()
    L = factor_ref[...].astype(f32)
    ri = lax.broadcasted_iota(jnp.int32, (n, n), 0)
    ci = lax.broadcasted_iota(jnp.int32, (n, n), 1)
    eye = ri == ci
    X = jnp.where(eye, 1.0 / jnp.where(eye, L, 1.0), 0.0)
    s = 1
    while s < n:
        pick = (ri // (2 * s) == ci // (2 * s)) & (ri % (2 * s) >= s) & (ci % (2 * s) < s)
        low = jnp.where(pick, L, 0.0)
        X = X - jnp.dot(
            X,
            jnp.dot(low, X, precision=HIGH, preferred_element_type=f32),
            precision=HIGH,
            preferred_element_type=f32,
        )
        s *= 2
    relay(1)
    inverse = lax.dot_general(
        X, X, (((0,), (0,)), ((), ())), precision=HIGH, preferred_element_type=f32
    )

    one_lane = lax.broadcasted_iota(jnp.int32, (1, bz), 1)
    bands = ((0, by), (1, HALO), (-1, HALO))

    def tables(value):
        rows = {
            (dx, dy, dz): value(dx, dy, dz)
            for dx in (-1, 0, 1)
            for dy in (-1, 0, 1)
            for dz in (-1, 0, 1)
        }
        out = [
            jnp.concatenate(
                [jnp.broadcast_to(rows[dx, dy, 0], (count, bz)) for dy, count in bands], axis=0
            )
            for dx in (-1, 0, 1)
        ]
        for pattern in edge.patterns:
            parts = []
            for dy, count in bands:
                line = None
                for j, key in enumerate(pattern):
                    if key is None:
                        continue
                    dx, start = key[0] - 1, GROUP * j
                    if key[1] == 0:
                        here = jnp.where(
                            one_lane < start + HALO, rows[dx, dy, -1], rows[dx, dy, 0]
                        )
                    else:
                        here = jnp.where(
                            one_lane < start + 2 * HALO, rows[dx, dy, 0], rows[dx, dy, 1]
                        )
                    line = here if line is None else jnp.where(one_lane >= start, here, line)
                parts.append(jnp.broadcast_to(line, (count, bz)))
            out.append(jnp.concatenate(parts, axis=0))
        return out

    def depths():
        plain = one_lane
        out = [plain] * 3
        for pattern in edge.patterns:
            line = None
            for j, key in enumerate(pattern):
                off = one_lane - GROUP * j
                if key is None:
                    here = jnp.full((1, bz), bz, jnp.int32)
                elif key[1] == 0:
                    here = jnp.where(off < HALO, off + bz - HALO, off - HALO)
                else:
                    here = jnp.where(off < 2 * HALO, off + bz - 2 * HALO, off - 2 * HALO)
                line = here if line is None else jnp.where(off >= 0, here, line)
            line = jnp.where(one_lane >= GROUP * edge.places, bz, line)
            out.append(line)
        return out

    def flag_of(i):
        return edge.block(i)[0] if i < ex else 3 + edge.pattern_of[i - ex]

    def build_edges(f, field, group):
        moved = {}
        for t in group:
            for j in range(edge.places):
                slab = edge.slab(t, j)
                if slab is None:
                    continue
                s, side = slab
                if f == 0 and s in (0, ex - 1):
                    moved[t, j] = None
                    continue
                which, k = edge.block(s)
                start, at = GROUP * j, 2 * HALO * k
                if side == 0:
                    own = spin(field[s], start + HALO)
                    far = spin(z_in[f, 1, which], start - at)
                else:
                    own = spin(field[s], start + 2 * HALO - bz)
                    far = spin(z_in[f, 0, which], start + HALO - at)
                moved[t, j] = own, far
        yield
        for t in group:
            acc = None
            for j in range(edge.places):
                start = GROUP * j
                if (t, j) not in moved:
                    acc = jnp.where(lane >= start, 0.0, acc)
                    break
                own, far = moved[t, j] or (0.0, 0.0)
                if edge.slab(t, j)[1] == 0:
                    here = jnp.where(lane < start + HALO, far, own)
                else:
                    here = jnp.where(lane < start + 2 * HALO, own, far)
                acc = here if acc is None else jnp.where(lane >= start, here, acc)
            field[ex + t] = jnp.where(lane < GROUP * edge.places, acc, 0.0)

    def pair_y(v):
        rows = v.reshape(ey // 8, 8, bz)
        swapped = jnp.where(odd_row, pltpu.roll(rows, 1, 1), pltpu.roll(rows, 7, 1))
        return (rows + swapped).reshape(ey, bz)

    def groups(lo, hi, span=SPAN):
        out = []
        for a, b in ((lo, hi), (ex, ex + tiles)):
            at = a
            while at < b:
                stop = min(b, at + span)
                out.append(list(range(at, stop)))
                at = stop
        return out

    def around(i):
        last = ex + tiles - 1
        before = (last, GROUP) if i == ex else (i - 1, 0)
        after = (ex, -GROUP) if i == last else (i + 1, 0)
        return before, after

    def faces(load, group):
        v, turned_v = {}, {}
        for i in group:
            v[i] = load(i)
        for at, k in (around(group[0])[0], around(group[-1])[1]):
            turned_v[at, k] = v[at] if k == 0 and at in v else spin(load(at), k)
        up = {i: up_z(v[i]) for i in group}
        yield
        gz, dn = {}, {}
        for i in group:
            gz[i] = FZ[i] * (v[i] - up[i])
            dn[i] = dn_z(gz[i])
        yield
        out = {}
        (b, kb), _ = around(group[0])
        gx = FX[group[0]] * (v[group[0]] - turned_v[b, kb])
        for i in group:
            if i == group[-1]:
                a, ka = around(i)[1]
                after = turned_v[a, ka]
            else:
                after = v[i + 1]
            gx_next = FX[i + 1] * (after - v[i])
            gy = FY[i] * (v[i] - up_y(v[i]))
            out[i] = (v[i], (gx - gx_next) + ((gy - dn_y(gy)) + (gz[i] - dn[i])))
            gx = gx_next
        return out

    def reads(name, group):
        return {(name, i) for i in group} | {
            (name, around(group[0])[0][0]),
            (name, around(group[-1])[1][0]),
        }

    def run(items):
        done, open_items, at = set(), [], 0
        while at < len(items) or open_items:
            still = []
            for gen, gives in open_items:
                try:
                    next(gen)
                    still.append((gen, gives))
                except StopIteration:
                    done |= gives
            open_items = still
            if not open_items and at < len(items):
                assert items[at][1] <= done, items[at][1] - done
            if at < len(items) and items[at][1] <= done:
                gen, _, gives = items[at]
                at += 1
                try:
                    next(gen)
                    open_items.append((gen, gives))
                except StopIteration:
                    done |= gives

    wait_all(1)
    relay(0)

    def limit(dx, dy, dz):
        return e_out[...] if (dx, dy, dz) == (0, 0, 0) else e_in[code(dx, dy, dz)]

    for k, (a, z) in enumerate(zip(tables(limit), depths())):
        z_f, even_f = z.astype(f32), (z - z % 2).astype(f32)
        FL[k] = (z_f < a).astype(f32)
        F1[k] = (even_f < a).astype(f32)

    items = []
    pairs, edge_pairs = ex // 2, tiles // 2
    last_pair = pairs + edge_pairs - 1

    def make_faces(group):
        up = {i: up_z(C[i]) for i in group}
        (b, kb), _ = around(group[0])
        before = None if group[0] == 0 else spin(C[b], kb)
        yield
        for i in group:
            c = C[i]
            if before is not None:
                FX[i] = 0.5 * (before + c)
            before = c
            FY[i] = 0.5 * (c + up_y(c))
            FZ[i] = 0.5 * (c + up[i])

    def make_wrap():
        around_face = spin(FX[ex], -GROUP)
        yield
        FX[ex + tiles] = around_face

    def make_inverse(group):
        dn = {i: dn_z(FZ[i]) for i in group}
        yield
        for i in group:
            fy = FY[i]
            diagonal = (FX[i] + FX[i + 1]) + (fy + dn_y(fy)) + (FZ[i] + dn[i])
            fl = FL[flag_of(i)]
            INV[i] = OMEGA * fl / (diagonal + 1.0 - fl)

    def make_pooled(group):
        pooled = {}
        for q in group:
            v = pair_y(C[2 * q] + C[2 * q + 1])
            pooled[q] = v, up_z(v), dn_z(v)
        yield
        for q in group:
            v, up, dn = pooled[q]
            C1[q] = (v + jnp.where(odd_lane, up, dn)) * 0.125

    def beside(q):
        before = (last_pair, GROUP) if q == pairs else (q - 1, 0)
        after = (pairs, -GROUP) if q == last_pair else (q + 1, 0)
        return before, after

    def make_coarse_inverse(group):
        found = {}
        for q in group:
            c = C1[q]
            (b, kb), (a, ka) = beside(q)
            found[q] = up_z(c, 2), dn_z(c, 2), spin(C1[b], kb), spin(C1[a], ka)
        yield
        for q in group:
            c = C1[q]
            up, dn, before, after = found[q]
            diagonal = 3.0 * c + 0.5 * ((before + after) + (up_y(c, 2) + dn_y(c, 2)) + (up + dn))
            fl = F1[flag_of(2 * q)]
            IC[q] = OMEGA * fl / (4.0 * diagonal + 1.0 - fl)

    def cut(lo, hi, span):
        return [list(range(a, min(hi, a + span))) for a in range(lo, hi, span)]

    def named(name, these):
        return {(name, i) for i in these}

    def face_items(lo, hi, needs):
        return [
            (make_faces(g), needs if lo < ex else named("c", range(tiles)), named("f", g))
            for g in cut(lo, hi, WIDE)
        ]

    def inverse_items(lo, hi):
        return [
            (make_inverse(g), named("f", g + [g[-1] + 1]), named("i", g)) for g in cut(lo, hi, WIDE)
        ]

    def pooled_items(lo, hi):
        needs = set() if lo < pairs else named("c", range(tiles))
        return [(make_pooled(g), needs, named("p", g)) for g in cut(lo, hi, WIDE // 2)]

    def coarse_items(lo, hi):
        return [
            (
                make_coarse_inverse(g),
                named("p", [at for q in g for at, _ in beside(q)] + g),
                named("n", g),
            )
            for g in cut(lo, hi, WIDE // 2)
        ]

    def edge_items(f, name):
        field = (R, C)[f]
        return [
            (build_edges(f, field, g), set() if f else {"arrived"}, named(name, g))
            for g in cut(0, tiles, EDGES)
        ]

    def mixed(*lists):
        out, lists = [], [list(x) for x in lists]
        while any(lists):
            for x in lists:
                if x:
                    out.append(x.pop(0))
        return out

    def arrive():
        wait_all(0)
        yield

    items += mixed(
        edge_items(1, "c"),
        face_items(0, ex, set()) + inverse_items(1, ex - 1),
        pooled_items(0, pairs) + coarse_items(1, pairs - 1),
    )
    items.append((arrive(), set(), {"arrived"}))
    items += mixed(
        edge_items(0, "r"),
        face_items(ex, ex + tiles, None)
        + [(make_wrap(), named("f", [ex]), named("f", [ex + tiles]))]
        + inverse_items(ex, ex + tiles),
        pooled_items(pairs, pairs + edge_pairs) + coarse_items(pairs, pairs + edge_pairs),
    )

    off = lane_y % GROUP
    slot0 = (lane_y // GROUP) * tiles

    def core_edge(t, lo_off, hi_off):
        slot = slot0 + t
        low = (slot >= lo_x) & (slot < hi_x) & lo_off
        high = (slot >= ex + lo_x) & (slot < ex + hi_x) & hi_off
        return (low | high) & (lane_y < GROUP * edge.places)

    core_off = (off >= HALO) & (off < 2 * HALO)
    core_tiles = [core_edge(t, core_off, core_off) for t in range(tiles)]
    core_lanes = (lane_y >= HALO) & (lane_y < bz - HALO)

    zeros = jnp.zeros((by, bz), f32)
    scalars = 8
    width = late.shape[-1]
    base = scalars if width == bz else bz
    col = lax.broadcasted_iota(jnp.int32, (1, width), 1)
    coupling = {}

    def couple():
        flux_z = FZ[lo_x, :by]
        flux_y = FY[lo_x]
        for i in range(lo_x + 1, hi_x):
            flux_z = flux_z + FZ[i, :by]
            flux_y = flux_y + FY[i]
        fl = FL[1]
        fl_up, fl_core = up_y(fl), fl[:by]
        step = fl_core - up_z(fl)[:by]
        inner = jnp.where(lane_y >= 1, flux_z * (step * step), 0.0)
        none = jnp.logical_and(off < 0, off >= 0)
        low_face = [core_edge(t, off == HALO, none) for t in range(tiles)]
        high_face = [core_edge(t, none, off == 2 * HALO) for t in range(tiles)]
        sides = {}

        def put(d, alone, shared):
            sides[d] = (total(alone), total(shared))

        alone = FX[lo_x, :by] * fl_core
        put((-1, 0, 0), alone, alone * FL[0, :by])
        alone = FX[hi_x, :by] * fl_core
        put((1, 0, 0), alone, alone * FL[2, :by])
        alone = jnp.where(row == 0, flux_y * fl, 0.0)
        put((0, -1, 0), alone, alone * fl_up)
        alone = jnp.where(row == by, flux_y * fl_up, 0.0)
        put((0, 1, 0), alone, alone * fl)
        parts = [zeros] * 4
        for t in range(tiles):
            f_edge = FL[3 + edge.pattern_of[t]]
            f_here, f_up = f_edge[:by], up_z(f_edge)[:by]
            fz = FZ[ex + t, :by]
            a = jnp.where(low_face[t], fz * f_here, 0.0)
            b = jnp.where(high_face[t], fz * f_up, 0.0)
            parts = [parts[0] + a, parts[1] + a * f_up, parts[2] + b, parts[3] + b * f_here]
        put((0, 0, -1), parts[0], parts[1])
        put((0, 0, 1), parts[2], parts[3])

        inner_sum = total(inner)
        yield
        yield
        diagonal = inner_sum
        late_row = jnp.zeros((1, width), f32)
        for (dx, dy, dz), (alone, shared) in sides.items():
            diagonal = diagonal + alone
            other = ((ix + dx) * ngy + iy + dy) * ngz + iz + dz
            valid = inside((dx, dy, dz))
            late_row = late_row - jnp.where((col == base + other) & valid, shared, 0.0)
        late_row = late_row + jnp.where(col == base + me, diagonal, 0.0)
        coupling[0] = late_row


    def solve(means):
        y_row = jnp.sum(inverse * means, axis=0, keepdims=True)
        y_col = jnp.sum(jnp.where(eye, y_row, 0.0), axis=1, keepdims=True)
        return y_row, y_col

    def block_row(dx, dy, dz):
        def near(at, step, count):
            return jnp.clip(at + step, 0, count - 1)

        b = (near(ix, dx, ngx) * ngy + near(iy, dy, ngy)) * ngz + near(iz, dz, ngz)
        return YB[pl.ds(b, 1)]

    def spread_blocks(y_col):
        YB[...] = jnp.broadcast_to(y_col, (n, bz))
        for k, v in enumerate(tables(block_row)):
            EY[k] = FL[k] * v

    cells = bx * by * bz

    def first_solve():
        collect(early, 0)
        m0_col = early[:, 0, 0:1]
        yield
        y_row = jnp.sum(inverse * (m0_col * (1.0 / cells)), axis=0, keepdims=True)
        yield
        y_col = jnp.sum(jnp.where(eye, y_row, 0.0), axis=1, keepdims=True)
        yield
        yield
        spread_blocks(y_col)

    sums = [[zeros, zeros] for _ in range(7)]
    parts = {}

    def add(i, k, v):
        if i < ex:
            if lo_x <= i < hi_x:
                sums[k][0] = sums[k][0] + v
        else:
            sums[k][1] = sums[k][1] + jnp.where(core_tiles[i - ex], v, 0.0)

    def coarse(field, group):
        found = yield from faces(lambda i: INV[i] * field[i], group)
        pooled = {}
        for i in group[::2]:
            gap = FL[flag_of(i)] * (field[i] - found[i][1])
            gap = gap + FL[flag_of(i + 1)] * (field[i + 1] - found[i + 1][1])
            gap = pair_y(gap)
            pooled[i] = (gap, up_z(gap), dn_z(gap))
        yield
        for i in group[::2]:
            gap, up, dn = pooled[i]
            below = IC[i // 2] * (gap + jnp.where(odd_lane, up, dn))
            for at in (i, i + 1):
                SEC[at] = found[at][0] + FL[flag_of(at)] * below

    def smooth(field, group, keep):
        found = yield from faces(lambda i: SEC[i], group)
        for i in group:
            v, lv = found[i]
            keep(i, v + INV[i] * (field[i] - lv))

    def image(load, group, keep):
        found = yield from faces(load, group)
        for i in group:
            keep(i, *found[i])

    def add_cycle(field, source, name, lo, hi, keep, extra):
        even, stop = (lo - 1) // 2 * 2, (hi + 2) // 2 * 2
        for group in groups(even, stop):
            if source is None:
                needs = {(k, at) for k in "fi" for _, at in reads("i", group)}
                needs |= named("n", [i // 2 for i in group]) | {"arrived"}
                needs |= named("r", range(tiles)) if group[0] >= ex else set()
            else:
                needs = reads(source, group)
            items.append((coarse(field, group), needs, {(name + "s", i) for i in group}))
        for group in groups(lo, hi):
            needs = reads(name + "s", group)
            if extra and group[0] >= ex:
                items.append(extra)
                extra = None
            items.append((smooth(field, group, keep), needs, {(name, i) for i in group}))

    def keep_direction(i, v):
        U[i] = v

    def keep_image(i, v, lv):
        w = FL[flag_of(i)] * lv
        W[i] = w
        if lo_x <= i < hi_x or i >= ex:
            D0[i] = v
        add(i, 0, R[i, :by] * v[:by])
        add(i, 1, w[:by] * v[:by])
        add(i, 2, w[:by])

    def keep_second(i, v):
        U[i] = v
        add(i, 3, W[i, :by] * v[:by])
        add(i, 4, R[i, :by] * v[:by])

    def keep_third(i, v, lv):
        q = FL[flag_of(i)][:by] * lv[:by]
        Q[i, :by] = q
        add(i, 5, q * v[:by])
        add(i, 6, q)

    def gather_sums(which):
        for k in which:
            a, b = sums[k]
            parts[k] = total(jnp.where(core_lanes, a, 0.0) + b)
        yield

    def core_of(name):
        return {(name, i) for i in range(lo_x, hi_x)} | {(name, ex + t) for t in range(tiles)}

    add_cycle(R, None, "d", 4, ex - 4, keep_direction, (first_solve(), set(), {"blocks"}))
    for group in groups(5, ex - 5):
        items.append(
            (image(lambda i: U[i] + EY[flag_of(i)], group, keep_image), reads("d", group) | {"blocks"}, {("w", i) for i in group})
        )
    add_cycle(W, "w", "u", 7, ex - 7, keep_second, None)
    items.append((couple(), set(), set()))
    items.append((gather_sums(range(3)), core_of("w"), set()))
    for group in groups(lo_x, hi_x):
        items.append(
            (image(lambda i: U[i], group, keep_third), reads("u", group), {("q", i) for i in group})
        )
    items.append((gather_sums(range(3, 5)), core_of("u"), set()))
    items.append((gather_sums(range(5, 7)), core_of("q"), set()))
    run(items)

    late_row = coupling[0]
    for k in range(7):
        late_row = jnp.where(col == k, parts[k], late_row)
    late_row = jnp.where(col == 7, m0, late_row)
    compact = base + 2 * n <= width
    if compact:
        late_row = jnp.where(col == base + n + me, parts[2], late_row)
    late_out[...] = late_row
    late[pl.ds(me, 1)] = late_row[None]
    spread(late_out, late, 1)
    if compact:
        spot = lax.broadcasted_iota(jnp.int32, (n, width), 1)
        owner = lax.broadcasted_iota(jnp.int32, (n, width), 0)
        own_lane = spot == base + owner
        placed = jnp.dot(
            inverse,
            (spot == base + n + owner).astype(f32),
            precision=HIGH,
            preferred_element_type=f32,
        )
    wait_sent(1)
    wait_sent(0)
    collect(late, 1)

    rows = late[:, 0, :]
    plain = jnp.sum(rows, axis=0, keepdims=True)
    if compact:
        y_col = jnp.sum(placed * plain, axis=1, keepdims=True) * (1.0 / cells)
    else:
        y_row, y_col = solve(rows[:, 2:3] * (1.0 / cells))
    spread_blocks(y_col)
    weighted = jnp.sum(rows * y_col, axis=0, keepdims=True)
    if compact:
        y_line = jnp.sum(jnp.where(own_lane, y_col, 0.0), axis=0, keepdims=True)
        quadratic = total(weighted * y_line)
    else:
        quadratic = total(weighted[:, base : base + n] * y_row)

    def pick(line, k):
        return jnp.sum(line[:, k : k + 1], axis=(0, 1), keepdims=True)

    rz, dad = pick(plain, 0), pick(plain, 1)
    w_u = pick(plain, 3) + pick(weighted, 2)
    r_u = pick(plain, 4) + pick(weighted, 7)
    u_q = (
        pick(plain, 5)
        + 2.0 * pick(weighted, 6)
        + quadratic
    )
    alpha, per_rz = rz / dad, 1.0 / rz
    new = (rz - alpha * dad) + alpha * (alpha * w_u - r_u)
    beta = new * per_rz
    grow = 1.0 + beta
    dad1 = grow * grow * dad - 2.0 * alpha * grow * w_u + alpha * alpha * u_q
    alpha1 = new / dad1
    c1 = alpha + alpha1 * grow
    c2 = alpha * alpha1

    def results(i, v, lv):
        fl = FL[flag_of(i)][:by]
        sol = c1 * D0[i, :by] - c2 * (U[i, :by] + v[:by])
        res = fl * R[i, :by] - c1 * W[i, :by] + c2 * (Q[i, :by] + fl * lv[:by])
        if i < ex:
            inner[i - lo_x] = sol, res
        else:
            SEC[i, :by], INV[i, :by] = sol, res

    inner = {}

    def turn_edges(xs):
        ends = {}
        for x in xs:
            tl, jl = edge.place(lo_x + x, 0)
            th, jh = edge.place(lo_x + x, 1)
            ends[x] = [
                (
                    spin(held[ex + tl, :by], -(GROUP * jl + HALO)),
                    spin(held[ex + th, :by], bz - HALO - (GROUP * jh + HALO)),
                )
                for held in (SEC, INV)
            ]
        yield
        for x in xs:
            for ref, whole, (low, high) in zip((sol_ref, res_ref), inner[x], ends[x]):
                whole = jnp.where(lane_y >= bz - HALO, high, whole)
                ref[x] = jnp.where(lane_y < HALO, low, whole)

    steps = [
        (image(lambda i: EY[flag_of(i)], group, results), set(), named("out", group))
        for group in reversed(groups(lo_x, hi_x))
    ]
    around_x = named("out", list(range(lo_x, hi_x)) + list(range(ex, ex + tiles)))
    steps += [(turn_edges(xs), around_x, set()) for xs in cut(0, bx, bx // 2)]
    run(steps)
    spread_done(early, 0)
    spread_done(late, 1)


def solution(mesh):
    counts = (mesh.shape["gx"], mesh.shape["gy"], mesh.shape["gz"])
    n = counts[0] * counts[1] * counts[2]

    def on_device(right_side, conductance, extents, coarse_factor):
        f32 = jnp.float32
        bx, by, bz = right_side.shape
        ex, ey = bx + 2 * HALO, by + 2 * HALO
        edge = Edge(bx, bz)
        slabs = ex + edge.tiles
        width = bz if n + 8 <= bz else bz + -(-n // 128) * 128
        vm = lambda *shape: pltpu.VMEM(shape, f32)
        field = vm(slabs, ey, bz)
        half = vm(slabs // 2, ey, bz)
        flags = vm(3 + len(edge.patterns), ey, bz)
        dma = pltpu.SemaphoreType.DMA
        scratch = [
            field,
            field,
            pltpu.VMEM(extents.shape, extents.dtype),
            pltpu.VMEM(coarse_factor.shape, coarse_factor.dtype),
            vm(1, bz),
            vm(27, 1, bz),
            vm(2, by, bz),
            vm(2, 2, 3, ey, bz),
            vm(1, bz),
            vm(n, 1, bz),
            vm(1, width),
            vm(n, 1, width),
            flags,
            flags,
            vm(slabs + 1, ey, bz),
            field,
            field,
            field,
            half,
            half,
            field,
            field,
            field,
            field,
            field,
            vm(n, bz),
            flags,
            dma((27,)),
            dma((27,)),
            dma((27,)),
            dma((27,)),
            dma((27,)),
            dma((27,)),
            dma((2,)),
            dma((2,)),
            dma((4,)),
        ]
        whole = pl.BlockSpec(memory_space=pltpu.VMEM)
        outer = pl.BlockSpec(memory_space=pltpu.HBM)
        both = pl.pallas_call(
            functools.partial(kernel, counts),
            out_shape=vm(2, bx, by, bz),
            in_specs=[outer, outer, outer, outer],
            out_specs=whole,
            scratch_shapes=scratch,
            compiler_params=pltpu.CompilerParams(
                collective_id=0, has_side_effects=True, vmem_limit_bytes=60000000
            ),
        )(right_side, conductance, extents, coarse_factor)
        return both[0], both[1]

    in_specs = (P("gx", "gy", "gz"), P("gx", "gy", "gz"), P("gx", "gy", "gz"), P())
    out_specs = (P("gx", "gy", "gz"), P("gx", "gy", "gz"))
    return jax.shard_map(
        on_device, mesh=mesh, in_specs=in_specs, out_specs=out_specs, check_vma=False
    )
```
